8 devices in a mesh: data: 8 (over z, y, x, core).
Axes of the slice: x: 2, y: 2, z: 1, core: 2. Of those that a mesh axis runs over, the one named last changes fastest.
Arguments:
- tokens: bfloat16 [8192, 768], P('data')
- w_in: bfloat16 [768, 3072], replicated
- w_out: bfloat16 [3072, 768], replicated
- task_heads: bfloat16 [4, 768, 3], replicated
- labels: int32 [4, 8192], P(None, 'data')
- label_mask: int32 [4, 8192], P(None, 'data')
Outputs:
- output 1: float32 [4], replicated
- output 2: float32 [2359296], P('data')
- output 3: float32 [2359296], P('data')
All inputs are finite; a program needn't handle non-finite values.
Results may differ from the reference program's by a relative error of at most 0.00839703.
Values are sent between devices in bfloat16 or wider.
A program may use at most 1 GiB of HBM per device.

```python
import jax
import jax.numpy as jnp
from jax import lax

MODEL_DIM = 768
HIDDEN_DIM = 3072
NUM_TASKS = 4
NUM_CLASSES = 3
TOK_DEV = 1024
GROUP_SIZE = 8
SOLVER_STEPS = 20


def draw_labels(rng_key):
    sub_keys = jax.random.split(rng_key, 7)
    tokens_total = TOK_DEV * GROUP_SIZE
    dev_class = jax.random.randint(sub_keys[0], (GROUP_SIZE, 1), 0, NUM_CLASSES)
    keep_draw = jax.random.randint(sub_keys[1], (GROUP_SIZE, TOK_DEV), 0, 4)
    free_class = jax.random.randint(sub_keys[2], (GROUP_SIZE, TOK_DEV), 0, NUM_CLASSES)
    common_class = jnp.where(keep_draw < 3, dev_class, free_class).reshape(tokens_total)
    noise_draw = jax.random.randint(sub_keys[3], (NUM_TASKS, tokens_total), 0, 4)
    task_class = jax.random.randint(sub_keys[4], (NUM_TASKS, tokens_total), 0, NUM_CLASSES)
    labels = jnp.where(noise_draw == 0, task_class, common_class[None, :]).astype(jnp.int32)
    mask_level = jax.random.randint(sub_keys[5], (NUM_TASKS, GROUP_SIZE, 1), 5, 100)
    mask_draw = jax.random.randint(sub_keys[6], (NUM_TASKS, GROUP_SIZE, TOK_DEV), 0, 100)
    label_mask = (mask_draw < mask_level).astype(jnp.int32).reshape(NUM_TASKS, tokens_total)
    return labels, label_mask


def setup_inputs(seed: int = 0) -> dict:
    rng_keys = jax.random.split(jax.random.key(seed), 6)
    tokens_total = TOK_DEV * GROUP_SIZE
    tokens = jax.random.normal(rng_keys[0], (tokens_total, MODEL_DIM), jnp.float32)
    w_in = jax.random.normal(rng_keys[1], (MODEL_DIM, HIDDEN_DIM), jnp.float32) * MODEL_DIM ** -0.5
    w_out = jax.random.normal(rng_keys[2], (HIDDEN_DIM, MODEL_DIM), jnp.float32) * HIDDEN_DIM ** -0.5
    shared_head = jax.random.normal(rng_keys[3], (MODEL_DIM, NUM_CLASSES), jnp.float32)
    own_head = jax.random.normal(rng_keys[4], (NUM_TASKS, MODEL_DIM, NUM_CLASSES), jnp.float32)
    head_sign = (1 - 2 * (jnp.arange(NUM_TASKS) % 2)).astype(jnp.float32)
    task_heads = (head_sign[:, None, None] * shared_head[None] + 0.6 * own_head) * (1.5 * MODEL_DIM ** -0.5)
    labels, label_mask = draw_labels(rng_keys[5])
    return {"tokens": tokens.astype(jnp.bfloat16), "w_in": w_in.astype(jnp.bfloat16), "w_out": w_out.astype(jnp.bfloat16), "task_heads": task_heads.astype(jnp.bfloat16), "labels": labels, "label_mask": label_mask}


def device_grads(x_loc, w_in, w_out, task_heads, lab_loc, mask_loc):
    pre_act = jnp.dot(x_loc, w_in, preferred_element_type=jnp.float32)
    act_out, gelu_slope = jax.jvp(jax.nn.gelu, (pre_act,), (jnp.ones_like(pre_act),))
    act_bf = act_out.astype(jnp.bfloat16)
    residual = x_loc.astype(jnp.float32) + jnp.dot(act_bf, w_out, preferred_element_type=jnp.float32)
    z_bf = residual.astype(jnp.bfloat16)
    heads_wide = task_heads.astype(jnp.float32)
    logits = jnp.einsum("bd,tdc->tbc", z_bf.astype(jnp.float32), heads_wide)
    soft_prob = jax.nn.softmax(logits, axis=-1)
    onehot = (lab_loc[:, :, None] == jnp.arange(NUM_CLASSES)[None, None, :]).astype(jnp.float32)
    d_logit = (mask_loc[:, :, None].astype(jnp.float32) * (soft_prob - onehot)).astype(jnp.bfloat16)
    d_resid = jnp.einsum("tbc,tdc->tbd", d_logit.astype(jnp.float32), heads_wide).astype(jnp.bfloat16)
    d_wide = d_resid.astype(jnp.float32)
    grad_w_out = jnp.einsum("bf,tbd->tfd", act_bf.astype(jnp.float32), d_wide)
    d_act = jnp.einsum("tbd,fd->tbf", d_wide, w_out.astype(jnp.float32))
    d_pre = (d_act * gelu_slope[None]).astype(jnp.bfloat16)
    grad_w_in = jnp.einsum("bd,tbf->tdf", x_loc.astype(jnp.float32), d_pre.astype(jnp.float32))
    return grad_w_in, grad_w_out


def solve_weights(gram_mat):
    step_scale = jnp.trace(gram_mat) / NUM_TASKS

    def solver_step(step_idx, weights):
        pull_vec = (gram_mat * weights[None, :]).sum(axis=1)
        raised = weights * jnp.exp(-pull_vec / step_scale)
        return raised / raised.sum()

    init_weights = jnp.full((NUM_TASKS,), 1.0 / NUM_TASKS, jnp.float32)
    return lax.fori_loop(0, SOLVER_STEPS, solver_step, init_weights)


def reference(tokens, w_in, w_out, task_heads, labels, label_mask):
    inv_count = 1.0 / jnp.maximum(label_mask.sum(axis=1), 1).astype(jnp.float32)
    tok_blocks = tokens.reshape(GROUP_SIZE, TOK_DEV, MODEL_DIM)
    lab_blocks = labels.reshape(NUM_TASKS, GROUP_SIZE, TOK_DEV).transpose(1, 0, 2)
    mask_blocks = label_mask.reshape(NUM_TASKS, GROUP_SIZE, TOK_DEV).transpose(1, 0, 2)
    flat_len = MODEL_DIM * HIDDEN_DIM

    def add_device(grad_sum, block_in):
        x_loc, lab_loc, mask_loc = block_in
        grad_w_in, grad_w_out = device_grads(x_loc, w_in, w_out, task_heads, lab_loc, mask_loc)
        flat_grad = jnp.concatenate([grad_w_in.reshape(NUM_TASKS, flat_len), grad_w_out.reshape(NUM_TASKS, flat_len)], axis=1)
        part_grad = (flat_grad * inv_count[:, None]).astype(jnp.bfloat16).astype(jnp.float32)
        return grad_sum + part_grad, None

    grad_sum, _ = lax.scan(add_device, jnp.zeros((NUM_TASKS, 2 * flat_len), jnp.float32), (tok_blocks, lab_blocks, mask_blocks))
    gram_mat = jnp.dot(grad_sum, grad_sum.T, preferred_element_type=jnp.float32)
    weights = solve_weights(gram_mat)
    combined = (weights[:, None] * grad_sum).sum(axis=0)
    return weights, combined[:flat_len], combined[flat_len:]
```

```python
import jax
import jax.numpy as jnp
from jax import lax
from jax.sharding import PartitionSpec as P

SOLVER_STEPS = 20


def solve_weights(gram_mat):
    num_tasks = gram_mat.shape[0]
    step_scale = jnp.trace(gram_mat) / num_tasks
    weights = jnp.full((num_tasks,), 1.0 / num_tasks, jnp.float32)
    for _ in range(SOLVER_STEPS):
        pull_vec = (gram_mat * weights[None, :]).sum(axis=1)
        raised = weights * jnp.exp(-pull_vec / step_scale)
        weights = raised / raised.sum()
    return weights


def gelu_pair(pre_act):
    return jax.jvp(jax.nn.gelu, (pre_act,), (jnp.ones_like(pre_act),))


def solution(mesh):
    n = mesh.shape["data"]

    def local_step(x_loc, w_in, w_out, heads, lab_loc, mask_loc):
        num_tasks, dim, _ = heads.shape
        hidden = w_in.shape[1]
        hid = hidden // n
        me = lax.axis_index("data")
        f32, bf16 = jnp.float32, jnp.bfloat16
        label_count = lax.psum(mask_loc.sum(axis=1), "data")
        inv_count = 1.0 / jnp.maximum(label_count, 1).astype(f32)
        x_all = lax.all_gather(x_loc, "data")
        pre_act = jnp.dot(x_loc, w_in, preferred_element_type=f32)
        act_bf = jax.nn.gelu(pre_act).astype(bf16)
        z_bf = (x_loc.astype(f32) + jnp.dot(act_bf, w_out, preferred_element_type=f32)).astype(bf16)
        logits = jnp.einsum("bd,tdc->tbc", z_bf, heads, preferred_element_type=f32)
        soft_prob = jax.nn.softmax(logits, axis=-1)
        onehot = (lab_loc[:, :, None] == jnp.arange(logits.shape[-1])).astype(f32)
        e_loc = (mask_loc[:, :, None].astype(f32) * (soft_prob - onehot)).astype(bf16)
        e_all = lax.all_gather(e_loc, "data")
        w_in_j = lax.dynamic_slice_in_dim(w_in, me * hid, hid, 1)
        w_out_j = lax.dynamic_slice_in_dim(w_out, me * hid, hid, 0)
        pre_j = jnp.einsum("gbd,df->gbf", x_all, w_in_j, preferred_element_type=f32)
        act_j, slope_j = gelu_pair(pre_j)
        act_j = act_j.astype(bf16)
        g_in, g_out = [], []
        for t in range(num_tasks):
            dz = jnp.einsum("gbc,dc->gbd", e_all[:, t], heads[t], preferred_element_type=f32).astype(bf16)
            part_out = jnp.einsum("gbf,gbd->gfd", act_j, dz, preferred_element_type=f32)
            d_act = jnp.einsum("gbd,fd->gbf", dz, w_out_j, preferred_element_type=f32)
            q = (d_act * slope_j).astype(bf16)
            part_in = jnp.einsum("gbd,gbf->gdf", x_all, q, preferred_element_type=f32)
            g_out.append((part_out * inv_count[t]).astype(bf16).sum(axis=0, dtype=f32))
            g_in.append((part_in * inv_count[t]).astype(bf16).sum(axis=0, dtype=f32))
        rows = []
        for t in range(num_tasks):
            rows.append(jnp.stack([(g_in[t] * g_in[s]).sum() + (g_out[t] * g_out[s]).sum() for s in range(num_tasks)]))
        gram = lax.psum(jnp.stack(rows), "data")
        w = solve_weights(gram)
        comb_in = sum(w[t] * g_in[t] for t in range(num_tasks))
        comb_out = sum(w[t] * g_out[t] for t in range(num_tasks))
        moved = lax.all_to_all(comb_in.reshape(n, dim // n, hid), "data", 0, 0)
        grad_in = moved.transpose(1, 0, 2).reshape(-1)
        return w, grad_in, comb_out.reshape(-1)

    return jax.shard_map(local_step, mesh=mesh, in_specs=(P("data", None), P(), P(), P(), P(None, "data"), P(None, "data")), out_specs=(P(), P("data"), P("data")), check_vma=False)
```

```python
import jax
import jax.numpy as jnp
from jax import lax
from jax.experimental import pallas as pl
from jax.experimental.pallas import tpu as pltpu
from jax.sharding import PartitionSpec as P

SOLVER_STEPS = 20
MESH = pl.DeviceIdType.MESH
F32, BF16 = jnp.float32, jnp.bfloat16
NUM_DEV = 8
TASKS = 4
CLASSES = 3
TOK = 1024
DIM = 768
HIDDEN = 3072
HID = HIDDEN // NUM_DEV
FEAT = DIM // NUM_DEV
HEAD_ROWS = 32
CHUNK = 768
ROWS = 512
PAIRS = [(t, s) for t in range(TASKS) for s in range(t, TASKS)]
GELU_C = 0.7978845608028654
GELU_K = 0.044715


def dot_nn(a, b):
    return lax.dot_general(a, b, (((1,), (0,)), ((), ())), preferred_element_type=F32)


def dot_nt(a, b):
    return lax.dot_general(a, b, (((1,), (1,)), ((), ())), preferred_element_type=F32)


def lanes(row, width):
    return jnp.concatenate([row] * (width // row.shape[1]), axis=1)


def gelu_value(p):
    return p * (0.5 * (1.0 + jnp.tanh(GELU_C * (p + GELU_K * (p * p * p)))))


def gelu_both(p):
    sq = p * p
    th = jnp.tanh(GELU_C * (p + GELU_K * (sq * p)))
    cdf = 0.5 * (1.0 + th)
    slope = cdf + (0.5 * p) * ((1.0 - th * th) * (GELU_C * (1.0 + (3.0 * GELU_K) * sq)))
    return p * cdf, slope


def kernel(x_hbm, w_in_hbm, w_out_hbm, head_ref, lab_ref, mask_ref, alpha_ref, out1_hbm, out2_hbm,
           xs, w1, w2, w1j, w1t, w2j, abuf, zacc, ef, es, etok, hm, act_t, slope_t, dz, q_t, acc1, acc2,
           cnt, inv, gram, gsend, grecv, stage1, stage2,
           x_send, x_recv, e_send, e_recv, c_send, c_recv, g_send, g_recv, o_send, o_recv, l_sem):
    me = lax.axis_index("data")
    core = lax.rem(me, 2)
    cx = lax.rem(lax.div(me, 2), 2)
    cy = lax.div(me, 4)

    def flip(v, b):
        return v + b - 2 * v * b

    def peer(slot):
        hop = slot // 2
        first, second = (1 if hop in (1, 3) else 0), (1 if hop in (2, 3) else 0)
        bx = first * (1 - core) + second * core
        by = first * core + second * (1 - core)
        bc = slot % 2
        return flip(cx, bx) * 2 + flip(cy, by) * 4 + flip(core, jnp.int32(bc))

    def remote(src, dst, send, recv, dev):
        return pltpu.make_async_remote_copy(src_ref=src, dst_ref=dst, send_sem=send, recv_sem=recv, device_id=(dev,), device_id_type=MESH)

    def x_copy(src_slot, dst_slot):
        dev = {1: 1, 2: 2, 4: 4, 3: 1, 5: 1, 6: 4, 7: 1}[dst_slot]
        return remote(xs.at[src_slot], xs.at[dst_slot], x_send.at[dst_slot], x_recv.at[dst_slot], peer(dev))

    def e_copy(slot):
        return remote(es.at[0], es.at[slot], e_send.at[slot], e_recv.at[slot], peer(slot))

    def c_copy(slot):
        return remote(cnt.at[0], cnt.at[slot], c_send.at[slot], c_recv.at[slot], peer(slot))

    def local(src, dst, i):
        return pltpu.make_async_copy(src, dst, l_sem.at[i])

    nchunk = HIDDEN // CHUNK
    load_x = local(x_hbm, xs.at[0], 0)
    load_w1 = [local(w_in_hbm.at[:, pl.ds(CHUNK * i, CHUNK)], w1.at[i], 1 + i) for i in range(nchunk)]
    load_w2 = [local(w_out_hbm.at[pl.ds(CHUNK * i, CHUNK), :], w2.at[i], 1 + nchunk + i) for i in range(nchunk)]
    load_w1j = local(w_in_hbm.at[:, pl.ds(pl.multiple_of(me * HID, HID), HID)], w1j, 1 + 2 * nchunk)
    load_w2j = local(w_out_hbm.at[pl.ds(pl.multiple_of(me * HID, HID), HID), :], w2j, 2 + 2 * nchunk)
    load_x.start()
    for i in range(nchunk):
        load_w1[i].start()
        load_w2[i].start()
    load_w1j.start()
    load_w2j.start()

    counts = jnp.sum(mask_ref[...].astype(F32), axis=1, keepdims=True)
    cnt[0, 0:TASKS, :] = jnp.broadcast_to(counts, (TASKS, 128))
    cnt[0, TASKS:8, :] = jnp.zeros((8 - TASKS, 128), F32)
    head = head_ref[...].astype(F32)
    row_task = lax.rem(lax.broadcasted_iota(jnp.int32, (HEAD_ROWS, DIM), 0), 8)
    for t in range(TASKS):
        hm[t] = jnp.where(row_task == t, head, 0.0).astype(BF16)

    barrier = pltpu.get_barrier_semaphore()
    for s in range(1, NUM_DEV):
        pl.semaphore_signal(barrier, inc=1, device_id=(peer(s),), device_id_type=MESH)
    pl.semaphore_wait(barrier, NUM_DEV - 1)

    load_x.wait()
    x_copy(0, 1).start()
    x_copy(0, 2).start()
    for s in range(1, NUM_DEV):
        c_copy(s).start()

    zacc[...] = xs[0].astype(F32)
    for c in load_w1 + load_w2:
        c.wait()

    def forward(i, carry):
        h = lax.div(i, TOK // ROWS)
        r = pl.ds(pl.multiple_of(lax.rem(i, TOK // ROWS) * ROWS, ROWS), ROWS)
        abuf[...] = gelu_value(dot_nn(xs[0, r, :], w1[h])).astype(BF16)
        zacc[r, :] += dot_nn(abuf[...], w2[h])
        return carry

    lax.fori_loop(0, nchunk * (TOK // ROWS), forward, 0)

    ef[...] = jnp.zeros_like(ef)
    for r in range(TOK // ROWS):
        cols = slice(r * ROWS, (r + 1) * ROWS)
        logits = dot_nt(head_ref[...], zacc[cols, :].astype(BF16))
        l = [logits[8 * c:8 * c + TASKS] for c in range(CLASSES)]
        top = jnp.maximum(jnp.maximum(l[0], l[1]), l[2])
        ex = [jnp.exp(v - top) for v in l]
        total = ex[0] + ex[1] + ex[2]
        lab = lab_ref[:, cols]
        m = mask_ref[:, cols].astype(F32)
        for c in range(CLASSES):
            ef[8 * c:8 * c + TASKS, cols] = m * (ex[c] / total - (lab == c).astype(F32))
    es[0] = ef[...].astype(BF16)

    acc1[...] = jnp.zeros_like(acc1)
    acc2[...] = jnp.zeros_like(acc2)
    load_w1j.wait()
    load_w2j.wait()
    w1t[...] = w1j[...].astype(F32).T.astype(BF16)

    for s in range(1, NUM_DEV):
        e_copy(s).start()
    total_cnt = cnt[0]
    for s in range(1, NUM_DEV):
        c_copy(s).wait_recv()
        total_cnt = total_cnt + cnt[s]
    inv[...] = lanes(1.0 / jnp.maximum(total_cnt, 1.0), DIM)

    def shard(s, carry):
        for k in range(1, NUM_DEV):
            @pl.when(s == k)
            def _():
                x_copy(0, k).wait_recv()
                e_copy(k).wait_recv()
                if k == 1:
                    x_copy(0, 2).wait_send()
                    x_copy(0, 4).start()
                if k in (2, 4, 6):
                    x_copy(k, k + 1).start()
                if k == 2:
                    x_copy(2, 6).start()

        etok[...] = es[s].astype(F32).T.astype(BF16)

        def preact(i, c):
            r = pl.ds(pl.multiple_of(i * ROWS, ROWS), ROWS)
            a, sl = gelu_both(dot_nt(w1t[...], xs[s, r, :]))
            act_t[:, r] = a.astype(BF16)
            slope_t[:, r] = sl
            return c

        lax.fori_loop(0, TOK // ROWS, preact, 0)

        def task(t, c):
            scale = inv[pl.ds(t, 1), :]
            dz[...] = dot_nn(etok[...], hm[t]).astype(BF16)
            q_t[...] = (dot_nt(w2j[...], dz[...]) * slope_t[...]).astype(BF16)
            acc2[t] += (dot_nn(act_t[...], dz[...]) * scale).astype(BF16).astype(F32)
            acc1[t] += (dot_nn(q_t[...], xs[s]) * scale).astype(BF16).astype(F32)
            return c

        lax.fori_loop(0, TASKS, task, 0)
        return carry

    lax.fori_loop(0, NUM_DEV, shard, 0)

    def gram_rows(i, sums):
        r = pl.ds(pl.multiple_of(i * 8, 8), 8)
        out = list(sums)
        for acc in (acc1, acc2):
            for c in range(DIM // 128):
                g = [acc[t, r, 128 * c:128 * c + 128] for t in range(TASKS)]
                for k, (t, u) in enumerate(PAIRS):
                    out[k] = out[k] + g[t] * g[u]
        return tuple(out)

    sums = lax.fori_loop(0, HID // 8, gram_rows, tuple(jnp.zeros((8, 128), F32) for _ in PAIRS))
    for k in range(len(PAIRS)):
        gram[me, k:k + 1, :] = jnp.broadcast_to(jnp.sum(sums[k]), (1, 128))
    gram[me, len(PAIRS):16, :] = jnp.zeros((16 - len(PAIRS), 128), F32)

    def gram_copy(s, block):
        return remote(gram.at[block], gram.at[block], g_send.at[s], g_recv.at[s], peer(s))

    for s in range(1, NUM_DEV):
        gram_copy(s, me).start()
    for s in range(1, NUM_DEV):
        gram_copy(s, me).wait_recv()
    gram_sum = gram[0]
    for d in range(1, NUM_DEV):
        gram_sum = gram_sum + gram[d]
    m = {}
    for k, (t, u) in enumerate(PAIRS):
        m[t, u] = m[u, t] = gram_sum[k:k + 1, :]
    step_scale = (m[0, 0] + m[1, 1] + m[2, 2] + m[3, 3]) / TASKS
    al = [jnp.full((1, 128), 1.0 / TASKS, F32) for _ in range(TASKS)]
    for _ in range(SOLVER_STEPS):
        raised = []
        for t in range(TASKS):
            pull = (m[t, 0] * al[0] + m[t, 1] * al[1]) + (m[t, 2] * al[2] + m[t, 3] * al[3])
            raised.append(al[t] * jnp.exp(-pull / step_scale))
        norm = (raised[0] + raised[1]) + (raised[2] + raised[3])
        al = [r / norm for r in raised]
    for t in range(TASKS):
        alpha_ref[t] = jnp.max(al[t])

    for c in range(DIM // 128):
        cols = slice(128 * c, 128 * c + 128)
        comb = al[0] * acc1[0, :, cols]
        for t in range(1, TASKS):
            comb = comb + al[t] * acc1[t, :, cols]
        gsend[cols, :] = comb.T

    def o_copy(s):
        dev = peer(s)
        rows = pl.ds(pl.multiple_of(dev * FEAT, FEAT), FEAT)
        return remote(gsend.at[rows, :], grecv.at[s], o_send.at[s], o_recv.at[s], dev)

    order = (6, 7, 4, 5, 2, 3, 1)
    for s in order:
        o_copy(s).start()

    for c in range(DIM // 128):
        cols = slice(128 * c, 128 * c + 128)
        comb = al[0] * acc2[0, :, cols]
        for t in range(1, TASKS):
            comb = comb + al[t] * acc2[t, :, cols]
        stage2[pl.ds(c, HID, stride=DIM // 128), :] = comb
    store2 = local(stage2, out2_hbm, 0)
    store2.start()

    per = HID // 128

    def place(dev, block):
        for b in range(per):
            stage1[pl.ds(dev * per + b, FEAT, stride=HIDDEN // 128), :] = block[:, 128 * b:128 * b + 128]

    def owner(slot):
        hop = slot // 2
        first, second = (1 if hop in (1, 3) else 0), (1 if hop in (2, 3) else 0)
        oc = flip(core, jnp.int32(slot % 2))
        bx = first * (1 - oc) + second * oc
        by = first * oc + second * (1 - oc)
        return flip(cx, bx) * 2 + flip(cy, by) * 4 + oc

    place(me, gsend[pl.ds(pl.multiple_of(me * FEAT, FEAT), FEAT), :])
    for s in (1, 2, 3, 4, 5, 6, 7):
        o_copy(s).wait_recv()
        place(owner(s), grecv[s])
    store1 = local(stage1, out1_hbm, 1)
    store1.start()

    x_copy(0, 1).wait_send()
    for k in (4, 3, 5, 6, 7):
        x_copy(0, k).wait_send()
    for s in range(1, NUM_DEV):
        e_copy(s).wait_send()
        c_copy(s).wait_send()
        gram_copy(s, me).wait_send()
        o_copy(s).wait_send()
    store2.wait()
    store1.wait()


def solution(mesh):
    def local_step(x_loc, w_in, w_out, heads, lab_loc, mask_loc):
        head_rows = jnp.pad(heads.transpose(2, 0, 1), ((0, 1), (0, 8 - TASKS), (0, 0))).reshape(HEAD_ROWS, DIM)
        hbm = pl.BlockSpec(memory_space=pl.ANY)
        vmem = pl.BlockSpec(memory_space=pltpu.VMEM)
        sem = pltpu.SemaphoreType.DMA((NUM_DEV,))
        v = pltpu.VMEM
        flat = NUM_DEV * 0 + DIM * HIDDEN // NUM_DEV // 128
        alpha, out1, out2 = pl.pallas_call(
            kernel,
            out_shape=(
                jax.ShapeDtypeStruct((TASKS,), F32),
                jax.ShapeDtypeStruct((flat, 128), F32),
                jax.ShapeDtypeStruct((flat, 128), F32),
            ),
            in_specs=[hbm, hbm, hbm, vmem, vmem, vmem],
            out_specs=(pl.BlockSpec(memory_space=pltpu.SMEM), hbm, hbm),
            scratch_shapes=[
                v((NUM_DEV, TOK, DIM), BF16),
                v((HIDDEN // CHUNK, DIM, CHUNK), BF16),
                v((HIDDEN // CHUNK, CHUNK, DIM), BF16),
                v((DIM, HID), BF16),
                v((HID, DIM), BF16),
                v((HID, DIM), BF16),
                v((ROWS, CHUNK), BF16),
                v((TOK, DIM), F32),
                v((HEAD_ROWS, TOK), F32),
                v((NUM_DEV, HEAD_ROWS, TOK), BF16),
                v((TOK, HEAD_ROWS), BF16),
                v((TASKS, HEAD_ROWS, DIM), BF16),
                v((HID, TOK), BF16),
                v((HID, TOK), F32),
                v((TOK, DIM), BF16),
                v((HID, TOK), BF16),
                v((TASKS, HID, DIM), F32),
                v((TASKS, HID, DIM), F32),
                v((NUM_DEV, 8, 128), F32),
                v((8, DIM), F32),
                v((NUM_DEV, 16, 128), F32),
                v((DIM, HID), F32),
                v((NUM_DEV, FEAT, HID), F32),
                v((flat, 128), F32),
                v((flat, 128), F32),
                sem, sem, sem, sem, sem, sem, sem, sem, sem, sem,
                pltpu.SemaphoreType.DMA((3 + 2 * (HIDDEN // CHUNK),)),
            ],
            compiler_params=pltpu.CompilerParams(collective_id=0, has_side_effects=True, vmem_limit_bytes=66_000_000),
            name="trunk",
        )(x_loc, w_in, w_out, head_rows, lab_loc, mask_loc)
        return alpha, out1.reshape(-1), out2.reshape(-1)

    return jax.shard_map(local_step, mesh=mesh, in_specs=(P("data", None), P(), P(), P(), P(None, "data"), P(None, "data")), out_specs=(P(), P("data"), P("data")), check_vma=False)
```

```python
import jax
import jax.numpy as jnp
from jax import lax
from jax.experimental import pallas as pl
from jax.experimental.pallas import tpu as pltpu
from jax.sharding import PartitionSpec as P

SOLVER_STEPS = 20
MESH = pl.DeviceIdType.MESH
F32, BF16 = jnp.float32, jnp.bfloat16
NUM_DEV = 8
TASKS = 4
CLASSES = 3
TOK = 1024
DIM = 768
HIDDEN = 3072
HID = HIDDEN // NUM_DEV
FEAT = DIM // NUM_DEV
HEAD_ROWS = 32
CHUNK = 768
ROWS = 512
NCHUNK = HIDDEN // CHUNK
QUARTER = TOK // TASKS
PAIRS = [(t, s) for t in range(TASKS) for s in range(t, TASKS)]
GELU_C = 0.7978845608028654
GELU_K = 0.044715


def dot_nn(a, b):
    return lax.dot_general(a, b, (((1,), (0,)), ((), ())), preferred_element_type=F32)


def dot_nt(a, b):
    return lax.dot_general(a, b, (((1,), (1,)), ((), ())), preferred_element_type=F32)


def lanes(row, width):
    return jnp.concatenate([row] * (width // row.shape[1]), axis=1)


def gelu_parts(p):
    a = (GELU_C * GELU_K) * (p * p)
    th = jnp.tanh(p * (a + GELU_C))
    return a, th, 0.5 + 0.5 * th


def gelu_value(p):
    return p * gelu_parts(p)[2]


def gelu_both(p):
    a, th, cdf = gelu_parts(p)
    slope = cdf + ((1.0 - th * th) * p) * (1.5 * a + 0.5 * GELU_C)
    return p * cdf, slope


def kernel(x_hbm, w_in_hbm, w_out_hbm, head_ref, lab_ref, mask_ref, alpha_ref, out1_hbm, out2_hbm,
           xs, w1, w2, w1j, w1t, w2j, abuf0, abuf1, zacc, hrow, hbc, ef, es, ecur, act0, act1, slope0, slope1,
           dz0, dz1, q0, q1, acc1, acc2, cnt, inv, gram, gsend, grecv, stage1, stage2,
           x_send, x_recv, e_send, e_recv, c_send, c_recv, g_send, g_recv, o_send, o_recv, l_sem):
    me = lax.axis_index("data")
    core = lax.rem(me, 2)
    cx = lax.rem(lax.div(me, 2), 2)
    cy = lax.div(me, 4)

    def flip(v, b):
        return v + b - 2 * v * b

    def peer(slot):
        hop = slot // 2
        first, second = (1 if hop in (1, 3) else 0), (1 if hop in (2, 3) else 0)
        bx = first * (1 - core) + second * core
        by = first * core + second * (1 - core)
        bc = slot % 2
        return flip(cx, bx) * 2 + flip(cy, by) * 4 + flip(core, jnp.int32(bc))

    def remote(src, dst, send, recv, dev):
        return pltpu.make_async_remote_copy(src_ref=src, dst_ref=dst, send_sem=send, recv_sem=recv, device_id=(dev,), device_id_type=MESH)

    def x_copy(src_slot, dst_slot):
        dev = {1: 1, 2: 2, 4: 4, 3: 1, 5: 1, 6: 4, 7: 1}[dst_slot]
        return remote(xs.at[src_slot], xs.at[dst_slot], x_send.at[dst_slot], x_recv.at[dst_slot], peer(dev))

    def e_copy(slot):
        return remote(es.at[0], es.at[slot], e_send.at[slot], e_recv.at[slot], peer(slot))

    def c_copy(slot):
        return remote(cnt.at[0], cnt.at[slot], c_send.at[slot], c_recv.at[slot], peer(slot))

    def local(src, dst, i):
        return pltpu.make_async_copy(src, dst, l_sem.at[i])

    def load_w1(i):
        return local(w_in_hbm.at[:, pl.ds(pl.multiple_of(CHUNK * i, CHUNK), CHUNK)], w1.at[i], 3 + i)

    def load_w2(i):
        return local(w_out_hbm.at[pl.ds(pl.multiple_of(CHUNK * i, CHUNK), CHUNK), :], w2.at[i], 3 + NCHUNK + i)

    load_x = local(x_hbm, xs.at[0], 0)
    load_w1j = local(w_in_hbm.at[:, pl.ds(pl.multiple_of(me * HID, HID), HID)], w1j, 1)
    load_w2j = local(w_out_hbm.at[pl.ds(pl.multiple_of(me * HID, HID), HID), :], w2j, 2)
    load_x.start()
    load_w1j.start()
    for i in range(NCHUNK):
        load_w1(i).start()
        load_w2(i).start()
    load_w2j.start()

    barrier = pltpu.get_barrier_semaphore()
    for s in range(1, NUM_DEV):
        pl.semaphore_signal(barrier, inc=1, device_id=(peer(s),), device_id_type=MESH)

    counts = jnp.sum(mask_ref[...].astype(F32), axis=1, keepdims=True)
    cnt[0, 0:TASKS, :] = jnp.broadcast_to(counts, (TASKS, 128))
    cnt[0, TASKS:8, :] = jnp.zeros((8 - TASKS, 128), F32)
    hrow[...] = jnp.zeros_like(hrow)
    for c in range(CLASSES):
        hrow[8 * c:8 * c + TASKS, :] = head_ref[c].astype(F32)
    head = hrow[...].astype(BF16)

    pl.semaphore_wait(barrier, NUM_DEV - 1)
    load_x.wait()
    x_copy(0, 1).start()
    x_copy(0, 2).start()
    for s in range(1, NUM_DEV):
        c_copy(s).start()

    block = lax.div(lax.broadcasted_iota(jnp.int32, (HEAD_ROWS, TASKS * CLASSES * 128), 1), 128)
    pick = lax.rem(block, CLASSES) * 8 + lax.div(block, CLASSES)
    ones = (lax.broadcasted_iota(jnp.int32, block.shape, 0) == pick).astype(F32).astype(BF16)
    wide = dot_nn(hrow[...].T.astype(BF16), ones)
    for k in range(TASKS * CLASSES):
        hbc[k] = wide[:, 128 * k:128 * k + 128]
    load_w1j.wait()
    w1t[...] = w1j[...].astype(F32).T.astype(BF16)

    abuf1[...] = jnp.zeros_like(abuf1)
    zacc[...] = xs[0].astype(F32)
    half0, half1 = slice(0, ROWS), slice(ROWS, TOK)

    def forward(h, carry):
        load_w1(h).wait()
        load_w2(h).wait()
        acc1[h] = jnp.zeros((HID, DIM), F32)
        acc2[h] = jnp.zeros((HID, DIM), F32)
        abuf0[...] = gelu_value(dot_nn(xs[0, half0, :], w1[h])).astype(BF16)
        zacc[half1, :] += dot_nn(abuf1[...], w2[jnp.maximum(h - 1, 0)])
        abuf1[...] = gelu_value(dot_nn(xs[0, half1, :], w1[h])).astype(BF16)
        zacc[half0, :] += dot_nn(abuf0[...], w2[h])
        return carry

    lax.fori_loop(0, NCHUNK, forward, 0)
    zacc[half1, :] += dot_nn(abuf1[...], w2[NCHUNK - 1])

    acts, slopes, dzs, qs = (act0, act1), (slope0, slope1), (dz0, dz1), (q0, q1)

    def preact(slot, part, quarter):
        r = pl.ds(pl.multiple_of(quarter * QUARTER, QUARTER), QUARTER)
        a, sl = gelu_both(dot_nt(w1t[...], xs[slot, r, :]))
        acts[part][:, r] = a.astype(BF16)
        slopes[part][:, r] = sl

    for r in range(TOK // ROWS):
        cols = slice(r * ROWS, (r + 1) * ROWS)
        logits = dot_nt(head, zacc[cols, :].astype(BF16))
        l = [logits[8 * c:8 * c + TASKS] for c in range(CLASSES)]
        top = jnp.maximum(jnp.maximum(l[0], l[1]), l[2])
        ex = [jnp.exp(v - top) for v in l]
        total = ex[0] + ex[1] + ex[2]
        lab = lab_ref[:, cols]
        m = mask_ref[:, cols].astype(F32)
        for c in range(CLASSES):
            err = m * (ex[c] / total - (lab == c).astype(F32))
            for t in range(TASKS):
                ef[8 * t + c:8 * t + c + 1, cols] = err[t:t + 1]
    for t in range(TASKS):
        ef[8 * t + CLASSES:8 * t + 8, :] = jnp.zeros((8 - CLASSES, TOK), F32)
    es[0] = ef[...].astype(BF16)
    for t in range(TASKS):
        ecur[0, t] = es[0, 8 * t:8 * t + 8, :].astype(F32)

    for k in range(TOK // QUARTER):
        preact(0, 0, k)

    def make_dz(dst, part, t):
        e = ecur[part, t]
        rows = [jnp.broadcast_to(e[c:c + 1, :], (16, TOK)) for c in range(CLASSES)]
        for k in range(DIM // 16):
            f = slice(16 * k, 16 * k + 16)
            h = [lanes(hbc[CLASSES * t + c, f, :], TOK) for c in range(CLASSES)]
            dst[f, :] = (h[0] * rows[0] + h[1] * rows[1] + h[2] * rows[2]).astype(BF16)

    for s in range(1, NUM_DEV):
        e_copy(s).start()
    make_dz(dz0, 0, 0)
    load_w2j.wait()
    total_cnt = cnt[0]
    for s in range(1, NUM_DEV):
        c_copy(s).wait_recv()
        total_cnt = total_cnt + cnt[s]
    inv[...] = lanes(1.0 / jnp.maximum(total_cnt, 1.0), DIM)

    def tokens_ready(s):
        for k in range(1, NUM_DEV):
            @pl.when(s == k - 1)
            def _():
                x_copy(0, k).wait_recv()
                if k == 2:
                    x_copy(0, 2).wait_send()
                    x_copy(0, 4).start()
                    x_copy(2, 6).start()
                if k in (2, 4, 6):
                    x_copy(k, k + 1).start()

    def errors_ready(s, part):
        for k in range(1, NUM_DEV):
            @pl.when(s == k - 1)
            def _():
                e_copy(k).wait_recv()
                for t in range(TASKS):
                    ecur[part, t] = es[k, 8 * t:8 * t + 8, :].astype(F32)

    def run_task(s, part, t, j, next_part, next_t):
        nxt = jnp.minimum(s + 1, NUM_DEV - 1)
        scale = inv[pl.ds(t, 1), :]
        qs[j][...] = (dot_nn(w2j[...], dzs[j][...]) * slopes[part][...]).astype(BF16)
        acc2[t] += (dot_nt(acts[part][...], dzs[j][...]) * scale).astype(BF16).astype(F32)
        make_dz(dzs[1 - j], next_part, next_t)
        preact(nxt, 1 - part, t)
        acc1[t] += (dot_nn(qs[j][...], xs[s]) * scale).astype(BF16).astype(F32)

    def shard_pair(sp, carry):
        for part in range(2):
            s = 2 * sp + part
            tokens_ready(s)

            def task_pair(tp, c):
                @pl.when(tp == 1)
                def _():
                    errors_ready(s, 1 - part)
                run_task(s, part, 2 * tp, 0, part, 2 * tp + 1)
                wrap = lax.div(2 * tp + 2, TASKS)
                run_task(s, part, 2 * tp + 1, 1, part + wrap * (1 - 2 * part), 2 * tp + 2 - TASKS * wrap)
                return c

            lax.fori_loop(0, TASKS // 2, task_pair, 0)
        return carry

    lax.fori_loop(0, NUM_DEV // 2, shard_pair, 0)

    def gram_rows(i, sums):
        r = pl.ds(pl.multiple_of(i * 8, 8), 8)
        out = list(sums)
        for acc in (acc1, acc2):
            for c in range(DIM // 128):
                g = [acc[t, r, 128 * c:128 * c + 128] for t in range(TASKS)]
                for k, (t, u) in enumerate(PAIRS):
                    out[k] = out[k] + g[t] * g[u]
        return tuple(out)

    sums = lax.fori_loop(0, HID // 8, gram_rows, tuple(jnp.zeros((8, 128), F32) for _ in PAIRS))
    for k in range(len(PAIRS)):
        gram[me, k:k + 1, :] = jnp.broadcast_to(jnp.sum(sums[k]), (1, 128))
    gram[me, len(PAIRS):16, :] = jnp.zeros((16 - len(PAIRS), 128), F32)

    def gram_copy(s, block):
        return remote(gram.at[block], gram.at[block], g_send.at[s], g_recv.at[s], peer(s))

    for s in range(1, NUM_DEV):
        gram_copy(s, me).start()
    for s in range(1, NUM_DEV):
        gram_copy(s, me).wait_recv()
    gram_sum = gram[0]
    for d in range(1, NUM_DEV):
        gram_sum = gram_sum + gram[d]
    m = {}
    for k, (t, u) in enumerate(PAIRS):
        m[t, u] = m[u, t] = gram_sum[k:k + 1, :]
    step_scale = (m[0, 0] + m[1, 1] + m[2, 2] + m[3, 3]) / TASKS
    al = [jnp.full((1, 128), 1.0 / TASKS, F32) for _ in range(TASKS)]
    for _ in range(SOLVER_STEPS):
        raised = []
        for t in range(TASKS):
            pull = (m[t, 0] * al[0] + m[t, 1] * al[1]) + (m[t, 2] * al[2] + m[t, 3] * al[3])
            raised.append(al[t] * jnp.exp(-pull / step_scale))
        norm = (raised[0] + raised[1]) + (raised[2] + raised[3])
        al = [r / norm for r in raised]
    for t in range(TASKS):
        alpha_ref[t] = jnp.max(al[t])

    for c in range(DIM // 128):
        cols = slice(128 * c, 128 * c + 128)
        comb = al[0] * acc1[0, :, cols]
        for t in range(1, TASKS):
            comb = comb + al[t] * acc1[t, :, cols]
        gsend[cols, :] = comb.T

    def o_copy(s):
        dev = peer(s)
        rows = pl.ds(pl.multiple_of(dev * FEAT, FEAT), FEAT)
        return remote(gsend.at[rows, :], grecv.at[s], o_send.at[s], o_recv.at[s], dev)

    order = (6, 7, 4, 5, 2, 3, 1)
    for s in order:
        o_copy(s).start()

    for c in range(DIM // 128):
        cols = slice(128 * c, 128 * c + 128)
        comb = al[0] * acc2[0, :, cols]
        for t in range(1, TASKS):
            comb = comb + al[t] * acc2[t, :, cols]
        stage2[pl.ds(c, HID, stride=DIM // 128), :] = comb
    store2 = local(stage2, out2_hbm, 0)
    store2.start()

    per = HID // 128

    def place(dev, block):
        for b in range(per):
            stage1[pl.ds(dev * per + b, FEAT, stride=HIDDEN // 128), :] = block[:, 128 * b:128 * b + 128]

    def owner(slot):
        hop = slot // 2
        first, second = (1 if hop in (1, 3) else 0), (1 if hop in (2, 3) else 0)
        oc = flip(core, jnp.int32(slot % 2))
        bx = first * (1 - oc) + second * oc
        by = first * oc + second * (1 - oc)
        return flip(cx, bx) * 2 + flip(cy, by) * 4 + oc

    place(me, gsend[pl.ds(pl.multiple_of(me * FEAT, FEAT), FEAT), :])
    for s in (1, 2, 3, 4, 5, 6, 7):
        o_copy(s).wait_recv()
        place(owner(s), grecv[s])
    store1 = local(stage1, out1_hbm, 1)
    store1.start()

    x_copy(0, 1).wait_send()
    for k in (4, 3, 5, 6, 7):
        x_copy(0, k).wait_send()
    for s in range(1, NUM_DEV):
        e_copy(s).wait_send()
        c_copy(s).wait_send()
        gram_copy(s, me).wait_send()
        o_copy(s).wait_send()
    store2.wait()
    store1.wait()


def solution(mesh):
    def local_step(x_loc, w_in, w_out, heads, lab_loc, mask_loc):
        hbm = pl.BlockSpec(memory_space=pl.ANY)
        vmem = pl.BlockSpec(memory_space=pltpu.VMEM)
        sem = pltpu.SemaphoreType.DMA((NUM_DEV,))
        v = pltpu.VMEM
        flat = DIM * HIDDEN // NUM_DEV // 128
        alpha, out1, out2 = pl.pallas_call(
            kernel,
            out_shape=(
                jax.ShapeDtypeStruct((TASKS,), F32),
                jax.ShapeDtypeStruct((flat, 128), F32),
                jax.ShapeDtypeStruct((flat, 128), F32),
            ),
            in_specs=[hbm, hbm, hbm, vmem, vmem, vmem],
            out_specs=(pl.BlockSpec(memory_space=pltpu.SMEM), hbm, hbm),
            scratch_shapes=[
                v((NUM_DEV, TOK, DIM), BF16),
                v((NCHUNK, DIM, CHUNK), BF16),
                v((NCHUNK, CHUNK, DIM), BF16),
                v((DIM, HID), BF16),
                v((HID, DIM), BF16),
                v((HID, DIM), BF16),
                v((ROWS, CHUNK), BF16),
                v((ROWS, CHUNK), BF16),
                v((TOK, DIM), F32),
                v((HEAD_ROWS, DIM), F32),
                v((TASKS * CLASSES, DIM, 128), F32),
                v((HEAD_ROWS, TOK), F32),
                v((NUM_DEV, HEAD_ROWS, TOK), BF16),
                v((2, TASKS, 8, TOK), F32),
                v((HID, TOK), BF16),
                v((HID, TOK), BF16),
                v((HID, TOK), F32),
                v((HID, TOK), F32),
                v((DIM, TOK), BF16),
                v((DIM, TOK), BF16),
                v((HID, TOK), BF16),
                v((HID, TOK), BF16),
                v((TASKS, HID, DIM), F32),
                v((TASKS, HID, DIM), F32),
                v((NUM_DEV, 8, 128), F32),
                v((8, DIM), F32),
                v((NUM_DEV, 16, 128), F32),
                v((DIM, HID), F32),
                v((NUM_DEV, FEAT, HID), F32),
                v((flat, 128), F32),
                v((flat, 128), F32),
                sem, sem, sem, sem, sem, sem, sem, sem, sem, sem,
                pltpu.SemaphoreType.DMA((3 + 2 * NCHUNK,)),
            ],
            compiler_params=pltpu.CompilerParams(collective_id=0, has_side_effects=True, vmem_limit_bytes=66_000_000),
            name="trunk",
        )(x_loc, w_in, w_out, heads.transpose(2, 0, 1), lab_loc, mask_loc)
        return alpha, out1.reshape(-1), out2.reshape(-1)

    return jax.shard_map(local_step, mesh=mesh, in_specs=(P("data", None), P(), P(), P(), P(None, "data"), P(None, "data")), out_specs=(P(), P("data"), P("data")), check_vma=False)
```

```python
import jax
import jax.numpy as jnp
from jax import lax
from jax.experimental import pallas as pl
from jax.experimental.pallas import tpu as pltpu
from jax.sharding import PartitionSpec as P

SOLVER_STEPS = 20
MESH = pl.DeviceIdType.MESH
F32, BF16 = jnp.float32, jnp.bfloat16
NUM_DEV = 8
TASKS = 4
CLASSES = 3
TOK = 1024
DIM = 768
HIDDEN = 3072
HID = HIDDEN // NUM_DEV
FEAT = DIM // NUM_DEV
HEAD_ROWS = 32
CHUNK = 768
ROWS = 512
NCHUNK = HIDDEN // CHUNK
QUARTER = TOK // TASKS
PAIRS = [(t, s) for t in range(TASKS) for s in range(t, TASKS)]
GELU_C = 0.7978845608028654
GELU_K = 0.044715


def dot_nn(a, b):
    return lax.dot_general(a, b, (((1,), (0,)), ((), ())), preferred_element_type=F32)


def dot_nt(a, b):
    return lax.dot_general(a, b, (((1,), (1,)), ((), ())), preferred_element_type=F32)


def lanes(row, width):
    return jnp.concatenate([row] * (width // row.shape[1]), axis=1)


def gelu_parts(p):
    a = (GELU_C * GELU_K) * (p * p)
    th = jnp.tanh(p * (a + GELU_C))
    return a, th, 0.5 + 0.5 * th


def gelu_value(p):
    return p * gelu_parts(p)[2]


def gelu_both(p):
    a, th, cdf = gelu_parts(p)
    slope = cdf + ((1.0 - th * th) * p) * (1.5 * a + 0.5 * GELU_C)
    return p * cdf, slope


def kernel(x_hbm, w_in_hbm, w_out_hbm, head_ref, lab_ref, mask_ref, alpha_ref, out1_hbm, out2_hbm,
           xs, w1, w2, w1j, w1t, w2j, abuf0, abuf1, zacc, hrow, hbc, ef, es, ecur, act0, act1, slope0, slope1,
           dz0, dz1, q0, q1, acc1, acc2, cnt, inv, gram, gsend, grecv, stage1, stage2,
           x_send, x_recv, e_send, e_recv, c_send, c_recv, g_send, g_recv, o_send, o_recv, l_sem):
    me = lax.axis_index("data")
    core = lax.rem(me, 2)
    cx = lax.rem(lax.div(me, 2), 2)
    cy = lax.div(me, 4)

    def flip(v, b):
        return v + b - 2 * v * b

    def peer(slot):
        hop = slot // 2
        first, second = (1 if hop in (1, 3) else 0), (1 if hop in (2, 3) else 0)
        bx = first * (1 - core) + second * core
        by = first * core + second * (1 - core)
        bc = slot % 2
        return flip(cx, bx) * 2 + flip(cy, by) * 4 + flip(core, jnp.int32(bc))

    def remote(src, dst, send, recv, dev):
        return pltpu.make_async_remote_copy(src_ref=src, dst_ref=dst, send_sem=send, recv_sem=recv, device_id=(dev,), device_id_type=MESH)

    def x_copy(src_slot, dst_slot):
        dev = {1: 1, 2: 2, 4: 4, 3: 1, 5: 1, 6: 4, 7: 1}[dst_slot]
        return remote(xs.at[src_slot], xs.at[dst_slot], x_send.at[dst_slot], x_recv.at[dst_slot], peer(dev))

    def e_copy(slot):
        return remote(es.at[0], es.at[slot], e_send.at[slot], e_recv.at[slot], peer(slot))

    def c_copy(slot):
        return remote(cnt.at[0], cnt.at[slot], c_send.at[slot], c_recv.at[slot], peer(slot))

    def local(src, dst, i):
        return pltpu.make_async_copy(src, dst, l_sem.at[i])

    def load_w1(i):
        return local(w_in_hbm.at[:, pl.ds(pl.multiple_of(CHUNK * i, CHUNK), CHUNK)], w1.at[i], 3 + i)

    def load_w2(i):
        return local(w_out_hbm.at[pl.ds(pl.multiple_of(CHUNK * i, CHUNK), CHUNK), :], w2.at[i], 3 + NCHUNK + i)

    load_x = local(x_hbm, xs.at[0], 0)
    load_w1j = local(w_in_hbm.at[:, pl.ds(pl.multiple_of(me * HID, HID), HID)], w1j, 1)
    load_w2j = local(w_out_hbm.at[pl.ds(pl.multiple_of(me * HID, HID), HID), :], w2j, 2)
    load_x.start()
    load_w1j.start()
    for i in range(NCHUNK):
        load_w1(i).start()
        load_w2(i).start()
    load_w2j.start()

    barrier = pltpu.get_barrier_semaphore()
    for s in range(1, NUM_DEV):
        pl.semaphore_signal(barrier, inc=1, device_id=(peer(s),), device_id_type=MESH)

    counts = jnp.sum(mask_ref[...].astype(F32), axis=1, keepdims=True)
    cnt[0, 0:TASKS, :] = jnp.broadcast_to(counts, (TASKS, 128))
    cnt[0, TASKS:8, :] = jnp.zeros((8 - TASKS, 128), F32)
    hrow[...] = jnp.zeros_like(hrow)
    for c in range(CLASSES):
        hrow[8 * c:8 * c + TASKS, :] = head_ref[c].astype(F32)
    head = hrow[...].astype(BF16)

    pl.semaphore_wait(barrier, NUM_DEV - 1)
    load_x.wait()
    x_copy(0, 1).start()
    x_copy(0, 2).start()
    for s in range(1, NUM_DEV):
        c_copy(s).start()

    block = lax.div(lax.broadcasted_iota(jnp.int32, (HEAD_ROWS, TASKS * CLASSES * 128), 1), 128)
    pick = lax.rem(block, CLASSES) * 8 + lax.div(block, CLASSES)
    ones = (lax.broadcasted_iota(jnp.int32, block.shape, 0) == pick).astype(F32).astype(BF16)
    wide = dot_nn(hrow[...].T.astype(BF16), ones)
    for k in range(TASKS * CLASSES):
        hbc[k] = wide[:, 128 * k:128 * k + 128]
    load_w1j.wait()
    w1t[...] = w1j[...].astype(F32).T.astype(BF16)

    abuf1[...] = jnp.zeros_like(abuf1)
    zacc[...] = xs[0].astype(F32)
    half0, half1 = slice(0, ROWS), slice(ROWS, TOK)

    def forward(h, carry):
        load_w1(h).wait()
        load_w2(h).wait()
        acc1[h] = jnp.zeros((HID, DIM), F32)
        acc2[h] = jnp.zeros((HID, DIM), F32)
        abuf0[...] = gelu_value(dot_nn(xs[0, half0, :], w1[h])).astype(BF16)
        zacc[half1, :] += dot_nn(abuf1[...], w2[jnp.maximum(h - 1, 0)])
        abuf1[...] = gelu_value(dot_nn(xs[0, half1, :], w1[h])).astype(BF16)
        zacc[half0, :] += dot_nn(abuf0[...], w2[h])
        return carry

    lax.fori_loop(0, NCHUNK, forward, 0)
    zacc[half1, :] += dot_nn(abuf1[...], w2[NCHUNK - 1])

    acts, slopes, dzs, qs = (act0, act1), (slope0, slope1), (dz0, dz1), (q0, q1)

    def preact(slot, part, quarter):
        r = pl.ds(pl.multiple_of(quarter * QUARTER, QUARTER), QUARTER)
        a, sl = gelu_both(dot_nt(w1t[...], xs[slot, r, :]))
        acts[part][:, r] = a.astype(BF16)
        slopes[part][:, r] = sl

    for r in range(TOK // ROWS):
        cols = slice(r * ROWS, (r + 1) * ROWS)
        logits = dot_nt(head, zacc[cols, :].astype(BF16))
        l = [logits[8 * c:8 * c + TASKS] for c in range(CLASSES)]
        top = jnp.maximum(jnp.maximum(l[0], l[1]), l[2])
        ex = [jnp.exp(v - top) for v in l]
        total = ex[0] + ex[1] + ex[2]
        lab = lab_ref[:, cols]
        m = mask_ref[:, cols].astype(F32)
        for c in range(CLASSES):
            err = m * (ex[c] / total - (lab == c).astype(F32))
            for t in range(TASKS):
                ef[8 * t + c:8 * t + c + 1, cols] = err[t:t + 1]
    for t in range(TASKS):
        ef[8 * t + CLASSES:8 * t + 8, :] = jnp.zeros((8 - CLASSES, TOK), F32)
    es[0] = ef[...].astype(BF16)
    for t in range(TASKS):
        ecur[0, t] = es[0, 8 * t:8 * t + 8, :].astype(F32)

    for k in range(TOK // QUARTER):
        preact(0, 0, k)

    def make_dz(dst, part, t):
        e = ecur[part, t]
        rows = [jnp.broadcast_to(e[c:c + 1, :], (16, TOK)) for c in range(CLASSES)]
        for k in range(DIM // 16):
            f = slice(16 * k, 16 * k + 16)
            h = [lanes(hbc[CLASSES * t + c, f, :], TOK) for c in range(CLASSES)]
            dst[f, :] = (h[0] * rows[0] + h[1] * rows[1] + h[2] * rows[2]).astype(BF16)

    for s in range(1, NUM_DEV):
        e_copy(s).start()
    make_dz(dz0, 0, 0)
    load_w2j.wait()
    total_cnt = cnt[0]
    for s in range(1, NUM_DEV):
        c_copy(s).wait_recv()
        total_cnt = total_cnt + cnt[s]
    inv[...] = lanes(1.0 / jnp.maximum(total_cnt, 1.0), DIM)
    x_copy(0, 2).wait_send()
    x_copy(0, 4).start()

    def tokens_ready(s):
        for k in range(1, NUM_DEV):
            @pl.when(s == k - 1)
            def _():
                x_copy(0, k).wait_recv()
                if k == 2:
                    x_copy(2, 6).start()
                if k in (2, 4, 6):
                    x_copy(k, k + 1).start()

    def errors_ready(s, part):
        for k in range(1, NUM_DEV):
            @pl.when(s == k - 1)
            def _():
                e_copy(k).wait_recv()
                for t in range(TASKS):
                    ecur[part, t] = es[k, 8 * t:8 * t + 8, :].astype(F32)

    def run_task(s, part, t, j, next_part, next_t):
        nxt = jnp.minimum(s + 1, NUM_DEV - 1)
        scale = inv[pl.ds(t, 1), :]
        qs[j][...] = (dot_nn(w2j[...], dzs[j][...]) * slopes[part][...]).astype(BF16)
        acc2[t] += (dot_nt(acts[part][...], dzs[j][...]) * scale).astype(BF16).astype(F32)
        make_dz(dzs[1 - j], next_part, next_t)
        preact(nxt, 1 - part, t)
        acc1[t] += (dot_nn(qs[j][...], xs[s]) * scale).astype(BF16).astype(F32)

    def shard_pair(sp, carry):
        for part in range(2):
            s = 2 * sp + part
            tokens_ready(s)

            def task_pair(tp, c):
                @pl.when(tp == 1)
                def _():
                    errors_ready(s, 1 - part)
                run_task(s, part, 2 * tp, 0, part, 2 * tp + 1)
                wrap = lax.div(2 * tp + 2, TASKS)
                run_task(s, part, 2 * tp + 1, 1, part + wrap * (1 - 2 * part), 2 * tp + 2 - TASKS * wrap)
                return c

            lax.fori_loop(0, TASKS // 2, task_pair, 0)
        return carry

    lax.fori_loop(0, NUM_DEV // 2, shard_pair, 0)

    def gram_rows(i, sums):
        r = pl.ds(pl.multiple_of(i * 8, 8), 8)
        out = list(sums)
        for acc in (acc1, acc2):
            for c in range(DIM // 128):
                g = [acc[t, r, 128 * c:128 * c + 128] for t in range(TASKS)]
                for k, (t, u) in enumerate(PAIRS):
                    out[k] = out[k] + g[t] * g[u]
        return tuple(out)

    sums = lax.fori_loop(0, HID // 8, gram_rows, tuple(jnp.zeros((8, 128), F32) for _ in PAIRS))
    for k in range(len(PAIRS)):
        gram[me, k:k + 1, :] = jnp.broadcast_to(jnp.sum(sums[k]), (1, 128))
    gram[me, len(PAIRS):16, :] = jnp.zeros((16 - len(PAIRS), 128), F32)

    def gram_copy(s, block):
        return remote(gram.at[block], gram.at[block], g_send.at[s], g_recv.at[s], peer(s))

    for s in range(1, NUM_DEV):
        gram_copy(s, me).start()
    for s in range(1, NUM_DEV):
        gram_copy(s, me).wait_recv()
    gram_sum = gram[0]
    for d in range(1, NUM_DEV):
        gram_sum = gram_sum + gram[d]
    m = {}
    for k, (t, u) in enumerate(PAIRS):
        m[t, u] = m[u, t] = gram_sum[k:k + 1, :]
    step_scale = (m[0, 0] + m[1, 1] + m[2, 2] + m[3, 3]) / TASKS
    al = [jnp.full((1, 128), 1.0 / TASKS, F32) for _ in range(TASKS)]
    for _ in range(SOLVER_STEPS):
        raised = []
        for t in range(TASKS):
            pull = (m[t, 0] * al[0] + m[t, 1] * al[1]) + (m[t, 2] * al[2] + m[t, 3] * al[3])
            raised.append(al[t] * jnp.exp(-pull / step_scale))
        norm = (raised[0] + raised[1]) + (raised[2] + raised[3])
        al = [r / norm for r in raised]
    for t in range(TASKS):
        alpha_ref[t] = jnp.max(al[t])

    for c in range(DIM // 128):
        cols = slice(128 * c, 128 * c + 128)
        comb = al[0] * acc1[0, :, cols]
        for t in range(1, TASKS):
            comb = comb + al[t] * acc1[t, :, cols]
        gsend[cols, :] = comb.T

    def o_copy(s):
        dev = peer(s)
        rows = pl.ds(pl.multiple_of(dev * FEAT, FEAT), FEAT)
        return remote(gsend.at[rows, :], grecv.at[s], o_send.at[s], o_recv.at[s], dev)

    order = (6, 7, 4, 5, 2, 3, 1)
    for s in order:
        o_copy(s).start()

    for c in range(DIM // 128):
        cols = slice(128 * c, 128 * c + 128)
        comb = al[0] * acc2[0, :, cols]
        for t in range(1, TASKS):
            comb = comb + al[t] * acc2[t, :, cols]
        stage2[pl.ds(c, HID, stride=DIM // 128), :] = comb
    store2 = local(stage2, out2_hbm, 0)
    store2.start()

    per = HID // 128

    def place(dev, block):
        for b in range(per):
            stage1[pl.ds(dev * per + b, FEAT, stride=HIDDEN // 128), :] = block[:, 128 * b:128 * b + 128]

    def owner(slot):
        hop = slot // 2
        first, second = (1 if hop in (1, 3) else 0), (1 if hop in (2, 3) else 0)
        oc = flip(core, jnp.int32(slot % 2))
        bx = first * (1 - oc) + second * oc
        by = first * oc + second * (1 - oc)
        return flip(cx, bx) * 2 + flip(cy, by) * 4 + oc

    place(me, gsend[pl.ds(pl.multiple_of(me * FEAT, FEAT), FEAT), :])
    for s in (1, 2, 3, 4, 5, 6, 7):
        o_copy(s).wait_recv()
        place(owner(s), grecv[s])
    store1 = local(stage1, out1_hbm, 1)
    store1.start()

    x_copy(0, 1).wait_send()
    for k in (4, 3, 5, 6, 7):
        x_copy(0, k).wait_send()
    for s in range(1, NUM_DEV):
        e_copy(s).wait_send()
        c_copy(s).wait_send()
        gram_copy(s, me).wait_send()
        o_copy(s).wait_send()
    store2.wait()
    store1.wait()


def solution(mesh):
    def local_step(x_loc, w_in, w_out, heads, lab_loc, mask_loc):
        hbm = pl.BlockSpec(memory_space=pl.ANY)
        vmem = pl.BlockSpec(memory_space=pltpu.VMEM)
        sem = pltpu.SemaphoreType.DMA((NUM_DEV,))
        v = pltpu.VMEM
        flat = DIM * HIDDEN // NUM_DEV // 128
        alpha, out1, out2 = pl.pallas_call(
            kernel,
            out_shape=(
                jax.ShapeDtypeStruct((TASKS,), F32),
                jax.ShapeDtypeStruct((flat, 128), F32),
                jax.ShapeDtypeStruct((flat, 128), F32),
            ),
            in_specs=[hbm, hbm, hbm, vmem, vmem, vmem],
            out_specs=(pl.BlockSpec(memory_space=pltpu.SMEM), hbm, hbm),
            scratch_shapes=[
                v((NUM_DEV, TOK, DIM), BF16),
                v((NCHUNK, DIM, CHUNK), BF16),
                v((NCHUNK, CHUNK, DIM), BF16),
                v((DIM, HID), BF16),
                v((HID, DIM), BF16),
                v((HID, DIM), BF16),
                v((ROWS, CHUNK), BF16),
                v((ROWS, CHUNK), BF16),
                v((TOK, DIM), F32),
                v((HEAD_ROWS, DIM), F32),
                v((TASKS * CLASSES, DIM, 128), F32),
                v((HEAD_ROWS, TOK), F32),
                v((NUM_DEV, HEAD_ROWS, TOK), BF16),
                v((2, TASKS, 8, TOK), F32),
                v((HID, TOK), BF16),
                v((HID, TOK), BF16),
                v((HID, TOK), F32),
                v((HID, TOK), F32),
                v((DIM, TOK), BF16),
                v((DIM, TOK), BF16),
                v((HID, TOK), BF16),
                v((HID, TOK), BF16),
                v((TASKS, HID, DIM), F32),
                v((TASKS, HID, DIM), F32),
                v((NUM_DEV, 8, 128), F32),
                v((8, DIM), F32),
                v((NUM_DEV, 16, 128), F32),
                v((DIM, HID), F32),
                v((NUM_DEV, FEAT, HID), F32),
                v((flat, 128), F32),
                v((flat, 128), F32),
                sem, sem, sem, sem, sem, sem, sem, sem, sem, sem,
                pltpu.SemaphoreType.DMA((3 + 2 * NCHUNK,)),
            ],
            compiler_params=pltpu.CompilerParams(collective_id=0, has_side_effects=True, vmem_limit_bytes=66_000_000),
            name="trunk",
        )(x_loc, w_in, w_out, heads.transpose(2, 0, 1), lab_loc, mask_loc)
        return alpha, out1.reshape(-1), out2.reshape(-1)

    return jax.shard_map(local_step, mesh=mesh, in_specs=(P("data", None), P(), P(), P(), P(None, "data"), P(None, "data")), out_specs=(P(), P("data"), P("data")), check_vma=False)
```

```python
import jax
import jax.numpy as jnp
from jax import lax
from jax.experimental import pallas as pl
from jax.experimental.pallas import tpu as pltpu
from jax.sharding import PartitionSpec as P

SOLVER_STEPS = 20
MESH = pl.DeviceIdType.MESH
F32, BF16 = jnp.float32, jnp.bfloat16
NUM_DEV = 8
TASKS = 4
CLASSES = 3
TOK = 1024
DIM = 768
HIDDEN = 3072
HID = HIDDEN // NUM_DEV
FEAT = DIM // NUM_DEV
HEAD_ROWS = 32
CHUNK = 768
ROWS = 512
NCHUNK = HIDDEN // CHUNK
QUARTER = TOK // TASKS
PAIRS = [(t, s) for t in range(TASKS) for s in range(t, TASKS)]
GELU_C = 0.7978845608028654
GELU_K = 0.044715


def dot_nn(a, b):
    return lax.dot_general(a, b, (((1,), (0,)), ((), ())), preferred_element_type=F32)


def dot_nt(a, b):
    return lax.dot_general(a, b, (((1,), (1,)), ((), ())), preferred_element_type=F32)


def lanes(row, width):
    return jnp.concatenate([row] * (width // row.shape[1]), axis=1)


def gelu_parts(p):
    a = (GELU_C * GELU_K) * (p * p)
    th = jnp.tanh(p * (a + GELU_C))
    return a, th, 0.5 + 0.5 * th


def gelu_value(p):
    return p * gelu_parts(p)[2]


def gelu_both(p):
    a, th, cdf = gelu_parts(p)
    slope = cdf + ((1.0 - th * th) * p) * (1.5 * a + 0.5 * GELU_C)
    return p * cdf, slope


def kernel(x_hbm, w_in_hbm, w_out_hbm, head_ref, lab_ref, mask_ref, alpha_ref, gx_hbm, out2_hbm,
           xs, w1, w2, w1j, w1t, w2j, abuf0, abuf1, zacc, hrow, hbc, ef, es, ecur, act0, act1, slope0, slope1,
           dz0, dz1, q0, q1, acc1, acc2, cnt, inv, gram, gsend, stage2,
           x_send, x_recv, e_send, e_recv, c_send, c_recv, g_send, g_recv, o_send, o_recv, l_sem):
    me = lax.axis_index("data")
    core = lax.rem(me, 2)
    cx = lax.rem(lax.div(me, 2), 2)
    cy = lax.div(me, 4)

    def flip(v, b):
        return v + b - 2 * v * b

    def peer(slot):
        hop = slot // 2
        first, second = (1 if hop in (1, 3) else 0), (1 if hop in (2, 3) else 0)
        bx = first * (1 - core) + second * core
        by = first * core + second * (1 - core)
        bc = slot % 2
        return flip(cx, bx) * 2 + flip(cy, by) * 4 + flip(core, jnp.int32(bc))

    def remote(src, dst, send, recv, dev):
        return pltpu.make_async_remote_copy(src_ref=src, dst_ref=dst, send_sem=send, recv_sem=recv, device_id=(dev,), device_id_type=MESH)

    def x_copy(src_slot, dst_slot):
        dev = {1: 1, 2: 2, 4: 4, 3: 1, 5: 1, 6: 4, 7: 1}[dst_slot]
        return remote(xs.at[src_slot], xs.at[dst_slot], x_send.at[dst_slot], x_recv.at[dst_slot], peer(dev))

    def e_copy(slot):
        return remote(es.at[0], es.at[slot], e_send.at[slot], e_recv.at[slot], peer(slot))

    def c_copy(slot):
        return remote(cnt.at[0], cnt.at[slot], c_send.at[slot], c_recv.at[slot], peer(slot))

    def local(src, dst, i):
        return pltpu.make_async_copy(src, dst, l_sem.at[i])

    def load_w1(i):
        return local(w_in_hbm.at[:, pl.ds(pl.multiple_of(CHUNK * i, CHUNK), CHUNK)], w1.at[i], 3 + i)

    def load_w2(i):
        return local(w_out_hbm.at[pl.ds(pl.multiple_of(CHUNK * i, CHUNK), CHUNK), :], w2.at[i], 3 + NCHUNK + i)

    load_x = local(x_hbm, xs.at[0], 0)
    load_w1j = local(w_in_hbm.at[:, pl.ds(pl.multiple_of(me * HID, HID), HID)], w1j, 1)
    load_w2j = local(w_out_hbm.at[pl.ds(pl.multiple_of(me * HID, HID), HID), :], w2j, 2)
    load_x.start()
    load_w1j.start()
    for i in range(NCHUNK):
        load_w1(i).start()
        load_w2(i).start()
    load_w2j.start()

    barrier = pltpu.get_barrier_semaphore()
    for s in range(1, NUM_DEV):
        pl.semaphore_signal(barrier, inc=1, device_id=(peer(s),), device_id_type=MESH)

    counts = jnp.sum(mask_ref[...].astype(F32), axis=1, keepdims=True)
    cnt[0, 0:TASKS, :] = jnp.broadcast_to(counts, (TASKS, 128))
    cnt[0, TASKS:8, :] = jnp.zeros((8 - TASKS, 128), F32)
    hrow[...] = jnp.zeros_like(hrow)
    for c in range(CLASSES):
        hrow[8 * c:8 * c + TASKS, :] = head_ref[c].astype(F32)
    head = hrow[...].astype(BF16)

    pl.semaphore_wait(barrier, NUM_DEV - 1)
    load_x.wait()
    x_copy(0, 1).start()
    x_copy(0, 2).start()
    for s in range(1, NUM_DEV):
        c_copy(s).start()

    block = lax.div(lax.broadcasted_iota(jnp.int32, (HEAD_ROWS, TASKS * CLASSES * 128), 1), 128)
    pick = lax.rem(block, CLASSES) * 8 + lax.div(block, CLASSES)
    ones = (lax.broadcasted_iota(jnp.int32, block.shape, 0) == pick).astype(F32).astype(BF16)
    wide = dot_nn(hrow[...].T.astype(BF16), ones)
    for k in range(TASKS * CLASSES):
        hbc[k] = wide[:, 128 * k:128 * k + 128]
    load_w1j.wait()
    w1t[...] = w1j[...].astype(F32).T.astype(BF16)

    abuf1[...] = jnp.zeros_like(abuf1)
    zacc[...] = xs[0].astype(F32)
    half0, half1 = slice(0, ROWS), slice(ROWS, TOK)

    acts, slopes, dzs, qs = (act0, act1), (slope0, slope1), (dz0, dz1), (q0, q1)

    def preact(slot, part, quarter):
        r = pl.ds(pl.multiple_of(quarter * QUARTER, QUARTER), QUARTER)
        a, sl = gelu_both(dot_nt(w1t[...], xs[slot, r, :]))
        acts[part][:, r] = a.astype(BF16)
        slopes[part][:, r] = sl

    def forward(h, carry):
        load_w1(h).wait()
        load_w2(h).wait()
        acc1[h] = jnp.zeros((HID, DIM), F32)
        acc2[h] = jnp.zeros((HID, DIM), F32)
        abuf0[...] = gelu_value(dot_nn(xs[0, half0, :], w1[h])).astype(BF16)
        zacc[half1, :] += dot_nn(abuf1[...], w2[jnp.maximum(h - 1, 0)])
        abuf1[...] = gelu_value(dot_nn(xs[0, half1, :], w1[h])).astype(BF16)
        zacc[half0, :] += dot_nn(abuf0[...], w2[h])
        preact(0, 0, h)
        return carry

    lax.fori_loop(0, NCHUNK, forward, 0)
    zacc[half1, :] += dot_nn(abuf1[...], w2[NCHUNK - 1])

    for r in range(TOK // ROWS):
        cols = slice(r * ROWS, (r + 1) * ROWS)
        logits = dot_nt(head, zacc[cols, :].astype(BF16))
        l = [logits[8 * c:8 * c + TASKS] for c in range(CLASSES)]
        top = jnp.maximum(jnp.maximum(l[0], l[1]), l[2])
        ex = [jnp.exp(v - top) for v in l]
        total = ex[0] + ex[1] + ex[2]
        lab = lab_ref[:, cols]
        m = mask_ref[:, cols].astype(F32)
        for c in range(CLASSES):
            err = m * (ex[c] / total - (lab == c).astype(F32))
            for t in range(TASKS):
                ef[8 * t + c:8 * t + c + 1, cols] = err[t:t + 1]
    for t in range(TASKS):
        ef[8 * t + CLASSES:8 * t + 8, :] = jnp.zeros((8 - CLASSES, TOK), F32)
    es[0] = ef[...].astype(BF16)
    for t in range(TASKS):
        ecur[0, t] = es[0, 8 * t:8 * t + 8, :].astype(F32)

    def make_dz(dst, part, t):
        e = ecur[part, t]
        rows = [jnp.broadcast_to(e[c:c + 1, :], (8, TOK)) for c in range(CLASSES)]
        for k in range(DIM // 8):
            f = slice(8 * k, 8 * k + 8)
            h = [lanes(hbc[CLASSES * t + c, f, :], TOK) for c in range(CLASSES)]
            dst[f, :] = (h[0] * rows[0] + h[1] * rows[1] + h[2] * rows[2]).astype(BF16)

    for s in range(1, NUM_DEV):
        e_copy(s).start()
    make_dz(dz0, 0, 0)
    load_w2j.wait()
    total_cnt = cnt[0]
    for s in range(1, NUM_DEV):
        c_copy(s).wait_recv()
        total_cnt = total_cnt + cnt[s]
    inv[...] = lanes(1.0 / jnp.maximum(total_cnt, 1.0), DIM)
    x_copy(0, 2).wait_send()
    x_copy(0, 4).start()

    def tokens_ready(s):
        for k in range(1, NUM_DEV):
            @pl.when(s == k - 1)
            def _():
                x_copy(0, k).wait_recv()
                if k == 2:
                    x_copy(2, 6).start()
                if k in (2, 4, 6):
                    x_copy(k, k + 1).start()

    def errors_ready(s, part):
        for k in range(1, NUM_DEV):
            @pl.when(s == k - 1)
            def _():
                e_copy(k).wait_recv()
                for t in range(TASKS):
                    ecur[part, t] = es[k, 8 * t:8 * t + 8, :].astype(F32)

    def run_task(s, part, t, j, next_part, next_t):
        nxt = jnp.minimum(s + 1, NUM_DEV - 1)
        scale = inv[pl.ds(t, 1), :]
        qs[j][...] = (dot_nn(w2j[...], dzs[j][...]) * slopes[part][...]).astype(BF16)
        acc2[t] += (dot_nt(acts[part][...], dzs[j][...]) * scale).astype(BF16).astype(F32)
        make_dz(dzs[1 - j], next_part, next_t)
        preact(nxt, 1 - part, t)
        acc1[t] += (dot_nn(qs[j][...], xs[s]) * scale).astype(BF16).astype(F32)

    def shard_pair(sp, carry):
        for part in range(2):
            s = 2 * sp + part
            tokens_ready(s)

            def task_pair(tp, c):
                @pl.when(tp == 1)
                def _():
                    errors_ready(s, 1 - part)
                run_task(s, part, 2 * tp, 0, part, 2 * tp + 1)
                wrap = lax.div(2 * tp + 2, TASKS)
                run_task(s, part, 2 * tp + 1, 1, part + wrap * (1 - 2 * part), 2 * tp + 2 - TASKS * wrap)
                return c

            lax.fori_loop(0, TASKS // 2, task_pair, 0)
        return carry

    lax.fori_loop(0, NUM_DEV // 2, shard_pair, 0)

    def gram_rows(i, sums):
        r = pl.ds(pl.multiple_of(i * 8, 8), 8)
        out = list(sums)
        for acc in (acc1, acc2):
            for c in range(DIM // 128):
                g = [acc[t, r, 128 * c:128 * c + 128] for t in range(TASKS)]
                for k, (t, u) in enumerate(PAIRS):
                    out[k] = out[k] + g[t] * g[u]
        return tuple(out)

    sums = lax.fori_loop(0, HID // 8, gram_rows, tuple(jnp.zeros((8, 128), F32) for _ in PAIRS))
    for k in range(len(PAIRS)):
        gram[me, k:k + 1, :] = jnp.broadcast_to(jnp.sum(sums[k]), (1, 128))
    gram[me, len(PAIRS):16, :] = jnp.zeros((16 - len(PAIRS), 128), F32)

    def gram_copy(s, block):
        return remote(gram.at[block], gram.at[block], g_send.at[s], g_recv.at[s], peer(s))

    for s in range(1, NUM_DEV):
        gram_copy(s, me).start()
    for s in range(1, NUM_DEV):
        gram_copy(s, me).wait_recv()
    gram_sum = gram[0]
    for d in range(1, NUM_DEV):
        gram_sum = gram_sum + gram[d]
    m = {}
    for k, (t, u) in enumerate(PAIRS):
        m[t, u] = m[u, t] = gram_sum[k:k + 1, :]
    step_scale = (m[0, 0] + m[1, 1] + m[2, 2] + m[3, 3]) / TASKS
    al = [jnp.full((1, 128), 1.0 / TASKS, F32) for _ in range(TASKS)]
    for _ in range(SOLVER_STEPS):
        raised = []
        for t in range(TASKS):
            pull = (m[t, 0] * al[0] + m[t, 1] * al[1]) + (m[t, 2] * al[2] + m[t, 3] * al[3])
            raised.append(al[t] * jnp.exp(-pull / step_scale))
        norm = (raised[0] + raised[1]) + (raised[2] + raised[3])
        al = [r / norm for r in raised]
    for t in range(TASKS):
        alpha_ref[t] = jnp.max(al[t])

    for c in range(DIM // 128):
        cols = slice(128 * c, 128 * c + 128)
        comb = al[0] * acc1[0, :, cols]
        for t in range(1, TASKS):
            comb = comb + al[t] * acc1[t, :, cols]
        gsend[cols, :] = comb.T

    def o_copy(s):
        dev = peer(s)
        rows = pl.ds(pl.multiple_of(dev * FEAT, FEAT), FEAT)
        return remote(gsend.at[rows, :], gx_hbm.at[me], o_send.at[s], o_recv.at[s], dev)

    order = (6, 7, 4, 5, 2, 3, 1)
    for s in order:
        o_copy(s).start()

    for c in range(DIM // 128):
        cols = slice(128 * c, 128 * c + 128)
        comb = al[0] * acc2[0, :, cols]
        for t in range(1, TASKS):
            comb = comb + al[t] * acc2[t, :, cols]
        stage2[pl.ds(c, HID, stride=DIM // 128), :] = comb
    store2 = local(stage2, out2_hbm, 0)
    store2.start()

    keep = local(gsend.at[pl.ds(pl.multiple_of(me * FEAT, FEAT), FEAT), :], gx_hbm.at[me], 1)
    keep.start()
    for s in range(1, NUM_DEV):
        o_copy(s).wait_recv()

    x_copy(0, 1).wait_send()
    for k in (4, 3, 5, 6, 7):
        x_copy(0, k).wait_send()
    for s in range(1, NUM_DEV):
        e_copy(s).wait_send()
        c_copy(s).wait_send()
        gram_copy(s, me).wait_send()
        o_copy(s).wait_send()
    store2.wait()
    keep.wait()


PER = HID // 128
FLAT = DIM * HIDDEN // NUM_DEV // 128
HALF = FEAT // 2


def finish(alpha_in, gx_hbm, g2_hbm, alpha_ref, out1_hbm, out2_hbm, blocks, stage1, stage2, in_sem, out_sem):
    loads = [pltpu.make_async_copy(gx_hbm.at[d], blocks.at[d], in_sem.at[d]) for d in range(NUM_DEV)]
    load2 = pltpu.make_async_copy(g2_hbm, stage2, in_sem.at[NUM_DEV])
    for c in loads:
        c.start()
    load2.start()
    for t in range(TASKS):
        alpha_ref[t] = alpha_in[t]
    for c in loads:
        c.wait()
    stores = []
    for h in range(2):
        for d in range(NUM_DEV):
            for b in range(PER):
                first = h * HALF * (HIDDEN // 128) + d * PER + b
                stage1[pl.ds(first, HALF, stride=HIDDEN // 128), :] = blocks[d, h * HALF:h * HALF + HALF, 128 * b:128 * b + 128]
        rows = pl.ds(h * FLAT // 2, FLAT // 2)
        stores.append(pltpu.make_async_copy(stage1.at[rows, :], out1_hbm.at[rows, :], out_sem.at[h]))
        stores[-1].start()
        if h == 0:
            load2.wait()
            stores.append(pltpu.make_async_copy(stage2, out2_hbm, out_sem.at[2]))
            stores[-1].start()
    for c in stores:
        c.wait()


def solution(mesh):
    def local_step(x_loc, w_in, w_out, heads, lab_loc, mask_loc):
        hbm = pl.BlockSpec(memory_space=pl.ANY)
        vmem = pl.BlockSpec(memory_space=pltpu.VMEM)
        sem = pltpu.SemaphoreType.DMA((NUM_DEV,))
        v = pltpu.VMEM
        alpha, gx, g2 = pl.pallas_call(
            kernel,
            out_shape=(
                jax.ShapeDtypeStruct((TASKS,), F32),
                jax.ShapeDtypeStruct((NUM_DEV, FEAT, HID), F32),
                jax.ShapeDtypeStruct((FLAT, 128), F32),
            ),
            in_specs=[hbm, hbm, hbm, vmem, vmem, vmem],
            out_specs=(pl.BlockSpec(memory_space=pltpu.SMEM), hbm, hbm),
            scratch_shapes=[
                v((NUM_DEV, TOK, DIM), BF16),
                v((NCHUNK, DIM, CHUNK), BF16),
                v((NCHUNK, CHUNK, DIM), BF16),
                v((DIM, HID), BF16),
                v((HID, DIM), BF16),
                v((HID, DIM), BF16),
                v((ROWS, CHUNK), BF16),
                v((ROWS, CHUNK), BF16),
                v((TOK, DIM), F32),
                v((HEAD_ROWS, DIM), F32),
                v((TASKS * CLASSES, DIM, 128), F32),
                v((HEAD_ROWS, TOK), F32),
                v((NUM_DEV, HEAD_ROWS, TOK), BF16),
                v((2, TASKS, 8, TOK), F32),
                v((HID, TOK), BF16),
                v((HID, TOK), BF16),
                v((HID, TOK), F32),
                v((HID, TOK), F32),
                v((DIM, TOK), BF16),
                v((DIM, TOK), BF16),
                v((HID, TOK), BF16),
                v((HID, TOK), BF16),
                v((TASKS, HID, DIM), F32),
                v((TASKS, HID, DIM), F32),
                v((NUM_DEV, 8, 128), F32),
                v((8, DIM), F32),
                v((NUM_DEV, 16, 128), F32),
                v((DIM, HID), F32),
                v((FLAT, 128), F32),
                sem, sem, sem, sem, sem, sem, sem, sem, sem, sem,
                pltpu.SemaphoreType.DMA((3 + 2 * NCHUNK,)),
            ],
            compiler_params=pltpu.CompilerParams(collective_id=0, has_side_effects=True, vmem_limit_bytes=66_000_000),
            name="trunk",
        )(x_loc, w_in, w_out, heads.transpose(2, 0, 1), lab_loc, mask_loc)
        smem = pl.BlockSpec(memory_space=pltpu.SMEM)
        alpha, out1, out2 = pl.pallas_call(
            finish,
            out_shape=(
                jax.ShapeDtypeStruct((TASKS,), F32),
                jax.ShapeDtypeStruct((FLAT, 128), F32),
                jax.ShapeDtypeStruct((FLAT, 128), F32),
            ),
            in_specs=[smem, hbm, hbm],
            out_specs=(smem, hbm, hbm),
            scratch_shapes=[
                v((NUM_DEV, FEAT, HID), F32),
                v((FLAT, 128), F32),
                v((FLAT, 128), F32),
                pltpu.SemaphoreType.DMA((NUM_DEV + 1,)),
                pltpu.SemaphoreType.DMA((3,)),
            ],
            name="finish",
        )(alpha, gx, g2)
        return alpha, out1.reshape(-1), out2.reshape(-1)

    return jax.shard_map(local_step, mesh=mesh, in_specs=(P("data", None), P(), P(), P(), P(None, "data"), P(None, "data")), out_specs=(P(), P("data"), P("data")), check_vma=False)
```

```python
import jax
import jax.numpy as jnp
from jax import lax
from jax.experimental import pallas as pl
from jax.experimental.pallas import tpu as pltpu
from jax.sharding import PartitionSpec as P

SOLVER_STEPS = 20
MESH = pl.DeviceIdType.MESH
F32, BF16 = jnp.float32, jnp.bfloat16
NUM_DEV = 8
TASKS = 4
CLASSES = 3
TOK = 1024
DIM = 768
HIDDEN = 3072
HID = HIDDEN // NUM_DEV
FEAT = DIM // NUM_DEV
HEAD_ROWS = 32
CHUNK = 768
ROWS = 512
NCHUNK = HIDDEN // CHUNK
QUARTER = TOK // TASKS
PAIRS = [(t, s) for t in range(TASKS) for s in range(t, TASKS)]
GELU_C = 0.7978845608028654
GELU_K = 0.044715


def dot_nn(a, b):
    return lax.dot_general(a, b, (((1,), (0,)), ((), ())), preferred_element_type=F32)


def dot_nt(a, b):
    return lax.dot_general(a, b, (((1,), (1,)), ((), ())), preferred_element_type=F32)


def lanes(row, width):
    return jnp.concatenate([row] * (width // row.shape[1]), axis=1)


def gelu_parts(p):
    a = (GELU_C * GELU_K) * (p * p)
    th = jnp.tanh(p * (a + GELU_C))
    return a, th, 0.5 + 0.5 * th


def gelu_value(p):
    return p * gelu_parts(p)[2]


def gelu_both(p):
    a, th, cdf = gelu_parts(p)
    slope = cdf + ((1.0 - th * th) * p) * (1.5 * a + 0.5 * GELU_C)
    return p * cdf, slope


def kernel(x_hbm, w_in_hbm, w_out_hbm, head_ref, lab_ref, mask_ref, alpha_ref, gx_hbm, out2_hbm,
           xs, w1, w2, w1j, w1t, w2j, abuf0, abuf1, zacc, hrow, hbc, ef, es, ecur, act0, act1, slope0, slope1,
           dz0, dz1, q0, q1, acc1, acc2, cnt, inv, gram, gsend, stage2,
           x_send, x_recv, e_send, e_recv, c_send, c_recv, g_send, g_recv, o_send, o_recv, l_sem):
    me = lax.axis_index("data")
    core = lax.rem(me, 2)
    cx = lax.rem(lax.div(me, 2), 2)
    cy = lax.div(me, 4)

    def flip(v, b):
        return v + b - 2 * v * b

    def peer(slot):
        hop = slot // 2
        first, second = (1 if hop in (1, 3) else 0), (1 if hop in (2, 3) else 0)
        bx = first * (1 - core) + second * core
        by = first * core + second * (1 - core)
        bc = slot % 2
        return flip(cx, bx) * 2 + flip(cy, by) * 4 + flip(core, jnp.int32(bc))

    def remote(src, dst, send, recv, dev):
        return pltpu.make_async_remote_copy(src_ref=src, dst_ref=dst, send_sem=send, recv_sem=recv, device_id=(dev,), device_id_type=MESH)

    def x_copy(src_slot, dst_slot):
        dev = {1: 1, 2: 2, 4: 4, 3: 1, 5: 1, 6: 4, 7: 1}[dst_slot]
        return remote(xs.at[src_slot], xs.at[dst_slot], x_send.at[dst_slot], x_recv.at[dst_slot], peer(dev))

    def e_copy(slot):
        return remote(es.at[0], es.at[slot], e_send.at[slot], e_recv.at[slot], peer(slot))

    def c_copy(slot):
        return remote(cnt.at[0], cnt.at[slot], c_send.at[slot], c_recv.at[slot], peer(slot))

    def local(src, dst, i):
        return pltpu.make_async_copy(src, dst, l_sem.at[i])

    def load_w1(i):
        return local(w_in_hbm.at[:, pl.ds(pl.multiple_of(CHUNK * i, CHUNK), CHUNK)], w1.at[i], 3 + i)

    def load_w2(i):
        return local(w_out_hbm.at[pl.ds(pl.multiple_of(CHUNK * i, CHUNK), CHUNK), :], w2.at[i], 3 + NCHUNK + i)

    load_x = local(x_hbm, xs.at[0], 0)
    load_w1j = local(w_in_hbm.at[:, pl.ds(pl.multiple_of(me * HID, HID), HID)], w1j, 1)
    load_w2j = local(w_out_hbm.at[pl.ds(pl.multiple_of(me * HID, HID), HID), :], w2j, 2)
    load_x.start()
    load_w1j.start()
    load_w1(0).start()
    load_w2(0).start()

    barrier = pltpu.get_barrier_semaphore()
    for s in range(1, NUM_DEV):
        pl.semaphore_signal(barrier, inc=1, device_id=(peer(s),), device_id_type=MESH)

    counts = jnp.sum(mask_ref[...].astype(F32), axis=1, keepdims=True)
    cnt[0, 0:TASKS, :] = jnp.broadcast_to(counts, (TASKS, 128))
    cnt[0, TASKS:8, :] = jnp.zeros((8 - TASKS, 128), F32)
    hrow[...] = jnp.zeros_like(hrow)
    for c in range(CLASSES):
        hrow[8 * c:8 * c + TASKS, :] = head_ref[c].astype(F32)
    head = hrow[...].astype(BF16)

    block = lax.div(lax.broadcasted_iota(jnp.int32, (HEAD_ROWS, TASKS * CLASSES * 128), 1), 128)
    pick = lax.rem(block, CLASSES) * 8 + lax.div(block, CLASSES)
    ones = (lax.broadcasted_iota(jnp.int32, block.shape, 0) == pick).astype(F32).astype(BF16)
    wide = dot_nn(hrow[...].T.astype(BF16), ones)
    for k in range(TASKS * CLASSES):
        hbc[k] = wide[:, 128 * k:128 * k + 128]
    pl.semaphore_wait(barrier, NUM_DEV - 1)
    load_x.wait()
    x_copy(0, 1).start()
    x_copy(0, 2).start()
    for s in range(1, NUM_DEV):
        c_copy(s).start()
    for i in range(1, NCHUNK):
        load_w1(i).start()
        load_w2(i).start()
    load_w2j.start()

    load_w1j.wait()
    w1t[...] = w1j[...].astype(F32).T.astype(BF16)

    abuf1[...] = jnp.zeros_like(abuf1)
    zacc[...] = xs[0].astype(F32)
    half0, half1 = slice(0, ROWS), slice(ROWS, TOK)

    acts, slopes, dzs, qs = (act0, act1), (slope0, slope1), (dz0, dz1), (q0, q1)

    def preact(slot, part, quarter):
        r = pl.ds(pl.multiple_of(quarter * QUARTER, QUARTER), QUARTER)
        a, sl = gelu_both(dot_nt(w1t[...], xs[slot, r, :]))
        acts[part][:, r] = a.astype(BF16)
        slopes[part][:, r] = sl

    def forward(h, carry):
        load_w1(h).wait()
        load_w2(h).wait()
        acc1[h] = jnp.zeros((HID, DIM), F32)
        acc2[h] = jnp.zeros((HID, DIM), F32)
        abuf0[...] = gelu_value(dot_nn(xs[0, half0, :], w1[h])).astype(BF16)
        zacc[half1, :] += dot_nn(abuf1[...], w2[jnp.maximum(h - 1, 0)])
        abuf1[...] = gelu_value(dot_nn(xs[0, half1, :], w1[h])).astype(BF16)
        zacc[half0, :] += dot_nn(abuf0[...], w2[h])
        preact(0, 0, h)
        return carry

    lax.fori_loop(0, NCHUNK, forward, 0)
    zacc[half1, :] += dot_nn(abuf1[...], w2[NCHUNK - 1])

    for r in range(TOK // ROWS):
        cols = slice(r * ROWS, (r + 1) * ROWS)
        logits = dot_nt(head, zacc[cols, :].astype(BF16))
        l = [logits[8 * c:8 * c + TASKS] for c in range(CLASSES)]
        top = jnp.maximum(jnp.maximum(l[0], l[1]), l[2])
        ex = [jnp.exp(v - top) for v in l]
        total = ex[0] + ex[1] + ex[2]
        lab = lab_ref[:, cols]
        m = mask_ref[:, cols].astype(F32)
        for c in range(CLASSES):
            err = m * (ex[c] / total - (lab == c).astype(F32))
            for t in range(TASKS):
                ef[8 * t + c:8 * t + c + 1, cols] = err[t:t + 1]
    for t in range(TASKS):
        ef[8 * t + CLASSES:8 * t + 8, :] = jnp.zeros((8 - CLASSES, TOK), F32)
    es[0] = ef[...].astype(BF16)
    for t in range(TASKS):
        ecur[0, t] = es[0, 8 * t:8 * t + 8, :].astype(F32)

    def make_dz(dst, part, t):
        e = ecur[part, t]
        rows = [jnp.broadcast_to(e[c:c + 1, :], (8, TOK)) for c in range(CLASSES)]
        for k in range(DIM // 8):
            f = slice(8 * k, 8 * k + 8)
            h = [lanes(hbc[CLASSES * t + c, f, :], TOK) for c in range(CLASSES)]
            dst[f, :] = (h[0] * rows[0] + h[1] * rows[1] + h[2] * rows[2]).astype(BF16)

    for s in range(1, NUM_DEV):
        e_copy(s).start()
    make_dz(dz0, 0, 0)
    load_w2j.wait()
    total_cnt = cnt[0]
    for s in range(1, NUM_DEV):
        c_copy(s).wait_recv()
        total_cnt = total_cnt + cnt[s]
    inv[...] = lanes(1.0 / jnp.maximum(total_cnt, 1.0), DIM)

    def tokens_ready(s):
        for k in range(1, NUM_DEV):
            @pl.when(s == k - 1)
            def _():
                x_copy(0, k).wait_recv()
                if k == 2:
                    x_copy(2, 6).start()
                if k in (2, 4, 6):
                    x_copy(k, k + 1).start()

    def errors_ready(s, part):
        for k in range(1, NUM_DEV):
            @pl.when(s == k - 1)
            def _():
                e_copy(k).wait_recv()
                for t in range(TASKS):
                    ecur[part, t] = es[k, 8 * t:8 * t + 8, :].astype(F32)

    def run_task(s, part, t, j, next_part, next_t):
        nxt = jnp.minimum(s + 1, NUM_DEV - 1)
        scale = inv[pl.ds(t, 1), :]
        qs[j][...] = (dot_nn(w2j[...], dzs[j][...]) * slopes[part][...]).astype(BF16)
        acc2[t] += (dot_nt(acts[part][...], dzs[j][...]) * scale).astype(BF16).astype(F32)
        make_dz(dzs[1 - j], next_part, next_t)
        preact(nxt, 1 - part, t)
        acc1[t] += (dot_nn(qs[j][...], xs[s]) * scale).astype(BF16).astype(F32)

    def shard_pair(sp, carry):
        for part in range(2):
            s = 2 * sp + part
            tokens_ready(s)

            def task_pair(tp, c):
                @pl.when(tp == 1)
                def _():
                    errors_ready(s, 1 - part)

                    @pl.when(s == 0)
                    def _():
                        x_copy(0, 2).wait_send()
                        x_copy(0, 4).start()

                run_task(s, part, 2 * tp, 0, part, 2 * tp + 1)
                wrap = lax.div(2 * tp + 2, TASKS)
                run_task(s, part, 2 * tp + 1, 1, part + wrap * (1 - 2 * part), 2 * tp + 2 - TASKS * wrap)
                return c

            lax.fori_loop(0, TASKS // 2, task_pair, 0)
        return carry

    lax.fori_loop(0, NUM_DEV // 2, shard_pair, 0)

    def gram_rows(i, sums):
        r = pl.ds(pl.multiple_of(i * 8, 8), 8)
        out = list(sums)
        for acc in (acc1, acc2):
            for c in range(DIM // 128):
                g = [acc[t, r, 128 * c:128 * c + 128] for t in range(TASKS)]
                for k, (t, u) in enumerate(PAIRS):
                    out[k] = out[k] + g[t] * g[u]
        return tuple(out)

    sums = lax.fori_loop(0, HID // 8, gram_rows, tuple(jnp.zeros((8, 128), F32) for _ in PAIRS))
    for k in range(len(PAIRS)):
        gram[me, k:k + 1, :] = jnp.broadcast_to(jnp.sum(sums[k]), (1, 128))
    gram[me, len(PAIRS):16, :] = jnp.zeros((16 - len(PAIRS), 128), F32)

    def gram_copy(s, block):
        return remote(gram.at[block], gram.at[block], g_send.at[s], g_recv.at[s], peer(s))

    for s in range(1, NUM_DEV):
        gram_copy(s, me).start()
    for s in range(1, NUM_DEV):
        gram_copy(s, me).wait_recv()
    gram_sum = gram[0]
    for d in range(1, NUM_DEV):
        gram_sum = gram_sum + gram[d]
    m = {}
    for k, (t, u) in enumerate(PAIRS):
        m[t, u] = m[u, t] = gram_sum[k:k + 1, :]
    step_scale = (m[0, 0] + m[1, 1] + m[2, 2] + m[3, 3]) / TASKS
    al = [jnp.full((1, 128), 1.0 / TASKS, F32) for _ in range(TASKS)]
    for _ in range(SOLVER_STEPS):
        raised = []
        for t in range(TASKS):
            pull = (m[t, 0] * al[0] + m[t, 1] * al[1]) + (m[t, 2] * al[2] + m[t, 3] * al[3])
            raised.append(al[t] * jnp.exp(-pull / step_scale))
        norm = (raised[0] + raised[1]) + (raised[2] + raised[3])
        al = [r / norm for r in raised]
    for t in range(TASKS):
        alpha_ref[t] = jnp.max(al[t])

    for c in range(DIM // 128):
        cols = slice(128 * c, 128 * c + 128)
        comb = al[0] * acc1[0, :, cols]
        for t in range(1, TASKS):
            comb = comb + al[t] * acc1[t, :, cols]
        gsend[cols, :] = comb.T

    def o_copy(s):
        dev = peer(s)
        rows = pl.ds(pl.multiple_of(dev * FEAT, FEAT), FEAT)
        return remote(gsend.at[rows, :], gx_hbm.at[me], o_send.at[s], o_recv.at[s], dev)

    order = (2, 4, 3, 5, 6, 7, 1)
    for s in order:
        o_copy(s).start()

    for c in range(DIM // 128):
        cols = slice(128 * c, 128 * c + 128)
        comb = al[0] * acc2[0, :, cols]
        for t in range(1, TASKS):
            comb = comb + al[t] * acc2[t, :, cols]
        stage2[pl.ds(c, HID, stride=DIM // 128), :] = comb
    store2 = local(stage2, out2_hbm, 0)
    store2.start()

    keep = local(gsend.at[pl.ds(pl.multiple_of(me * FEAT, FEAT), FEAT), :], gx_hbm.at[me], 1)
    keep.start()
    for s in range(1, NUM_DEV):
        o_copy(s).wait_recv()

    x_copy(0, 1).wait_send()
    for k in (4, 3, 5, 6, 7):
        x_copy(0, k).wait_send()
    for s in range(1, NUM_DEV):
        e_copy(s).wait_send()
        c_copy(s).wait_send()
        gram_copy(s, me).wait_send()
        o_copy(s).wait_send()
    store2.wait()
    keep.wait()


PER = HID // 128
FLAT = DIM * HIDDEN // NUM_DEV // 128
HALF = FEAT // 2


def finish(alpha_in, gx_hbm, g2_hbm, alpha_ref, out1_hbm, out2_hbm, blocks, stage1, stage2, in_sem, out_sem):
    loads = [pltpu.make_async_copy(gx_hbm.at[d], blocks.at[d], in_sem.at[d]) for d in range(NUM_DEV)]
    load2 = pltpu.make_async_copy(g2_hbm, stage2, in_sem.at[NUM_DEV])
    for c in loads:
        c.start()
    load2.start()
    for t in range(TASKS):
        alpha_ref[t] = alpha_in[t]
    for c in loads:
        c.wait()
    stores = []
    for h in range(2):
        for d in range(NUM_DEV):
            for b in range(PER):
                first = h * HALF * (HIDDEN // 128) + d * PER + b
                stage1[pl.ds(first, HALF, stride=HIDDEN // 128), :] = blocks[d, h * HALF:h * HALF + HALF, 128 * b:128 * b + 128]
        rows = pl.ds(h * FLAT // 2, FLAT // 2)
        stores.append(pltpu.make_async_copy(stage1.at[rows, :], out1_hbm.at[rows, :], out_sem.at[h]))
        stores[-1].start()
        if h == 0:
            load2.wait()
            stores.append(pltpu.make_async_copy(stage2, out2_hbm, out_sem.at[2]))
            stores[-1].start()
    for c in stores:
        c.wait()


def solution(mesh):
    def local_step(x_loc, w_in, w_out, heads, lab_loc, mask_loc):
        hbm = pl.BlockSpec(memory_space=pl.ANY)
        vmem = pl.BlockSpec(memory_space=pltpu.VMEM)
        sem = pltpu.SemaphoreType.DMA((NUM_DEV,))
        v = pltpu.VMEM
        alpha, gx, g2 = pl.pallas_call(
            kernel,
            out_shape=(
                jax.ShapeDtypeStruct((TASKS,), F32),
                jax.ShapeDtypeStruct((NUM_DEV, FEAT, HID), F32),
                jax.ShapeDtypeStruct((FLAT, 128), F32),
            ),
            in_specs=[hbm, hbm, hbm, vmem, vmem, vmem],
            out_specs=(pl.BlockSpec(memory_space=pltpu.SMEM), hbm, hbm),
            scratch_shapes=[
                v((NUM_DEV, TOK, DIM), BF16),
                v((NCHUNK, DIM, CHUNK), BF16),
                v((NCHUNK, CHUNK, DIM), BF16),
                v((DIM, HID), BF16),
                v((HID, DIM), BF16),
                v((HID, DIM), BF16),
                v((ROWS, CHUNK), BF16),
                v((ROWS, CHUNK), BF16),
                v((TOK, DIM), F32),
                v((HEAD_ROWS, DIM), F32),
                v((TASKS * CLASSES, DIM, 128), F32),
                v((HEAD_ROWS, TOK), F32),
                v((NUM_DEV, HEAD_ROWS, TOK), BF16),
                v((2, TASKS, 8, TOK), F32),
                v((HID, TOK), BF16),
                v((HID, TOK), BF16),
                v((HID, TOK), F32),
                v((HID, TOK), F32),
                v((DIM, TOK), BF16),
                v((DIM, TOK), BF16),
                v((HID, TOK), BF16),
                v((HID, TOK), BF16),
                v((TASKS, HID, DIM), F32),
                v((TASKS, HID, DIM), F32),
                v((NUM_DEV, 8, 128), F32),
                v((8, DIM), F32),
                v((NUM_DEV, 16, 128), F32),
                v((DIM, HID), F32),
                v((FLAT, 128), F32),
                sem, sem, sem, sem, sem, sem, sem, sem, sem, sem,
                pltpu.SemaphoreType.DMA((3 + 2 * NCHUNK,)),
            ],
            compiler_params=pltpu.CompilerParams(collective_id=0, has_side_effects=True, vmem_limit_bytes=66_000_000),
            name="trunk",
        )(x_loc, w_in, w_out, heads.transpose(2, 0, 1), lab_loc, mask_loc)
        smem = pl.BlockSpec(memory_space=pltpu.SMEM)
        alpha, out1, out2 = pl.pallas_call(
            finish,
            out_shape=(
                jax.ShapeDtypeStruct((TASKS,), F32),
                jax.ShapeDtypeStruct((FLAT, 128), F32),
                jax.ShapeDtypeStruct((FLAT, 128), F32),
            ),
            in_specs=[smem, hbm, hbm],
            out_specs=(smem, hbm, hbm),
            scratch_shapes=[
                v((NUM_DEV, FEAT, HID), F32),
                v((FLAT, 128), F32),
                v((FLAT, 128), F32),
                pltpu.SemaphoreType.DMA((NUM_DEV + 1,)),
                pltpu.SemaphoreType.DMA((3,)),
            ],
            name="finish",
        )(alpha, gx, g2)
        return alpha, out1.reshape(-1), out2.reshape(-1)

    return jax.shard_map(local_step, mesh=mesh, in_specs=(P("data", None), P(), P(), P(), P(None, "data"), P(None, "data")), out_specs=(P(), P("data"), P("data")), check_vma=False)
```

```python
import jax
import jax.numpy as jnp
from jax import lax
from jax.experimental import pallas as pl
from jax.experimental.pallas import tpu as pltpu
from jax.sharding import PartitionSpec as P

SOLVER_STEPS = 20
MESH = pl.DeviceIdType.MESH
F32, BF16 = jnp.float32, jnp.bfloat16
NUM_DEV = 8
TASKS = 4
CLASSES = 3
TOK = 1024
DIM = 768
HIDDEN = 3072
HID = HIDDEN // NUM_DEV
FEAT = DIM // NUM_DEV
HEAD_ROWS = 32
CHUNK = 768
ROWS = 512
NCHUNK = HIDDEN // CHUNK
QUARTER = TOK // TASKS
PAIRS = [(t, s) for t in range(TASKS) for s in range(t, TASKS)]
GELU_C = 0.7978845608028654
GELU_K = 0.044715


def dot_nn(a, b):
    return lax.dot_general(a, b, (((1,), (0,)), ((), ())), preferred_element_type=F32)


def dot_nt(a, b):
    return lax.dot_general(a, b, (((1,), (1,)), ((), ())), preferred_element_type=F32)


def lanes(row, width):
    return jnp.concatenate([row] * (width // row.shape[1]), axis=1)


def gelu_parts(p):
    a = (GELU_C * GELU_K) * (p * p)
    th = jnp.tanh(p * (a + GELU_C))
    return a, th, 0.5 + 0.5 * th


def gelu_value(p):
    return p * gelu_parts(p)[2]


def gelu_both(p):
    a, th, cdf = gelu_parts(p)
    slope = cdf + ((1.0 - th * th) * p) * (1.5 * a + 0.5 * GELU_C)
    return p * cdf, slope


def kernel(x_hbm, w_in_hbm, w_out_hbm, head_ref, lab_ref, mask_ref, alpha_ref, gx_hbm, out2_hbm,
           xs, w1, w2, w1j, w1t, w2j, abuf0, abuf1, zacc, hrow, hbc, ef, es, ecur, act0, act1, slope0, slope1,
           dz0, dz1, q0, q1, acc1, acc2, cnt, inv, gram, gsend, stage2,
           x_send, x_recv, f_send, f_recv, e_send, e_recv, c_send, c_recv, g_send, g_recv, o_send, o_recv, l_sem):
    me = lax.axis_index("data")
    core = lax.rem(me, 2)
    cx = lax.rem(lax.div(me, 2), 2)
    cy = lax.div(me, 4)

    def flip(v, b):
        return v + b - 2 * v * b

    def peer(s):
        return flip(cx, s // 2 % 2) * 2 + flip(cy, s // 4) * 4 + flip(core, jnp.int32(s % 2))

    def remote(src, dst, send, recv, dev):
        return pltpu.make_async_remote_copy(src_ref=src, dst_ref=dst, send_sem=send, recv_sem=recv, device_id=(dev,), device_id_type=MESH)

    half = pl.ds(pl.multiple_of(core * ROWS, ROWS), ROWS)
    x_dev, y_dev = peer(2), peer(4)
    first_dev = core * y_dev + (1 - core) * x_dev
    second_dev = core * x_dev + (1 - core) * y_dev

    def swap_copy():
        return remote(xs.at[0], xs.at[1], x_send.at[1], x_recv.at[1], peer(1))

    def hop(src, dst, i, dev):
        return remote(xs.at[src, half, :], xs.at[dst, half, :], x_send.at[i], x_recv.at[dst], dev)

    def arrived(m):
        return hop(0, m, 2, x_dev)

    hops = {
        2: lambda: hop(0, 2 + core, 2, first_dev),
        3: lambda: hop(1, 3 - core, 3, second_dev),
        4: lambda: hop(1, 4 + core, 4, first_dev),
        5: lambda: hop(0, 5 - core, 5, second_dev),
        6: lambda: hop(2, 6, 6, y_dev),
        7: lambda: hop(3, 7, 7, x_dev),
    }

    def hand(m):
        return remote(xs.at[m, half, :], xs.at[m, half, :], f_send.at[m], f_recv.at[m], peer(1))

    def arrival_slot(s):
        bx, by = s // 2 % 2, s // 4
        return 6 + core if bx and by else 2 + 2 * core if bx else 5 - 2 * core if by else 1

    def e_copy(s):
        slot = arrival_slot(s)
        return remote(es.at[0], es.at[slot], e_send.at[s], e_recv.at[slot], peer(s))

    def e_arrived(slot):
        return remote(es.at[0], es.at[slot], e_send.at[1], e_recv.at[slot], peer(1))

    def c_copy(s):
        return remote(cnt.at[0], cnt.at[s], c_send.at[s], c_recv.at[s], peer(s))

    def local(src, dst, i):
        return pltpu.make_async_copy(src, dst, l_sem.at[i])

    def load_w1(i):
        return local(w_in_hbm.at[:, pl.ds(pl.multiple_of(CHUNK * i, CHUNK), CHUNK)], w1.at[i], 3 + i)

    def load_w2(i):
        return local(w_out_hbm.at[pl.ds(pl.multiple_of(CHUNK * i, CHUNK), CHUNK), :], w2.at[i], 3 + NCHUNK + i)

    load_x = local(x_hbm, xs.at[0], 0)
    load_w1j = local(w_in_hbm.at[:, pl.ds(pl.multiple_of(me * HID, HID), HID)], w1j, 1)
    load_w2j = local(w_out_hbm.at[pl.ds(pl.multiple_of(me * HID, HID), HID), :], w2j, 2)
    load_x.start()
    load_w1j.start()
    load_w1(0).start()
    load_w2(0).start()

    barrier = pltpu.get_barrier_semaphore()
    for s in range(1, NUM_DEV):
        pl.semaphore_signal(barrier, inc=1, device_id=(peer(s),), device_id_type=MESH)

    counts = jnp.sum(mask_ref[...].astype(F32), axis=1, keepdims=True)
    cnt[0, 0:TASKS, :] = jnp.broadcast_to(counts, (TASKS, 128))
    cnt[0, TASKS:8, :] = jnp.zeros((8 - TASKS, 128), F32)
    hrow[...] = jnp.zeros_like(hrow)
    for c in range(CLASSES):
        hrow[8 * c:8 * c + TASKS, :] = head_ref[c].astype(F32)
    head = hrow[...].astype(BF16)

    block = lax.div(lax.broadcasted_iota(jnp.int32, (HEAD_ROWS, TASKS * CLASSES * 128), 1), 128)
    pick = lax.rem(block, CLASSES) * 8 + lax.div(block, CLASSES)
    ones = (lax.broadcasted_iota(jnp.int32, block.shape, 0) == pick).astype(F32).astype(BF16)
    wide = dot_nn(hrow[...].T.astype(BF16), ones)
    for k in range(TASKS * CLASSES):
        hbc[k] = wide[:, 128 * k:128 * k + 128]
    pl.semaphore_wait(barrier, NUM_DEV - 1)
    load_x.wait()
    hops[2]().start()
    swap_copy().start()
    for s in range(1, NUM_DEV):
        c_copy(s).start()
    for i in range(1, NCHUNK):
        load_w1(i).start()
        load_w2(i).start()
    load_w2j.start()

    load_w1j.wait()
    w1t[...] = w1j[...].astype(F32).T.astype(BF16)

    abuf1[...] = jnp.zeros_like(abuf1)
    zacc[...] = xs[0].astype(F32)
    half0, half1 = slice(0, ROWS), slice(ROWS, TOK)

    acts, slopes, dzs, qs = (act0, act1), (slope0, slope1), (dz0, dz1), (q0, q1)

    def preact(slot, part, quarter):
        r = pl.ds(pl.multiple_of(quarter * QUARTER, QUARTER), QUARTER)
        a, sl = gelu_both(dot_nt(w1t[...], xs[slot, r, :]))
        acts[part][:, r] = a.astype(BF16)
        slopes[part][:, r] = sl

    def forward(h, carry):
        load_w1(h).wait()
        load_w2(h).wait()
        acc1[h] = jnp.zeros((HID, DIM), F32)
        acc2[h] = jnp.zeros((HID, DIM), F32)
        @pl.when(h == 1)
        def _():
            swap_copy().wait_recv()
            hops[3]().start()

        abuf0[...] = gelu_value(dot_nn(xs[0, half0, :], w1[h])).astype(BF16)
        zacc[half1, :] += dot_nn(abuf1[...], w2[jnp.maximum(h - 1, 0)])
        abuf1[...] = gelu_value(dot_nn(xs[0, half1, :], w1[h])).astype(BF16)
        zacc[half0, :] += dot_nn(abuf0[...], w2[h])
        preact(0, 0, h)
        return carry

    lax.fori_loop(0, NCHUNK, forward, 0)
    zacc[half1, :] += dot_nn(abuf1[...], w2[NCHUNK - 1])

    for r in range(TOK // ROWS):
        cols = slice(r * ROWS, (r + 1) * ROWS)
        logits = dot_nt(head, zacc[cols, :].astype(BF16))
        l = [logits[8 * c:8 * c + TASKS] for c in range(CLASSES)]
        top = jnp.maximum(jnp.maximum(l[0], l[1]), l[2])
        ex = [jnp.exp(v - top) for v in l]
        total = ex[0] + ex[1] + ex[2]
        lab = lab_ref[:, cols]
        m = mask_ref[:, cols].astype(F32)
        for c in range(CLASSES):
            err = m * (ex[c] / total - (lab == c).astype(F32))
            for t in range(TASKS):
                ef[8 * t + c:8 * t + c + 1, cols] = err[t:t + 1]
    for t in range(TASKS):
        ef[8 * t + CLASSES:8 * t + 8, :] = jnp.zeros((8 - CLASSES, TOK), F32)
    es[0] = ef[...].astype(BF16)
    for t in range(TASKS):
        ecur[0, t] = es[0, 8 * t:8 * t + 8, :].astype(F32)

    def make_dz(dst, part, t):
        e = ecur[part, t]
        rows = [jnp.broadcast_to(e[c:c + 1, :], (8, TOK)) for c in range(CLASSES)]
        for k in range(DIM // 8):
            f = slice(8 * k, 8 * k + 8)
            h = [lanes(hbc[CLASSES * t + c, f, :], TOK) for c in range(CLASSES)]
            dst[f, :] = (h[0] * rows[0] + h[1] * rows[1] + h[2] * rows[2]).astype(BF16)

    for s in range(1, NUM_DEV):
        e_copy(s).start()
    make_dz(dz0, 0, 0)
    load_w2j.wait()
    total_cnt = cnt[0]
    for s in range(1, NUM_DEV):
        c_copy(s).wait_recv()
        total_cnt = total_cnt + cnt[s]
    inv[...] = lanes(1.0 / jnp.maximum(total_cnt, 1.0), DIM)

    def tokens_pass(s):
        for k in (0, 2, 4):
            @pl.when(s == k)
            def _():
                for m in (k + 2, k + 3):
                    arrived(m).wait_recv()
                    hand(m).start()
                if k < 4:
                    for m in (k + 4, k + 5):
                        hops[m]().start()

    def tokens_ready(s):
        for m in range(2, NUM_DEV):
            @pl.when(s == m - 1)
            def _():
                hand(m).wait_recv()

    def errors_ready(s, part):
        for k in range(1, NUM_DEV):
            @pl.when(s == k - 1)
            def _():
                e_arrived(k).wait_recv()
                for t in range(TASKS):
                    ecur[part, t] = es[k, 8 * t:8 * t + 8, :].astype(F32)

    def run_task(s, part, t, j, next_part, next_t):
        nxt = jnp.minimum(s + 1, NUM_DEV - 1)
        scale = inv[pl.ds(t, 1), :]
        qs[j][...] = (dot_nn(w2j[...], dzs[j][...]) * slopes[part][...]).astype(BF16)
        acc2[t] += (dot_nt(acts[part][...], dzs[j][...]) * scale).astype(BF16).astype(F32)
        make_dz(dzs[1 - j], next_part, next_t)
        preact(nxt, 1 - part, t)
        acc1[t] += (dot_nn(qs[j][...], xs[s]) * scale).astype(BF16).astype(F32)

    def shard_pair(sp, carry):
        for part in range(2):
            s = 2 * sp + part
            tokens_ready(s)

            def task_pair(tp, c):
                @pl.when(tp == 1)
                def _():
                    errors_ready(s, 1 - part)
                    if part == 0:
                        tokens_pass(s)

                run_task(s, part, 2 * tp, 0, part, 2 * tp + 1)
                wrap = lax.div(2 * tp + 2, TASKS)
                run_task(s, part, 2 * tp + 1, 1, part + wrap * (1 - 2 * part), 2 * tp + 2 - TASKS * wrap)
                return c

            lax.fori_loop(0, TASKS // 2, task_pair, 0)
        return carry

    lax.fori_loop(0, NUM_DEV // 2, shard_pair, 0)

    def gram_rows(i, sums):
        r = pl.ds(pl.multiple_of(i * 8, 8), 8)
        out = list(sums)
        for acc in (acc1, acc2):
            for c in range(DIM // 128):
                g = [acc[t, r, 128 * c:128 * c + 128] for t in range(TASKS)]
                for k, (t, u) in enumerate(PAIRS):
                    out[k] = out[k] + g[t] * g[u]
        return tuple(out)

    sums = lax.fori_loop(0, HID // 8, gram_rows, tuple(jnp.zeros((8, 128), F32) for _ in PAIRS))
    for k in range(len(PAIRS)):
        gram[me, k:k + 1, :] = jnp.broadcast_to(jnp.sum(sums[k]), (1, 128))
    gram[me, len(PAIRS):16, :] = jnp.zeros((16 - len(PAIRS), 128), F32)

    def gram_copy(s, block):
        return remote(gram.at[block], gram.at[block], g_send.at[s], g_recv.at[s], peer(s))

    for s in range(1, NUM_DEV):
        gram_copy(s, me).start()
    for s in range(1, NUM_DEV):
        gram_copy(s, me).wait_recv()
    gram_sum = gram[0]
    for d in range(1, NUM_DEV):
        gram_sum = gram_sum + gram[d]
    m = {}
    for k, (t, u) in enumerate(PAIRS):
        m[t, u] = m[u, t] = gram_sum[k:k + 1, :]
    step_scale = (m[0, 0] + m[1, 1] + m[2, 2] + m[3, 3]) / TASKS
    al = [jnp.full((1, 128), 1.0 / TASKS, F32) for _ in range(TASKS)]
    for _ in range(SOLVER_STEPS):
        raised = []
        for t in range(TASKS):
            pull = (m[t, 0] * al[0] + m[t, 1] * al[1]) + (m[t, 2] * al[2] + m[t, 3] * al[3])
            raised.append(al[t] * jnp.exp(-pull / step_scale))
        norm = (raised[0] + raised[1]) + (raised[2] + raised[3])
        al = [r / norm for r in raised]
    for t in range(TASKS):
        alpha_ref[t] = jnp.max(al[t])

    for c in range(DIM // 128):
        cols = slice(128 * c, 128 * c + 128)
        comb = al[0] * acc1[0, :, cols]
        for t in range(1, TASKS):
            comb = comb + al[t] * acc1[t, :, cols]
        gsend[cols, :] = comb.T

    def o_copy(s):
        dev = peer(s)
        rows = pl.ds(pl.multiple_of(dev * FEAT, FEAT), FEAT)
        return remote(gsend.at[rows, :], gx_hbm.at[me], o_send.at[s], o_recv.at[s], dev)

    order = (2, 4, 3, 5, 6, 7, 1)
    for s in order:
        o_copy(s).start()

    for c in range(DIM // 128):
        cols = slice(128 * c, 128 * c + 128)
        comb = al[0] * acc2[0, :, cols]
        for t in range(1, TASKS):
            comb = comb + al[t] * acc2[t, :, cols]
        stage2[pl.ds(c, HID, stride=DIM // 128), :] = comb
    store2 = local(stage2, out2_hbm, 0)
    store2.start()

    keep = local(gsend.at[pl.ds(pl.multiple_of(me * FEAT, FEAT), FEAT), :], gx_hbm.at[me], 1)
    keep.start()
    for s in range(1, NUM_DEV):
        o_copy(s).wait_recv()

    swap_copy().wait_send()
    for m in range(2, NUM_DEV):
        hops[m]().wait_send()
        hand(m).wait_send()
    for s in range(1, NUM_DEV):
        e_copy(s).wait_send()
        c_copy(s).wait_send()
        gram_copy(s, me).wait_send()
        o_copy(s).wait_send()
    store2.wait()
    keep.wait()


PER = HID // 128
FLAT = DIM * HIDDEN // NUM_DEV // 128
HALF = FEAT // 2


def finish(alpha_in, gx_hbm, g2_hbm, alpha_ref, out1_hbm, out2_hbm, blocks, stage1, stage2, in_sem, out_sem):
    loads = [pltpu.make_async_copy(gx_hbm.at[d], blocks.at[d], in_sem.at[d]) for d in range(NUM_DEV)]
    load2 = pltpu.make_async_copy(g2_hbm, stage2, in_sem.at[NUM_DEV])
    for c in loads:
        c.start()
    load2.start()
    for t in range(TASKS):
        alpha_ref[t] = alpha_in[t]
    for c in loads:
        c.wait()
    stores = []
    for h in range(2):
        for d in range(NUM_DEV):
            for b in range(PER):
                first = h * HALF * (HIDDEN // 128) + d * PER + b
                stage1[pl.ds(first, HALF, stride=HIDDEN // 128), :] = blocks[d, h * HALF:h * HALF + HALF, 128 * b:128 * b + 128]
        rows = pl.ds(h * FLAT // 2, FLAT // 2)
        stores.append(pltpu.make_async_copy(stage1.at[rows, :], out1_hbm.at[rows, :], out_sem.at[h]))
        stores[-1].start()
        if h == 0:
            load2.wait()
            stores.append(pltpu.make_async_copy(stage2, out2_hbm, out_sem.at[2]))
            stores[-1].start()
    for c in stores:
        c.wait()


def solution(mesh):
    def local_step(x_loc, w_in, w_out, heads, lab_loc, mask_loc):
        hbm = pl.BlockSpec(memory_space=pl.ANY)
        vmem = pl.BlockSpec(memory_space=pltpu.VMEM)
        sem = pltpu.SemaphoreType.DMA((NUM_DEV,))
        v = pltpu.VMEM
        alpha, gx, g2 = pl.pallas_call(
            kernel,
            out_shape=(
                jax.ShapeDtypeStruct((TASKS,), F32),
                jax.ShapeDtypeStruct((NUM_DEV, FEAT, HID), F32),
                jax.ShapeDtypeStruct((FLAT, 128), F32),
            ),
            in_specs=[hbm, hbm, hbm, vmem, vmem, vmem],
            out_specs=(pl.BlockSpec(memory_space=pltpu.SMEM), hbm, hbm),
            scratch_shapes=[
                v((NUM_DEV, TOK, DIM), BF16),
                v((NCHUNK, DIM, CHUNK), BF16),
                v((NCHUNK, CHUNK, DIM), BF16),
                v((DIM, HID), BF16),
                v((HID, DIM), BF16),
                v((HID, DIM), BF16),
                v((ROWS, CHUNK), BF16),
                v((ROWS, CHUNK), BF16),
                v((TOK, DIM), F32),
                v((HEAD_ROWS, DIM), F32),
                v((TASKS * CLASSES, DIM, 128), F32),
                v((HEAD_ROWS, TOK), F32),
                v((NUM_DEV, HEAD_ROWS, TOK), BF16),
                v((2, TASKS, 8, TOK), F32),
                v((HID, TOK), BF16),
                v((HID, TOK), BF16),
                v((HID, TOK), F32),
                v((HID, TOK), F32),
                v((DIM, TOK), BF16),
                v((DIM, TOK), BF16),
                v((HID, TOK), BF16),
                v((HID, TOK), BF16),
                v((TASKS, HID, DIM), F32),
                v((TASKS, HID, DIM), F32),
                v((NUM_DEV, 8, 128), F32),
                v((8, DIM), F32),
                v((NUM_DEV, 16, 128), F32),
                v((DIM, HID), F32),
                v((FLAT, 128), F32),
                sem, sem, sem, sem, sem, sem, sem, sem, sem, sem, sem, sem,
                pltpu.SemaphoreType.DMA((3 + 2 * NCHUNK,)),
            ],
            compiler_params=pltpu.CompilerParams(collective_id=0, has_side_effects=True, vmem_limit_bytes=66_000_000),
            name="trunk",
        )(x_loc, w_in, w_out, heads.transpose(2, 0, 1), lab_loc, mask_loc)
        smem = pl.BlockSpec(memory_space=pltpu.SMEM)
        alpha, out1, out2 = pl.pallas_call(
            finish,
            out_shape=(
                jax.ShapeDtypeStruct((TASKS,), F32),
                jax.ShapeDtypeStruct((FLAT, 128), F32),
                jax.ShapeDtypeStruct((FLAT, 128), F32),
            ),
            in_specs=[smem, hbm, hbm],
            out_specs=(smem, hbm, hbm),
            scratch_shapes=[
                v((NUM_DEV, FEAT, HID), F32),
                v((FLAT, 128), F32),
                v((FLAT, 128), F32),
                pltpu.SemaphoreType.DMA((NUM_DEV + 1,)),
                pltpu.SemaphoreType.DMA((3,)),
            ],
            name="finish",
        )(alpha, gx, g2)
        return alpha, out1.reshape(-1), out2.reshape(-1)

    return jax.shard_map(local_step, mesh=mesh, in_specs=(P("data", None), P(), P(), P(), P(None, "data"), P(None, "data")), out_specs=(P(), P("data"), P("data")), check_vma=False)
```

```python
import jax
import jax.numpy as jnp
from jax import lax
from jax.experimental import pallas as pl
from jax.experimental.pallas import tpu as pltpu
from jax.sharding import PartitionSpec as P

SOLVER_STEPS = 20
MESH = pl.DeviceIdType.MESH
F32, BF16 = jnp.float32, jnp.bfloat16
NUM_DEV = 8
TASKS = 4
CLASSES = 3
TOK = 1024
DIM = 768
HIDDEN = 3072
HID = HIDDEN // NUM_DEV
FEAT = DIM // NUM_DEV
HEAD_ROWS = 32
CHUNK = 768
ROWS = 512
NCHUNK = HIDDEN // CHUNK
QUARTER = TOK // TASKS
PAIRS = [(t, s) for t in range(TASKS) for s in range(t, TASKS)]
GELU_C = 0.7978845608028654
GELU_K = 0.044715


def dot_nn(a, b):
    return lax.dot_general(a, b, (((1,), (0,)), ((), ())), preferred_element_type=F32)


def dot_nt(a, b):
    return lax.dot_general(a, b, (((1,), (1,)), ((), ())), preferred_element_type=F32)


def lanes(row, width):
    return jnp.concatenate([row] * (width // row.shape[1]), axis=1)


def gelu_parts(p):
    a = (GELU_C * GELU_K) * (p * p)
    th = jnp.tanh(p * (a + GELU_C))
    return a, th, 0.5 + 0.5 * th


def gelu_value(p):
    return p * gelu_parts(p)[2]


def gelu_both(p):
    a, th, cdf = gelu_parts(p)
    slope = cdf + ((1.0 - th * th) * p) * (1.5 * a + 0.5 * GELU_C)
    return p * cdf, slope


def kernel(x_hbm, w_in_hbm, w_out_hbm, head_ref, lab_ref, mask_ref, alpha_ref, gx_hbm, out2_hbm,
           xs, w1, w2, w1j, w1t, w2j, abuf0, abuf1, zacc, hrow, hbc, ef, es, ecur, act0, act1, slope0, slope1,
           dz0, dz1, q0, q1, acc1, acc2, cnt, inv, gram, gsend, stage2,
           x_send, x_recv, f_send, f_recv, e_send, e_recv, c_send, c_recv, g_send, g_recv, o_send, o_recv, l_sem):
    me = lax.axis_index("data")
    core = lax.rem(me, 2)
    cx = lax.rem(lax.div(me, 2), 2)
    cy = lax.div(me, 4)

    def flip(v, b):
        return v + b - 2 * v * b

    def peer(s):
        return flip(cx, s // 2 % 2) * 2 + flip(cy, s // 4) * 4 + flip(core, jnp.int32(s % 2))

    def remote(src, dst, send, recv, dev):
        return pltpu.make_async_remote_copy(src_ref=src, dst_ref=dst, send_sem=send, recv_sem=recv, device_id=(dev,), device_id_type=MESH)

    half = pl.ds(pl.multiple_of(core * ROWS, ROWS), ROWS)
    x_dev, y_dev = peer(2), peer(4)
    first_dev = core * y_dev + (1 - core) * x_dev
    second_dev = core * x_dev + (1 - core) * y_dev

    def swap_copy():
        return remote(xs.at[0], xs.at[1], x_send.at[1], x_recv.at[1], peer(1))

    def hop(src, dst, i, dev):
        return remote(xs.at[src, half, :], xs.at[dst, half, :], x_send.at[i], x_recv.at[dst], dev)

    def arrived(m):
        return hop(0, m, 2, x_dev)

    hops = {
        2: lambda: hop(0, 2 + core, 2, first_dev),
        3: lambda: hop(1, 3 - core, 3, second_dev),
        4: lambda: hop(1, 4 + core, 4, first_dev),
        5: lambda: hop(0, 5 - core, 5, second_dev),
        6: lambda: hop(2, 6, 6, y_dev),
        7: lambda: hop(3, 7, 7, x_dev),
    }

    def hand(m):
        return remote(xs.at[m, half, :], xs.at[m, half, :], f_send.at[m], f_recv.at[m], peer(1))

    def arrival_slot(s):
        bx, by = s // 2 % 2, s // 4
        return 6 + core if bx and by else 2 + 2 * core if bx else 5 - 2 * core if by else 1

    def e_copy(s):
        slot = arrival_slot(s)
        return remote(es.at[0], es.at[slot], e_send.at[s], e_recv.at[slot], peer(s))

    def e_arrived(slot):
        return remote(es.at[0], es.at[slot], e_send.at[1], e_recv.at[slot], peer(1))

    def c_copy(s):
        return remote(cnt.at[0], cnt.at[s], c_send.at[s], c_recv.at[s], peer(s))

    def local(src, dst, i):
        return pltpu.make_async_copy(src, dst, l_sem.at[i])

    def load_w1(i):
        return local(w_in_hbm.at[:, pl.ds(pl.multiple_of(CHUNK * i, CHUNK), CHUNK)], w1.at[i], 3 + i)

    def load_w2(i):
        return local(w_out_hbm.at[pl.ds(pl.multiple_of(CHUNK * i, CHUNK), CHUNK), :], w2.at[i], 3 + NCHUNK + i)

    load_x = local(x_hbm, xs.at[0], 0)
    load_w1j = local(w_in_hbm.at[:, pl.ds(pl.multiple_of(me * HID, HID), HID)], w1j, 1)
    load_w2j = local(w_out_hbm.at[pl.ds(pl.multiple_of(me * HID, HID), HID), :], w2j, 2)
    load_x.start()
    load_w1j.start()
    load_w1(0).start()
    load_w2(0).start()

    barrier = pltpu.get_barrier_semaphore()
    for s in range(1, NUM_DEV):
        pl.semaphore_signal(barrier, inc=1, device_id=(peer(s),), device_id_type=MESH)

    counts = jnp.sum(mask_ref[...].astype(F32), axis=1, keepdims=True)
    cnt[0, 0:TASKS, :] = jnp.broadcast_to(counts, (TASKS, 128))
    cnt[0, TASKS:8, :] = jnp.zeros((8 - TASKS, 128), F32)
    hrow[...] = jnp.zeros_like(hrow)
    for c in range(CLASSES):
        hrow[8 * c:8 * c + TASKS, :] = head_ref[c].astype(F32)
    head = hrow[...].astype(BF16)

    block = lax.div(lax.broadcasted_iota(jnp.int32, (HEAD_ROWS, TASKS * CLASSES * 128), 1), 128)
    pick = lax.rem(block, CLASSES) * 8 + lax.div(block, CLASSES)
    ones = (lax.broadcasted_iota(jnp.int32, block.shape, 0) == pick).astype(F32).astype(BF16)
    wide = dot_nn(hrow[...].T.astype(BF16), ones)
    for k in range(TASKS * CLASSES):
        hbc[k] = wide[:, 128 * k:128 * k + 128]
    pl.semaphore_wait(barrier, NUM_DEV - 1)
    load_x.wait()
    hops[2]().start()
    swap_copy().start()
    for s in range(1, NUM_DEV):
        c_copy(s).start()
    for i in range(1, NCHUNK):
        load_w1(i).start()
        load_w2(i).start()
    load_w2j.start()

    load_w1j.wait()
    w1t[...] = w1j[...].astype(F32).T.astype(BF16)

    abuf1[...] = jnp.zeros_like(abuf1)
    zacc[...] = xs[0].astype(F32)
    half0, half1 = slice(0, ROWS), slice(ROWS, TOK)

    acts, slopes, dzs, qs = (act0, act1), (slope0, slope1), (dz0, dz1), (q0, q1)

    def preact(slot, part, quarter):
        r = pl.ds(pl.multiple_of(quarter * QUARTER, QUARTER), QUARTER)
        a, sl = gelu_both(dot_nt(w1t[...], xs[slot, r, :]))
        acts[part][:, r] = a.astype(BF16)
        slopes[part][:, r] = sl

    def forward(h, carry):
        load_w1(h).wait()
        load_w2(h).wait()
        acc1[h] = jnp.zeros((HID, DIM), F32)
        acc2[h] = jnp.zeros((HID, DIM), F32)
        @pl.when(h == 1)
        def _():
            swap_copy().wait_recv()
            hops[3]().start()

        abuf0[...] = gelu_value(dot_nn(xs[0, half0, :], w1[h])).astype(BF16)
        zacc[half1, :] += dot_nn(abuf1[...], w2[jnp.maximum(h - 1, 0)])
        abuf1[...] = gelu_value(dot_nn(xs[0, half1, :], w1[h])).astype(BF16)
        zacc[half0, :] += dot_nn(abuf0[...], w2[h])
        preact(0, 0, h)
        return carry

    lax.fori_loop(0, NCHUNK, forward, 0)
    zacc[half1, :] += dot_nn(abuf1[...], w2[NCHUNK - 1])

    for r in range(TOK // ROWS):
        cols = slice(r * ROWS, (r + 1) * ROWS)
        logits = dot_nt(head, zacc[cols, :].astype(BF16))
        l = [logits[8 * c:8 * c + TASKS] for c in range(CLASSES)]
        top = jnp.maximum(jnp.maximum(l[0], l[1]), l[2])
        ex = [jnp.exp(v - top) for v in l]
        total = ex[0] + ex[1] + ex[2]
        lab = lab_ref[:, cols]
        m = mask_ref[:, cols].astype(F32)
        for c in range(CLASSES):
            err = m * (ex[c] / total - (lab == c).astype(F32))
            for t in range(TASKS):
                ef[8 * t + c:8 * t + c + 1, cols] = err[t:t + 1]
    for t in range(TASKS):
        ef[8 * t + CLASSES:8 * t + 8, :] = jnp.zeros((8 - CLASSES, TOK), F32)
    es[0] = ef[...].astype(BF16)
    for t in range(TASKS):
        ecur[0, t] = es[0, 8 * t:8 * t + 8, :].astype(F32)

    def make_dz(dst, part, t):
        e = ecur[part, t]
        rows = [jnp.broadcast_to(e[c:c + 1, :], (8, TOK)) for c in range(CLASSES)]
        for k in range(DIM // 8):
            f = slice(8 * k, 8 * k + 8)
            h = [lanes(hbc[CLASSES * t + c, f, :], TOK) for c in range(CLASSES)]
            dst[f, :] = (h[0] * rows[0] + h[1] * rows[1] + h[2] * rows[2]).astype(BF16)

    for s in range(1, NUM_DEV):
        e_copy(s).start()
    make_dz(dz0, 0, 0)
    load_w2j.wait()
    total_cnt = cnt[0]
    for s in range(1, NUM_DEV):
        c_copy(s).wait_recv()
        total_cnt = total_cnt + cnt[s]
    inv[...] = lanes(1.0 / jnp.maximum(total_cnt, 1.0), DIM)

    def link_half_ready(s):
        for k in (1, 3, 5):
            @pl.when(s == k)
            def _():
                for m in (k + 1, k + 2):
                    arrived(m).wait_recv()
                    hand(m).start()

    def other_half_ready(s):
        for m in range(2, NUM_DEV):
            @pl.when(s == m - 1)
            def _():
                hand(m).wait_recv()
        for k, after in ((0, (4, 5)), (2, (6, 7))):
            @pl.when(s == k)
            def _():
                for m in after:
                    hops[m]().start()

    def errors_ready(s, part):
        for k in range(1, NUM_DEV):
            @pl.when(s == k - 1)
            def _():
                e_arrived(k).wait_recv()
                for t in range(TASKS):
                    ecur[part, t] = es[k, 8 * t:8 * t + 8, :].astype(F32)

    def run_task(s, part, t, j, next_part, next_t):
        nxt = jnp.minimum(s + 1, NUM_DEV - 1)
        scale = inv[pl.ds(t, 1), :]
        qs[j][...] = (dot_nn(w2j[...], dzs[j][...]) * slopes[part][...]).astype(BF16)
        acc2[t] += (dot_nt(acts[part][...], dzs[j][...]) * scale).astype(BF16).astype(F32)
        make_dz(dzs[1 - j], next_part, next_t)
        preact(nxt, 1 - part, lax.rem(t + 2 * core, TASKS))
        acc1[t] += (dot_nn(qs[j][...], xs[s]) * scale).astype(BF16).astype(F32)

    def shard_pair(sp, carry):
        for part in range(2):
            s = 2 * sp + part
            link_half_ready(s)

            def task_pair(tp, c):
                @pl.when(tp == 1)
                def _():
                    errors_ready(s, 1 - part)
                    other_half_ready(s)

                run_task(s, part, 2 * tp, 0, part, 2 * tp + 1)
                wrap = lax.div(2 * tp + 2, TASKS)
                run_task(s, part, 2 * tp + 1, 1, part + wrap * (1 - 2 * part), 2 * tp + 2 - TASKS * wrap)
                return c

            lax.fori_loop(0, TASKS // 2, task_pair, 0)
        return carry

    lax.fori_loop(0, NUM_DEV // 2, shard_pair, 0)

    def gram_rows(i, sums):
        r = pl.ds(pl.multiple_of(i * 8, 8), 8)
        out = list(sums)
        for acc in (acc1, acc2):
            for c in range(DIM // 128):
                g = [acc[t, r, 128 * c:128 * c + 128] for t in range(TASKS)]
                for k, (t, u) in enumerate(PAIRS):
                    out[k] = out[k] + g[t] * g[u]
        return tuple(out)

    sums = lax.fori_loop(0, HID // 8, gram_rows, tuple(jnp.zeros((8, 128), F32) for _ in PAIRS))
    for k in range(len(PAIRS)):
        gram[me, k:k + 1, :] = jnp.broadcast_to(jnp.sum(sums[k]), (1, 128))
    gram[me, len(PAIRS):16, :] = jnp.zeros((16 - len(PAIRS), 128), F32)

    def gram_copy(s, block):
        return remote(gram.at[block], gram.at[block], g_send.at[s], g_recv.at[s], peer(s))

    for s in range(1, NUM_DEV):
        gram_copy(s, me).start()
    for s in range(1, NUM_DEV):
        gram_copy(s, me).wait_recv()
    gram_sum = gram[0]
    for d in range(1, NUM_DEV):
        gram_sum = gram_sum + gram[d]
    m = {}
    for k, (t, u) in enumerate(PAIRS):
        m[t, u] = m[u, t] = gram_sum[k:k + 1, :]
    step_scale = (m[0, 0] + m[1, 1] + m[2, 2] + m[3, 3]) / TASKS
    al = [jnp.full((1, 128), 1.0 / TASKS, F32) for _ in range(TASKS)]
    for _ in range(SOLVER_STEPS):
        raised = []
        for t in range(TASKS):
            pull = (m[t, 0] * al[0] + m[t, 1] * al[1]) + (m[t, 2] * al[2] + m[t, 3] * al[3])
            raised.append(al[t] * jnp.exp(-pull / step_scale))
        norm = (raised[0] + raised[1]) + (raised[2] + raised[3])
        al = [r / norm for r in raised]
    for t in range(TASKS):
        alpha_ref[t] = jnp.max(al[t])

    for c in range(DIM // 128):
        cols = slice(128 * c, 128 * c + 128)
        comb = al[0] * acc1[0, :, cols]
        for t in range(1, TASKS):
            comb = comb + al[t] * acc1[t, :, cols]
        gsend[cols, :] = comb.T

    def o_copy(s):
        dev = peer(s)
        rows = pl.ds(pl.multiple_of(dev * FEAT, FEAT), FEAT)
        return remote(gsend.at[rows, :], gx_hbm.at[me], o_send.at[s], o_recv.at[s], dev)

    order = (2, 4, 3, 5, 6, 7, 1)
    for s in order:
        o_copy(s).start()

    for c in range(DIM // 128):
        cols = slice(128 * c, 128 * c + 128)
        comb = al[0] * acc2[0, :, cols]
        for t in range(1, TASKS):
            comb = comb + al[t] * acc2[t, :, cols]
        stage2[pl.ds(c, HID, stride=DIM // 128), :] = comb
    store2 = local(stage2, out2_hbm, 0)
    store2.start()

    keep = local(gsend.at[pl.ds(pl.multiple_of(me * FEAT, FEAT), FEAT), :], gx_hbm.at[me], 1)
    keep.start()
    for s in range(1, NUM_DEV):
        o_copy(s).wait_recv()

    swap_copy().wait_send()
    for m in range(2, NUM_DEV):
        hops[m]().wait_send()
        hand(m).wait_send()
    for s in range(1, NUM_DEV):
        e_copy(s).wait_send()
        c_copy(s).wait_send()
        gram_copy(s, me).wait_send()
        o_copy(s).wait_send()
    store2.wait()
    keep.wait()


PER = HID // 128
FLAT = DIM * HIDDEN // NUM_DEV // 128
HALF = FEAT // 2


def finish(alpha_in, gx_hbm, g2_hbm, alpha_ref, out1_hbm, out2_hbm, blocks, stage1, stage2, in_sem, out_sem):
    halves = [[pltpu.make_async_copy(gx_hbm.at[d, pl.ds(h * HALF, HALF), :], blocks.at[d, pl.ds(h * HALF, HALF), :], in_sem.at[h, d]) for d in range(NUM_DEV)] for h in range(2)]
    load2 = pltpu.make_async_copy(g2_hbm, stage2, out_sem.at[3])
    store2 = pltpu.make_async_copy(stage2, out2_hbm, out_sem.at[2])
    for c in halves[0]:
        c.start()
    load2.start()
    for c in halves[1]:
        c.start()
    for t in range(TASKS):
        alpha_ref[t] = alpha_in[t]
    stores = [store2]
    for h in range(2):
        for c in halves[h]:
            c.wait()
        if h == 1:
            load2.wait()
            store2.start()
        for d in range(NUM_DEV):
            for b in range(PER):
                first = h * HALF * (HIDDEN // 128) + d * PER + b
                stage1[pl.ds(first, HALF, stride=HIDDEN // 128), :] = blocks[d, h * HALF:h * HALF + HALF, 128 * b:128 * b + 128]
        rows = pl.ds(h * FLAT // 2, FLAT // 2)
        stores.append(pltpu.make_async_copy(stage1.at[rows, :], out1_hbm.at[rows, :], out_sem.at[h]))
        stores[-1].start()
    for c in stores:
        c.wait()


def solution(mesh):
    def local_step(x_loc, w_in, w_out, heads, lab_loc, mask_loc):
        hbm = pl.BlockSpec(memory_space=pl.ANY)
        vmem = pl.BlockSpec(memory_space=pltpu.VMEM)
        sem = pltpu.SemaphoreType.DMA((NUM_DEV,))
        v = pltpu.VMEM
        alpha, gx, g2 = pl.pallas_call(
            kernel,
            out_shape=(
                jax.ShapeDtypeStruct((TASKS,), F32),
                jax.ShapeDtypeStruct((NUM_DEV, FEAT, HID), F32),
                jax.ShapeDtypeStruct((FLAT, 128), F32),
            ),
            in_specs=[hbm, hbm, hbm, vmem, vmem, vmem],
            out_specs=(pl.BlockSpec(memory_space=pltpu.SMEM), hbm, hbm),
            scratch_shapes=[
                v((NUM_DEV, TOK, DIM), BF16),
                v((NCHUNK, DIM, CHUNK), BF16),
                v((NCHUNK, CHUNK, DIM), BF16),
                v((DIM, HID), BF16),
                v((HID, DIM), BF16),
                v((HID, DIM), BF16),
                v((ROWS, CHUNK), BF16),
                v((ROWS, CHUNK), BF16),
                v((TOK, DIM), F32),
                v((HEAD_ROWS, DIM), F32),
                v((TASKS * CLASSES, DIM, 128), F32),
                v((HEAD_ROWS, TOK), F32),
                v((NUM_DEV, HEAD_ROWS, TOK), BF16),
                v((2, TASKS, 8, TOK), F32),
                v((HID, TOK), BF16),
                v((HID, TOK), BF16),
                v((HID, TOK), F32),
                v((HID, TOK), F32),
                v((DIM, TOK), BF16),
                v((DIM, TOK), BF16),
                v((HID, TOK), BF16),
                v((HID, TOK), BF16),
                v((TASKS, HID, DIM), F32),
                v((TASKS, HID, DIM), F32),
                v((NUM_DEV, 8, 128), F32),
                v((8, DIM), F32),
                v((NUM_DEV, 16, 128), F32),
                v((DIM, HID), F32),
                v((FLAT, 128), F32),
                sem, sem, sem, sem, sem, sem, sem, sem, sem, sem, sem, sem,
                pltpu.SemaphoreType.DMA((3 + 2 * NCHUNK,)),
            ],
            compiler_params=pltpu.CompilerParams(collective_id=0, has_side_effects=True, vmem_limit_bytes=66_000_000),
            name="trunk",
        )(x_loc, w_in, w_out, heads.transpose(2, 0, 1), lab_loc, mask_loc)
        smem = pl.BlockSpec(memory_space=pltpu.SMEM)
        alpha, out1, out2 = pl.pallas_call(
            finish,
            out_shape=(
                jax.ShapeDtypeStruct((TASKS,), F32),
                jax.ShapeDtypeStruct((FLAT, 128), F32),
                jax.ShapeDtypeStruct((FLAT, 128), F32),
            ),
            in_specs=[smem, hbm, hbm],
            out_specs=(smem, hbm, hbm),
            scratch_shapes=[
                v((NUM_DEV, FEAT, HID), F32),
                v((FLAT, 128), F32),
                v((FLAT, 128), F32),
                pltpu.SemaphoreType.DMA((2, NUM_DEV)),
                pltpu.SemaphoreType.DMA((4,)),
            ],
            name="finish",
        )(alpha, gx, g2)
        return alpha, out1.reshape(-1), out2.reshape(-1)

    return jax.shard_map(local_step, mesh=mesh, in_specs=(P("data", None), P(), P(), P(), P(None, "data"), P(None, "data")), out_specs=(P(), P("data"), P("data")), check_vma=False)
```

```python
import jax
import jax.numpy as jnp
from jax import lax
from jax.experimental import pallas as pl
from jax.experimental.pallas import tpu as pltpu
from jax.sharding import PartitionSpec as P

SOLVER_STEPS = 20
MESH = pl.DeviceIdType.MESH
F32, BF16 = jnp.float32, jnp.bfloat16
NUM_DEV = 8
TASKS = 4
CLASSES = 3
TOK = 1024
DIM = 768
HIDDEN = 3072
HID = HIDDEN // NUM_DEV
FEAT = DIM // NUM_DEV
HEAD_ROWS = 32
CHUNK = 768
ROWS = 512
NCHUNK = HIDDEN // CHUNK
QUARTER = TOK // TASKS
PAIRS = [(t, s) for t in range(TASKS) for s in range(t, TASKS)]
GELU_C = 0.7978845608028654
GELU_K = 0.044715


def dot_nn(a, b):
    return lax.dot_general(a, b, (((1,), (0,)), ((), ())), preferred_element_type=F32)


def dot_nt(a, b):
    return lax.dot_general(a, b, (((1,), (1,)), ((), ())), preferred_element_type=F32)


def lanes(row, width):
    return jnp.concatenate([row] * (width // row.shape[1]), axis=1)


def gelu_parts(p):
    a = (GELU_C * GELU_K) * (p * p)
    th = jnp.tanh(p * (a + GELU_C))
    return a, th, 0.5 + 0.5 * th


def gelu_value(p):
    return p * gelu_parts(p)[2]


def gelu_both(p):
    a, th, cdf = gelu_parts(p)
    slope = cdf + ((1.0 - th * th) * p) * (1.5 * a + 0.5 * GELU_C)
    return p * cdf, slope


def kernel(x_hbm, w_in_hbm, w_out_hbm, head_ref, lab_ref, mask_ref, alpha_ref, gx, stage2,
           xs, w1, w2, w1j, w1t, w2j, abuf0, abuf1, zacc, hrow, hbc, ef, es, ecur, act0, act1, slope0, slope1,
           dz0, dz1, q0, q1, acc1, acc2, cnt, inv, gram, gsend,
           x_send, x_recv, f_send, f_recv, e_send, e_recv, c_send, c_recv, g_send, g_recv, o_send, o_recv, l_sem):
    me = lax.axis_index("data")
    core = lax.rem(me, 2)
    cx = lax.rem(lax.div(me, 2), 2)
    cy = lax.div(me, 4)

    def flip(v, b):
        return v + b - 2 * v * b

    def peer(s):
        return flip(cx, s // 2 % 2) * 2 + flip(cy, s // 4) * 4 + flip(core, jnp.int32(s % 2))

    def remote(src, dst, send, recv, dev):
        return pltpu.make_async_remote_copy(src_ref=src, dst_ref=dst, send_sem=send, recv_sem=recv, device_id=(dev,), device_id_type=MESH)

    half = pl.ds(pl.multiple_of(core * ROWS, ROWS), ROWS)
    x_dev, y_dev = peer(2), peer(4)
    first_dev = core * y_dev + (1 - core) * x_dev
    second_dev = core * x_dev + (1 - core) * y_dev

    def swap_copy():
        return remote(xs.at[0], xs.at[1], x_send.at[1], x_recv.at[1], peer(1))

    def hop(src, dst, i, dev):
        return remote(xs.at[src, half, :], xs.at[dst, half, :], x_send.at[i], x_recv.at[dst], dev)

    def arrived(m):
        return hop(0, m, 2, x_dev)

    hops = {
        2: lambda: hop(0, 2 + core, 2, first_dev),
        3: lambda: hop(1, 3 - core, 3, second_dev),
        4: lambda: hop(1, 4 + core, 4, first_dev),
        5: lambda: hop(0, 5 - core, 5, second_dev),
        6: lambda: hop(2, 6, 6, y_dev),
        7: lambda: hop(3, 7, 7, x_dev),
    }

    def hand(m):
        return remote(xs.at[m, half, :], xs.at[m, half, :], f_send.at[m], f_recv.at[m], peer(1))

    def arrival_slot(s):
        bx, by = s // 2 % 2, s // 4
        return 6 + core if bx and by else 2 + 2 * core if bx else 5 - 2 * core if by else 1

    def e_copy(s):
        slot = arrival_slot(s)
        return remote(es.at[0], es.at[slot], e_send.at[s], e_recv.at[slot], peer(s))

    def e_arrived(slot):
        return remote(es.at[0], es.at[slot], e_send.at[1], e_recv.at[slot], peer(1))

    def c_copy(s):
        return remote(cnt.at[0], cnt.at[s], c_send.at[s], c_recv.at[s], peer(s))

    def local(src, dst, i):
        return pltpu.make_async_copy(src, dst, l_sem.at[i])

    def load_w1(i):
        return local(w_in_hbm.at[:, pl.ds(pl.multiple_of(CHUNK * i, CHUNK), CHUNK)], w1.at[i], 3 + i)

    def load_w2(i):
        return local(w_out_hbm.at[pl.ds(pl.multiple_of(CHUNK * i, CHUNK), CHUNK), :], w2.at[i], 3 + NCHUNK + i)

    load_x = local(x_hbm, xs.at[0], 0)
    load_w1j = local(w_in_hbm.at[:, pl.ds(pl.multiple_of(me * HID, HID), HID)], w1j, 1)
    load_w2j = local(w_out_hbm.at[pl.ds(pl.multiple_of(me * HID, HID), HID), :], w2j, 2)
    load_x.start()
    load_w1j.start()
    load_w1(0).start()
    load_w2(0).start()

    barrier = pltpu.get_barrier_semaphore()
    for s in range(1, NUM_DEV):
        pl.semaphore_signal(barrier, inc=1, device_id=(peer(s),), device_id_type=MESH)

    counts = jnp.sum(mask_ref[...].astype(F32), axis=1, keepdims=True)
    cnt[0, 0:TASKS, :] = jnp.broadcast_to(counts, (TASKS, 128))
    cnt[0, TASKS:8, :] = jnp.zeros((8 - TASKS, 128), F32)
    hrow[...] = jnp.zeros_like(hrow)
    for c in range(CLASSES):
        hrow[8 * c:8 * c + TASKS, :] = head_ref[c].astype(F32)
    head = hrow[...].astype(BF16)

    block = lax.div(lax.broadcasted_iota(jnp.int32, (HEAD_ROWS, TASKS * CLASSES * 128), 1), 128)
    pick = lax.rem(block, CLASSES) * 8 + lax.div(block, CLASSES)
    ones = (lax.broadcasted_iota(jnp.int32, block.shape, 0) == pick).astype(F32).astype(BF16)
    wide = dot_nn(hrow[...].T.astype(BF16), ones)
    for k in range(TASKS * CLASSES):
        hbc[k] = wide[:, 128 * k:128 * k + 128]
    pl.semaphore_wait(barrier, NUM_DEV - 1)
    load_x.wait()
    hops[2]().start()
    swap_copy().start()
    for s in range(1, NUM_DEV):
        c_copy(s).start()
    for i in range(1, NCHUNK):
        load_w1(i).start()
        load_w2(i).start()
    load_w2j.start()

    load_w1j.wait()
    w1t[...] = w1j[...].astype(F32).T.astype(BF16)

    abuf1[...] = jnp.zeros_like(abuf1)
    zacc[...] = xs[0].astype(F32)
    half0, half1 = slice(0, ROWS), slice(ROWS, TOK)

    acts, slopes, dzs, qs = (act0, act1), (slope0, slope1), (dz0, dz1), (q0, q1)

    def preact(slot, part, quarter):
        r = pl.ds(pl.multiple_of(quarter * QUARTER, QUARTER), QUARTER)
        a, sl = gelu_both(dot_nt(w1t[...], xs[slot, r, :]))
        acts[part][:, r] = a.astype(BF16)
        slopes[part][:, r] = sl

    def forward(h, carry):
        load_w1(h).wait()
        load_w2(h).wait()
        acc1[h] = jnp.zeros((HID, DIM), F32)
        acc2[h] = jnp.zeros((HID, DIM), F32)
        @pl.when(h == 1)
        def _():
            swap_copy().wait_recv()
            hops[3]().start()

        abuf0[...] = gelu_value(dot_nn(xs[0, half0, :], w1[h])).astype(BF16)
        zacc[half1, :] += dot_nn(abuf1[...], w2[jnp.maximum(h - 1, 0)])
        abuf1[...] = gelu_value(dot_nn(xs[0, half1, :], w1[h])).astype(BF16)
        zacc[half0, :] += dot_nn(abuf0[...], w2[h])
        preact(0, 0, h)
        return carry

    lax.fori_loop(0, NCHUNK, forward, 0)
    zacc[half1, :] += dot_nn(abuf1[...], w2[NCHUNK - 1])

    for r in range(TOK // ROWS):
        cols = slice(r * ROWS, (r + 1) * ROWS)
        logits = dot_nt(head, zacc[cols, :].astype(BF16))
        l = [logits[8 * c:8 * c + TASKS] for c in range(CLASSES)]
        top = jnp.maximum(jnp.maximum(l[0], l[1]), l[2])
        ex = [jnp.exp(v - top) for v in l]
        total = ex[0] + ex[1] + ex[2]
        lab = lab_ref[:, cols]
        m = mask_ref[:, cols].astype(F32)
        for c in range(CLASSES):
            err = m * (ex[c] / total - (lab == c).astype(F32))
            for t in range(TASKS):
                ef[8 * t + c:8 * t + c + 1, cols] = err[t:t + 1]
    for t in range(TASKS):
        ef[8 * t + CLASSES:8 * t + 8, :] = jnp.zeros((8 - CLASSES, TOK), F32)
    es[0] = ef[...].astype(BF16)
    for t in range(TASKS):
        ecur[0, t] = es[0, 8 * t:8 * t + 8, :].astype(F32)

    def make_dz(dst, part, t):
        e = ecur[part, t]
        rows = [jnp.broadcast_to(e[c:c + 1, :], (8, TOK)) for c in range(CLASSES)]
        for k in range(DIM // 8):
            f = slice(8 * k, 8 * k + 8)
            h = [lanes(hbc[CLASSES * t + c, f, :], TOK) for c in range(CLASSES)]
            dst[f, :] = (h[0] * rows[0] + h[1] * rows[1] + h[2] * rows[2]).astype(BF16)

    for s in range(1, NUM_DEV):
        e_copy(s).start()
    make_dz(dz0, 0, 0)
    load_w2j.wait()
    total_cnt = cnt[0]
    for s in range(1, NUM_DEV):
        c_copy(s).wait_recv()
        total_cnt = total_cnt + cnt[s]
    inv[...] = lanes(1.0 / jnp.maximum(total_cnt, 1.0), DIM)

    def link_half_ready(s):
        for k in (1, 3, 5):
            @pl.when(s == k)
            def _():
                for m in (k + 1, k + 2):
                    arrived(m).wait_recv()
                    hand(m).start()

    def other_half_ready(s):
        for m in range(2, NUM_DEV):
            @pl.when(s == m - 1)
            def _():
                hand(m).wait_recv()
        for k, after in ((0, (4, 5)), (2, (6, 7))):
            @pl.when(s == k)
            def _():
                for m in after:
                    hops[m]().start()

    def errors_ready(s, part):
        for k in range(1, NUM_DEV):
            @pl.when(s == k - 1)
            def _():
                e_arrived(k).wait_recv()
                for t in range(TASKS):
                    ecur[part, t] = es[k, 8 * t:8 * t + 8, :].astype(F32)

    def run_task(s, part, t, j, next_part, next_t):
        nxt = jnp.minimum(s + 1, NUM_DEV - 1)
        scale = inv[pl.ds(t, 1), :]
        qs[j][...] = (dot_nn(w2j[...], dzs[j][...]) * slopes[part][...]).astype(BF16)
        acc2[t] += (dot_nt(acts[part][...], dzs[j][...]) * scale).astype(BF16).astype(F32)
        make_dz(dzs[1 - j], next_part, next_t)
        preact(nxt, 1 - part, lax.rem(t + 2 * core, TASKS))
        acc1[t] += (dot_nn(qs[j][...], xs[s]) * scale).astype(BF16).astype(F32)

    def shard_pair(sp, carry):
        for part in range(2):
            s = 2 * sp + part
            link_half_ready(s)

            def task_pair(tp, c):
                @pl.when(tp == 1)
                def _():
                    errors_ready(s, 1 - part)
                    other_half_ready(s)

                run_task(s, part, 2 * tp, 0, part, 2 * tp + 1)
                wrap = lax.div(2 * tp + 2, TASKS)
                run_task(s, part, 2 * tp + 1, 1, part + wrap * (1 - 2 * part), 2 * tp + 2 - TASKS * wrap)
                return c

            lax.fori_loop(0, TASKS // 2, task_pair, 0)
        return carry

    lax.fori_loop(0, NUM_DEV // 2, shard_pair, 0)

    def gram_rows(i, sums):
        r = pl.ds(pl.multiple_of(i * 8, 8), 8)
        out = list(sums)
        for acc in (acc1, acc2):
            for c in range(DIM // 128):
                g = [acc[t, r, 128 * c:128 * c + 128] for t in range(TASKS)]
                for k, (t, u) in enumerate(PAIRS):
                    out[k] = out[k] + g[t] * g[u]
        return tuple(out)

    sums = lax.fori_loop(0, HID // 8, gram_rows, tuple(jnp.zeros((8, 128), F32) for _ in PAIRS))
    for k in range(len(PAIRS)):
        gram[me, k:k + 1, :] = jnp.broadcast_to(jnp.sum(sums[k]), (1, 128))
    gram[me, len(PAIRS):16, :] = jnp.zeros((16 - len(PAIRS), 128), F32)

    def gram_copy(s, block):
        return remote(gram.at[block], gram.at[block], g_send.at[s], g_recv.at[s], peer(s))

    for s in range(1, NUM_DEV):
        gram_copy(s, me).start()
    for s in range(1, NUM_DEV):
        gram_copy(s, me).wait_recv()
    gram_sum = gram[0]
    for d in range(1, NUM_DEV):
        gram_sum = gram_sum + gram[d]
    m = {}
    for k, (t, u) in enumerate(PAIRS):
        m[t, u] = m[u, t] = gram_sum[k:k + 1, :]
    step_scale = (m[0, 0] + m[1, 1] + m[2, 2] + m[3, 3]) / TASKS
    al = [jnp.full((1, 128), 1.0 / TASKS, F32) for _ in range(TASKS)]
    for _ in range(SOLVER_STEPS):
        raised = []
        for t in range(TASKS):
            pull = (m[t, 0] * al[0] + m[t, 1] * al[1]) + (m[t, 2] * al[2] + m[t, 3] * al[3])
            raised.append(al[t] * jnp.exp(-pull / step_scale))
        norm = (raised[0] + raised[1]) + (raised[2] + raised[3])
        al = [r / norm for r in raised]
    for t in range(TASKS):
        alpha_ref[t:t + 1, :] = al[t]

    for c in range(DIM // 128):
        cols = slice(128 * c, 128 * c + 128)
        comb = al[0] * acc1[0, :, cols]
        for t in range(1, TASKS):
            comb = comb + al[t] * acc1[t, :, cols]
        gsend[cols, :] = comb.T

    def o_copy(s):
        dev = peer(s)
        rows = pl.ds(pl.multiple_of(dev * FEAT, FEAT), FEAT)
        return remote(gsend.at[rows, :], gx.at[me], o_send.at[s], o_recv.at[s], dev)

    order = (2, 4, 3, 5, 6, 7, 1)
    for s in order:
        o_copy(s).start()

    for c in range(DIM // 128):
        cols = slice(128 * c, 128 * c + 128)
        comb = al[0] * acc2[0, :, cols]
        for t in range(1, TASKS):
            comb = comb + al[t] * acc2[t, :, cols]
        stage2[pl.ds(c, HID, stride=DIM // 128), :] = comb

    gx[me] = gsend[pl.ds(pl.multiple_of(me * FEAT, FEAT), FEAT), :]
    for s in range(1, NUM_DEV):
        o_copy(s).wait_recv()

    swap_copy().wait_send()
    for m in range(2, NUM_DEV):
        hops[m]().wait_send()
        hand(m).wait_send()
    for s in range(1, NUM_DEV):
        e_copy(s).wait_send()
        c_copy(s).wait_send()
        gram_copy(s, me).wait_send()
        o_copy(s).wait_send()


PER = HID // 128
FLAT = DIM * HIDDEN // NUM_DEV // 128
HALF = FEAT // 2


def finish(alpha_in, blocks, stage2, alpha_ref, out1_hbm, out2_hbm, stage1, out_sem):
    stores = [pltpu.make_async_copy(stage2, out2_hbm, out_sem.at[2])]
    stores[0].start()
    for t in range(TASKS):
        alpha_ref[t] = jnp.max(alpha_in[t:t + 1, :])
    for h in range(2):
        for d in range(NUM_DEV):
            for b in range(PER):
                first = h * HALF * (HIDDEN // 128) + d * PER + b
                stage1[pl.ds(first, HALF, stride=HIDDEN // 128), :] = blocks[d, h * HALF:h * HALF + HALF, 128 * b:128 * b + 128]
        rows = pl.ds(h * FLAT // 2, FLAT // 2)
        stores.append(pltpu.make_async_copy(stage1.at[rows, :], out1_hbm.at[rows, :], out_sem.at[h]))
        stores[-1].start()
    for c in stores:
        c.wait()


def solution(mesh):
    def local_step(x_loc, w_in, w_out, heads, lab_loc, mask_loc):
        hbm = pl.BlockSpec(memory_space=pl.ANY)
        vmem = pl.BlockSpec(memory_space=pltpu.VMEM)
        sem = pltpu.SemaphoreType.DMA((NUM_DEV,))
        v = pltpu.VMEM
        alpha, gx, g2 = pl.pallas_call(
            kernel,
            out_shape=(
                v((TASKS, 128), F32),
                v((NUM_DEV, FEAT, HID), F32),
                v((FLAT, 128), F32),
            ),
            in_specs=[hbm, hbm, hbm, vmem, vmem, vmem],
            out_specs=(vmem, vmem, vmem),
            scratch_shapes=[
                v((NUM_DEV, TOK, DIM), BF16),
                v((NCHUNK, DIM, CHUNK), BF16),
                v((NCHUNK, CHUNK, DIM), BF16),
                v((DIM, HID), BF16),
                v((HID, DIM), BF16),
                v((HID, DIM), BF16),
                v((ROWS, CHUNK), BF16),
                v((ROWS, CHUNK), BF16),
                v((TOK, DIM), F32),
                v((HEAD_ROWS, DIM), F32),
                v((TASKS * CLASSES, DIM, 128), F32),
                v((HEAD_ROWS, TOK), F32),
                v((NUM_DEV, HEAD_ROWS, TOK), BF16),
                v((2, TASKS, 8, TOK), F32),
                v((HID, TOK), BF16),
                v((HID, TOK), BF16),
                v((HID, TOK), F32),
                v((HID, TOK), F32),
                v((DIM, TOK), BF16),
                v((DIM, TOK), BF16),
                v((HID, TOK), BF16),
                v((HID, TOK), BF16),
                v((TASKS, HID, DIM), F32),
                v((TASKS, HID, DIM), F32),
                v((NUM_DEV, 8, 128), F32),
                v((8, DIM), F32),
                v((NUM_DEV, 16, 128), F32),
                v((DIM, HID), F32),
                sem, sem, sem, sem, sem, sem, sem, sem, sem, sem, sem, sem,
                pltpu.SemaphoreType.DMA((3 + 2 * NCHUNK,)),
            ],
            compiler_params=pltpu.CompilerParams(collective_id=0, has_side_effects=True, vmem_limit_bytes=62_000_000),
            name="trunk",
        )(x_loc, w_in, w_out, heads.transpose(2, 0, 1), lab_loc, mask_loc)
        smem = pl.BlockSpec(memory_space=pltpu.SMEM)
        alpha, out1, out2 = pl.pallas_call(
            finish,
            out_shape=(
                jax.ShapeDtypeStruct((TASKS,), F32),
                jax.ShapeDtypeStruct((FLAT, 128), F32),
                jax.ShapeDtypeStruct((FLAT, 128), F32),
            ),
            in_specs=[vmem, vmem, vmem],
            out_specs=(smem, hbm, hbm),
            scratch_shapes=[
                v((FLAT, 128), F32),
                pltpu.SemaphoreType.DMA((3,)),
            ],
            compiler_params=pltpu.CompilerParams(vmem_limit_bytes=8_000_000),
            name="finish",
        )(alpha, gx, g2)
        return alpha, out1.reshape(-1), out2.reshape(-1)

    return jax.shard_map(local_step, mesh=mesh, in_specs=(P("data", None), P(), P(), P(), P(None, "data"), P(None, "data")), out_specs=(P(), P("data"), P("data")), check_vma=False)
```

```python
import jax
import jax.numpy as jnp
from jax import lax
from jax.experimental import pallas as pl
from jax.experimental.pallas import tpu as pltpu
from jax.sharding import PartitionSpec as P

SOLVER_STEPS = 20
MESH = pl.DeviceIdType.MESH
F32, BF16 = jnp.float32, jnp.bfloat16
NUM_DEV = 8
TASKS = 4
CLASSES = 3
TOK = 1024
DIM = 768
HIDDEN = 3072
HID = HIDDEN // NUM_DEV
FEAT = DIM // NUM_DEV
HEAD_ROWS = 32
CHUNK = 768
ROWS = 512
NCHUNK = HIDDEN // CHUNK
QUARTER = TOK // TASKS
PAIRS = [(t, s) for t in range(TASKS) for s in range(t, TASKS)]
GELU_C = 0.7978845608028654
GELU_K = 0.044715


def dot_nn(a, b):
    return lax.dot_general(a, b, (((1,), (0,)), ((), ())), preferred_element_type=F32)


def dot_nt(a, b):
    return lax.dot_general(a, b, (((1,), (1,)), ((), ())), preferred_element_type=F32)


def lanes(row, width):
    return jnp.concatenate([row] * (width // row.shape[1]), axis=1)


def gelu_parts(p):
    a = (GELU_C * GELU_K) * (p * p)
    th = jnp.tanh(p * (a + GELU_C))
    return a, th, 0.5 + 0.5 * th


def gelu_value(p):
    return p * gelu_parts(p)[2]


def gelu_both(p):
    a, th, cdf = gelu_parts(p)
    slope = cdf + ((1.0 - th * th) * p) * (1.5 * a + 0.5 * GELU_C)
    return p * cdf, slope


def kernel(x_hbm, w_in_hbm, w_out_hbm, head_ref, lab_ref, mask_ref, alpha_ref, gx, stage2,
           xs, w1, w2, w1j, w1t, w2j, abuf0, abuf1, zacc, hrow, hbc, ef, es, ecur, act0, act1, slope0, slope1,
           dz0, dz1, q0, q1, acc1, acc2, cnt, inv, gram, gsend,
           x_send, x_recv, f_send, f_recv, e_send, e_recv, c_send, c_recv, g_send, g_recv, o_send, o_recv, l_sem):
    me = lax.axis_index("data")
    core = lax.rem(me, 2)
    cx = lax.rem(lax.div(me, 2), 2)
    cy = lax.div(me, 4)

    def flip(v, b):
        return v + b - 2 * v * b

    def peer(s):
        return flip(cx, s // 2 % 2) * 2 + flip(cy, s // 4) * 4 + flip(core, jnp.int32(s % 2))

    def remote(src, dst, send, recv, dev):
        return pltpu.make_async_remote_copy(src_ref=src, dst_ref=dst, send_sem=send, recv_sem=recv, device_id=(dev,), device_id_type=MESH)

    half = pl.ds(pl.multiple_of(core * ROWS, ROWS), ROWS)
    x_dev, y_dev = peer(2), peer(4)
    first_dev = core * y_dev + (1 - core) * x_dev
    second_dev = core * x_dev + (1 - core) * y_dev

    def swap_copy():
        return remote(xs.at[0], xs.at[1], x_send.at[1], x_recv.at[1], peer(1))

    def hop(src, dst, i, dev):
        return remote(xs.at[src, half, :], xs.at[dst, half, :], x_send.at[i], x_recv.at[dst], dev)

    def arrived(m):
        return hop(0, m, 2, x_dev)

    hops = {
        2: lambda: hop(0, 2 + core, 2, first_dev),
        3: lambda: hop(1, 3 - core, 3, second_dev),
        4: lambda: hop(1, 4 + core, 4, first_dev),
        5: lambda: hop(0, 5 - core, 5, second_dev),
        6: lambda: hop(2 + 3 * core, 6, 6, second_dev),
        7: lambda: hop(4 - core, 7, 7, second_dev),
    }

    def hand(m):
        return remote(xs.at[m, half, :], xs.at[m, half, :], f_send.at[m], f_recv.at[m], peer(1))

    def arrival_slot(s):
        bx, by = s // 2 % 2, s // 4
        return 6 + core if bx and by else 2 + 2 * core if bx else 5 - 2 * core if by else 1

    def e_copy(s):
        slot = arrival_slot(s)
        return remote(es.at[0], es.at[slot], e_send.at[s], e_recv.at[slot], peer(s))

    def e_arrived(slot):
        return remote(es.at[0], es.at[slot], e_send.at[1], e_recv.at[slot], peer(1))

    def c_copy(s):
        return remote(cnt.at[0], cnt.at[s], c_send.at[s], c_recv.at[s], peer(s))

    def local(src, dst, i):
        return pltpu.make_async_copy(src, dst, l_sem.at[i])

    def load_w1(i):
        return local(w_in_hbm.at[:, pl.ds(pl.multiple_of(CHUNK * i, CHUNK), CHUNK)], w1.at[i], 3 + i)

    def load_w2(i):
        return local(w_out_hbm.at[pl.ds(pl.multiple_of(CHUNK * i, CHUNK), CHUNK), :], w2.at[i], 3 + NCHUNK + i)

    load_x = local(x_hbm, xs.at[0], 0)
    load_w1j = local(w_in_hbm.at[:, pl.ds(pl.multiple_of(me * HID, HID), HID)], w1j, 1)
    load_w2j = local(w_out_hbm.at[pl.ds(pl.multiple_of(me * HID, HID), HID), :], w2j, 2)
    load_x.start()
    load_w1j.start()
    load_w1(0).start()
    load_w2(0).start()

    barrier = pltpu.get_barrier_semaphore()
    for s in range(1, NUM_DEV):
        pl.semaphore_signal(barrier, inc=1, device_id=(peer(s),), device_id_type=MESH)

    counts = jnp.sum(mask_ref[...].astype(F32), axis=1, keepdims=True)
    cnt[0, 0:TASKS, :] = jnp.broadcast_to(counts, (TASKS, 128))
    cnt[0, TASKS:8, :] = jnp.zeros((8 - TASKS, 128), F32)
    hrow[...] = jnp.zeros_like(hrow)
    for c in range(CLASSES):
        hrow[8 * c:8 * c + TASKS, :] = head_ref[c].astype(F32)
    head = hrow[...].astype(BF16)

    block = lax.div(lax.broadcasted_iota(jnp.int32, (HEAD_ROWS, TASKS * CLASSES * 128), 1), 128)
    pick = lax.rem(block, CLASSES) * 8 + lax.div(block, CLASSES)
    ones = (lax.broadcasted_iota(jnp.int32, block.shape, 0) == pick).astype(F32).astype(BF16)
    wide = dot_nn(hrow[...].T.astype(BF16), ones)
    for k in range(TASKS * CLASSES):
        hbc[k] = wide[:, 128 * k:128 * k + 128]
    pl.semaphore_wait(barrier, NUM_DEV - 1)
    load_x.wait()
    hops[2]().start()
    swap_copy().start()
    for s in range(1, NUM_DEV):
        c_copy(s).start()
    for i in range(1, NCHUNK):
        load_w1(i).start()
        load_w2(i).start()
    load_w2j.start()

    load_w1j.wait()
    w1t[...] = w1j[...].astype(F32).T.astype(BF16)

    abuf1[...] = jnp.zeros_like(abuf1)
    zacc[...] = xs[0].astype(F32)
    half0, half1 = slice(0, ROWS), slice(ROWS, TOK)

    acts, slopes, dzs, qs = (act0, act1), (slope0, slope1), (dz0, dz1), (q0, q1)

    def preact(slot, part, quarter):
        r = pl.ds(pl.multiple_of(quarter * QUARTER, QUARTER), QUARTER)
        a, sl = gelu_both(dot_nt(w1t[...], xs[slot, r, :]))
        acts[part][:, r] = a.astype(BF16)
        slopes[part][:, r] = sl

    def forward(h, carry):
        load_w1(h).wait()
        load_w2(h).wait()
        acc1[h] = jnp.zeros((HID, DIM), F32)
        acc2[h] = jnp.zeros((HID, DIM), F32)
        @pl.when(h == 1)
        def _():
            swap_copy().wait_recv()
            hops[3]().start()

        abuf0[...] = gelu_value(dot_nn(xs[0, half0, :], w1[h])).astype(BF16)
        zacc[half1, :] += dot_nn(abuf1[...], w2[jnp.maximum(h - 1, 0)])
        abuf1[...] = gelu_value(dot_nn(xs[0, half1, :], w1[h])).astype(BF16)
        zacc[half0, :] += dot_nn(abuf0[...], w2[h])
        preact(0, 0, h)
        return carry

    lax.fori_loop(0, NCHUNK, forward, 0)
    zacc[half1, :] += dot_nn(abuf1[...], w2[NCHUNK - 1])

    for r in range(TOK // ROWS):
        cols = slice(r * ROWS, (r + 1) * ROWS)
        logits = dot_nt(head, zacc[cols, :].astype(BF16))
        l = [logits[8 * c:8 * c + TASKS] for c in range(CLASSES)]
        top = jnp.maximum(jnp.maximum(l[0], l[1]), l[2])
        ex = [jnp.exp(v - top) for v in l]
        total = ex[0] + ex[1] + ex[2]
        lab = lab_ref[:, cols]
        m = mask_ref[:, cols].astype(F32)
        for c in range(CLASSES):
            err = m * (ex[c] / total - (lab == c).astype(F32))
            for t in range(TASKS):
                ef[8 * t + c:8 * t + c + 1, cols] = err[t:t + 1]
    for t in range(TASKS):
        ef[8 * t + CLASSES:8 * t + 8, :] = jnp.zeros((8 - CLASSES, TOK), F32)
    es[0] = ef[...].astype(BF16)
    for t in range(TASKS):
        ecur[0, t] = es[0, 8 * t:8 * t + 8, :].astype(F32)

    def make_dz(dst, part, t):
        e = ecur[part, t]
        rows = [jnp.broadcast_to(e[c:c + 1, :], (8, TOK)) for c in range(CLASSES)]
        for k in range(DIM // 8):
            f = slice(8 * k, 8 * k + 8)
            h = [lanes(hbc[CLASSES * t + c, f, :], TOK) for c in range(CLASSES)]
            dst[f, :] = (h[0] * rows[0] + h[1] * rows[1] + h[2] * rows[2]).astype(BF16)

    for s in range(1, NUM_DEV):
        e_copy(s).start()
    make_dz(dz0, 0, 0)
    load_w2j.wait()
    total_cnt = cnt[0]
    for s in range(1, NUM_DEV):
        c_copy(s).wait_recv()
        total_cnt = total_cnt + cnt[s]
    inv[...] = lanes(1.0 / jnp.maximum(total_cnt, 1.0), DIM)

    def link_half_ready(s):
        for k, slots in ((1, (2, 3)), (3, (4, 5)), (5, (6,)), (6, (7,))):
            @pl.when(s == k)
            def _():
                for m in slots:
                    arrived(m).wait_recv()
                    hand(m).start()
                if k == 3:
                    hops[6]().start()
                    hops[7]().start()

    def other_half_ready(s):
        for m in range(2, NUM_DEV):
            @pl.when(s == m - 1)
            def _():
                hand(m).wait_recv()

        @pl.when(s == 0)
        def _():
            hops[4]().start()
            hops[5]().start()

    def errors_ready(s, part):
        for k in range(1, NUM_DEV):
            @pl.when(s == k - 1)
            def _():
                e_arrived(k).wait_recv()
                for t in range(TASKS):
                    ecur[part, t] = es[k, 8 * t:8 * t + 8, :].astype(F32)

    def run_task(s, part, t, j, next_part, next_t):
        nxt = jnp.minimum(s + 1, NUM_DEV - 1)
        scale = inv[pl.ds(t, 1), :]
        qs[j][...] = (dot_nn(w2j[...], dzs[j][...]) * slopes[part][...]).astype(BF16)
        acc2[t] += (dot_nt(acts[part][...], dzs[j][...]) * scale).astype(BF16).astype(F32)
        make_dz(dzs[1 - j], next_part, next_t)
        preact(nxt, 1 - part, lax.rem(t + 2 * core, TASKS))
        acc1[t] += (dot_nn(qs[j][...], xs[s]) * scale).astype(BF16).astype(F32)

    def shard_pair(sp, carry):
        for part in range(2):
            s = 2 * sp + part
            link_half_ready(s)

            def task_pair(tp, c):
                @pl.when(tp == 1)
                def _():
                    errors_ready(s, 1 - part)
                    other_half_ready(s)

                run_task(s, part, 2 * tp, 0, part, 2 * tp + 1)
                wrap = lax.div(2 * tp + 2, TASKS)
                run_task(s, part, 2 * tp + 1, 1, part + wrap * (1 - 2 * part), 2 * tp + 2 - TASKS * wrap)
                return c

            lax.fori_loop(0, TASKS // 2, task_pair, 0)
        return carry

    lax.fori_loop(0, NUM_DEV // 2, shard_pair, 0)

    def gram_rows(i, sums):
        r = pl.ds(pl.multiple_of(i * 8, 8), 8)
        out = list(sums)
        for acc in (acc1, acc2):
            for c in range(DIM // 128):
                g = [acc[t, r, 128 * c:128 * c + 128] for t in range(TASKS)]
                for k, (t, u) in enumerate(PAIRS):
                    out[k] = out[k] + g[t] * g[u]
        return tuple(out)

    sums = lax.fori_loop(0, HID // 8, gram_rows, tuple(jnp.zeros((8, 128), F32) for _ in PAIRS))
    for k in range(len(PAIRS)):
        gram[me, k:k + 1, :] = jnp.broadcast_to(jnp.sum(sums[k]), (1, 128))
    gram[me, len(PAIRS):16, :] = jnp.zeros((16 - len(PAIRS), 128), F32)

    def gram_copy(s, block):
        return remote(gram.at[block], gram.at[block], g_send.at[s], g_recv.at[s], peer(s))

    for s in range(1, NUM_DEV):
        gram_copy(s, me).start()
    for s in range(1, NUM_DEV):
        gram_copy(s, me).wait_recv()
    gram_sum = gram[0]
    for d in range(1, NUM_DEV):
        gram_sum = gram_sum + gram[d]
    m = {}
    for k, (t, u) in enumerate(PAIRS):
        m[t, u] = m[u, t] = gram_sum[k:k + 1, :]
    step_scale = (m[0, 0] + m[1, 1] + m[2, 2] + m[3, 3]) / TASKS
    al = [jnp.full((1, 128), 1.0 / TASKS, F32) for _ in range(TASKS)]
    for _ in range(SOLVER_STEPS):
        raised = []
        for t in range(TASKS):
            pull = (m[t, 0] * al[0] + m[t, 1] * al[1]) + (m[t, 2] * al[2] + m[t, 3] * al[3])
            raised.append(al[t] * jnp.exp(-pull / step_scale))
        norm = (raised[0] + raised[1]) + (raised[2] + raised[3])
        al = [r / norm for r in raised]
    for t in range(TASKS):
        alpha_ref[t:t + 1, :] = al[t]

    for c in range(DIM // 128):
        cols = slice(128 * c, 128 * c + 128)
        comb = al[0] * acc1[0, :, cols]
        for t in range(1, TASKS):
            comb = comb + al[t] * acc1[t, :, cols]
        gsend[cols, :] = comb.T

    def o_copy(s):
        dev = peer(s)
        rows = pl.ds(pl.multiple_of(dev * FEAT, FEAT), FEAT)
        return remote(gsend.at[rows, :], gx.at[me], o_send.at[s], o_recv.at[s], dev)

    order = (2, 4, 3, 5, 6, 7, 1)
    for s in order:
        o_copy(s).start()

    for c in range(DIM // 128):
        cols = slice(128 * c, 128 * c + 128)
        comb = al[0] * acc2[0, :, cols]
        for t in range(1, TASKS):
            comb = comb + al[t] * acc2[t, :, cols]
        stage2[pl.ds(c, HID, stride=DIM // 128), :] = comb

    gx[me] = gsend[pl.ds(pl.multiple_of(me * FEAT, FEAT), FEAT), :]
    for s in range(1, NUM_DEV):
        o_copy(s).wait_recv()

    swap_copy().wait_send()
    for m in range(2, NUM_DEV):
        hops[m]().wait_send()
        hand(m).wait_send()
    for s in range(1, NUM_DEV):
        e_copy(s).wait_send()
        c_copy(s).wait_send()
        gram_copy(s, me).wait_send()
        o_copy(s).wait_send()


PER = HID // 128
FLAT = DIM * HIDDEN // NUM_DEV // 128
HALF = FEAT // 2


def finish(alpha_in, blocks, stage2, alpha_ref, out1_hbm, out2_hbm, stage1, out_sem):
    stores = [pltpu.make_async_copy(stage2, out2_hbm, out_sem.at[2])]
    stores[0].start()
    for t in range(TASKS):
        alpha_ref[t] = jnp.max(alpha_in[t:t + 1, :])
    for h in range(2):
        for d in range(NUM_DEV):
            for b in range(PER):
                first = h * HALF * (HIDDEN // 128) + d * PER + b
                stage1[pl.ds(first, HALF, stride=HIDDEN // 128), :] = blocks[d, h * HALF:h * HALF + HALF, 128 * b:128 * b + 128]
        rows = pl.ds(h * FLAT // 2, FLAT // 2)
        stores.append(pltpu.make_async_copy(stage1.at[rows, :], out1_hbm.at[rows, :], out_sem.at[h]))
        stores[-1].start()
    for c in stores:
        c.wait()


def solution(mesh):
    def local_step(x_loc, w_in, w_out, heads, lab_loc, mask_loc):
        hbm = pl.BlockSpec(memory_space=pl.ANY)
        vmem = pl.BlockSpec(memory_space=pltpu.VMEM)
        sem = pltpu.SemaphoreType.DMA((NUM_DEV,))
        v = pltpu.VMEM
        alpha, gx, g2 = pl.pallas_call(
            kernel,
            out_shape=(
                v((TASKS, 128), F32),
                v((NUM_DEV, FEAT, HID), F32),
                v((FLAT, 128), F32),
            ),
            in_specs=[hbm, hbm, hbm, vmem, vmem, vmem],
            out_specs=(vmem, vmem, vmem),
            scratch_shapes=[
                v((NUM_DEV, TOK, DIM), BF16),
                v((NCHUNK, DIM, CHUNK), BF16),
                v((NCHUNK, CHUNK, DIM), BF16),
                v((DIM, HID), BF16),
                v((HID, DIM), BF16),
                v((HID, DIM), BF16),
                v((ROWS, CHUNK), BF16),
                v((ROWS, CHUNK), BF16),
                v((TOK, DIM), F32),
                v((HEAD_ROWS, DIM), F32),
                v((TASKS * CLASSES, DIM, 128), F32),
                v((HEAD_ROWS, TOK), F32),
                v((NUM_DEV, HEAD_ROWS, TOK), BF16),
                v((2, TASKS, 8, TOK), F32),
                v((HID, TOK), BF16),
                v((HID, TOK), BF16),
                v((HID, TOK), F32),
                v((HID, TOK), F32),
                v((DIM, TOK), BF16),
                v((DIM, TOK), BF16),
                v((HID, TOK), BF16),
                v((HID, TOK), BF16),
                v((TASKS, HID, DIM), F32),
                v((TASKS, HID, DIM), F32),
                v((NUM_DEV, 8, 128), F32),
                v((8, DIM), F32),
                v((NUM_DEV, 16, 128), F32),
                v((DIM, HID), F32),
                sem, sem, sem, sem, sem, sem, sem, sem, sem, sem, sem, sem,
                pltpu.SemaphoreType.DMA((3 + 2 * NCHUNK,)),
            ],
            compiler_params=pltpu.CompilerParams(collective_id=0, has_side_effects=True, vmem_limit_bytes=62_000_000),
            name="trunk",
        )(x_loc, w_in, w_out, heads.transpose(2, 0, 1), lab_loc, mask_loc)
        smem = pl.BlockSpec(memory_space=pltpu.SMEM)
        alpha, out1, out2 = pl.pallas_call(
            finish,
            out_shape=(
                jax.ShapeDtypeStruct((TASKS,), F32),
                jax.ShapeDtypeStruct((FLAT, 128), F32),
                jax.ShapeDtypeStruct((FLAT, 128), F32),
            ),
            in_specs=[vmem, vmem, vmem],
            out_specs=(smem, hbm, hbm),
            scratch_shapes=[
                v((FLAT, 128), F32),
                pltpu.SemaphoreType.DMA((3,)),
            ],
            compiler_params=pltpu.CompilerParams(vmem_limit_bytes=8_000_000),
            name="finish",
        )(alpha, gx, g2)
        return alpha, out1.reshape(-1), out2.reshape(-1)

    return jax.shard_map(local_step, mesh=mesh, in_specs=(P("data", None), P(), P(), P(), P(None, "data"), P(None, "data")), out_specs=(P(), P("data"), P("data")), check_vma=False)
```

```python
import jax
import jax.numpy as jnp
from jax import lax
from jax.experimental import pallas as pl
from jax.experimental.pallas import tpu as pltpu
from jax.sharding import PartitionSpec as P

SOLVER_STEPS = 20
MESH = pl.DeviceIdType.MESH
F32, BF16 = jnp.float32, jnp.bfloat16
NUM_DEV = 8
TASKS = 4
CLASSES = 3
TOK = 1024
DIM = 768
HIDDEN = 3072
HID = HIDDEN // NUM_DEV
FEAT = DIM // NUM_DEV
HEAD_ROWS = 32
PITCH = TOK + 128
CHUNK = 768
ROWS = 512
NCHUNK = HIDDEN // CHUNK
QUARTER = TOK // TASKS
PAIRS = [(t, s) for t in range(TASKS) for s in range(t, TASKS)]
GELU_C = 0.7978845608028654
GELU_K = 0.044715


def dot_nn(a, b):
    return lax.dot_general(a, b, (((1,), (0,)), ((), ())), preferred_element_type=F32)


def dot_nt(a, b):
    return lax.dot_general(a, b, (((1,), (1,)), ((), ())), preferred_element_type=F32)


def lanes(row, width):
    return jnp.concatenate([row] * (width // row.shape[1]), axis=1)


def gelu_parts(p):
    a = (GELU_C * GELU_K) * (p * p)
    th = jnp.tanh(p * (a + GELU_C))
    return a, th, 0.5 + 0.5 * th


def gelu_value(p):
    return p * gelu_parts(p)[2]


def gelu_both(p):
    a, th, cdf = gelu_parts(p)
    slope = cdf + ((1.0 - th * th) * p) * (1.5 * a + 0.5 * GELU_C)
    return p * cdf, slope


def kernel(x_hbm, w_in_hbm, w_out_hbm, head_ref, lab_ref, mask_ref, alpha_ref, gx, stage2,
           xs, w1, w2, w1j, w1t, w2j, abuf0, abuf1, zacc, hrow, hbc, ef, es, ecur, act0, act1, slope0, slope1,
           dz0, dz1, q0, q1, acc1, acc2, cnt, inv, gram, gsend,
           x_send, x_recv, f_send, f_recv, e_send, e_recv, c_send, c_recv, g_send, g_recv, o_send, o_recv, l_sem):
    me = lax.axis_index("data")
    core = lax.rem(me, 2)
    cx = lax.rem(lax.div(me, 2), 2)
    cy = lax.div(me, 4)

    def flip(v, b):
        return v + b - 2 * v * b

    def peer(s):
        return flip(cx, s // 2 % 2) * 2 + flip(cy, s // 4) * 4 + flip(core, jnp.int32(s % 2))

    def remote(src, dst, send, recv, dev):
        return pltpu.make_async_remote_copy(src_ref=src, dst_ref=dst, send_sem=send, recv_sem=recv, device_id=(dev,), device_id_type=MESH)

    half = pl.ds(pl.multiple_of(core * ROWS, ROWS), ROWS)
    x_dev, y_dev = peer(2), peer(4)
    first_dev = core * y_dev + (1 - core) * x_dev
    second_dev = core * x_dev + (1 - core) * y_dev

    def swap_copy():
        return remote(xs.at[0], xs.at[1], x_send.at[1], x_recv.at[1], peer(1))

    def hop(src, dst, i, dev):
        return remote(xs.at[src, half, :], xs.at[dst, half, :], x_send.at[i], x_recv.at[dst], dev)

    def arrived(m):
        return hop(0, m, 2, x_dev)

    hops = {
        2: lambda: hop(0, 2 + core, 2, first_dev),
        3: lambda: hop(1, 3 - core, 3, second_dev),
        4: lambda: hop(1, 4 + core, 4, first_dev),
        5: lambda: hop(0, 5 - core, 5, second_dev),
        6: lambda: hop(2 + 3 * core, 6, 6, second_dev),
        7: lambda: hop(4 - core, 7, 7, second_dev),
    }

    def hand(m):
        return remote(xs.at[m, half, :], xs.at[m, half, :], f_send.at[m], f_recv.at[m], peer(1))

    def arrival_slot(s):
        bx, by = s // 2 % 2, s // 4
        return 6 + core if bx and by else 2 + 2 * core if bx else 5 - 2 * core if by else 1

    def e_copy(s):
        slot = arrival_slot(s)
        return remote(es.at[0], es.at[slot], e_send.at[s], e_recv.at[slot], peer(s))

    def e_arrived(slot):
        return remote(es.at[0], es.at[slot], e_send.at[1], e_recv.at[slot], peer(1))

    def c_copy(s):
        return remote(cnt.at[0], cnt.at[s], c_send.at[s], c_recv.at[s], peer(s))

    def local(src, dst, i):
        return pltpu.make_async_copy(src, dst, l_sem.at[i])

    def load_w1(i):
        return local(w_in_hbm.at[:, pl.ds(pl.multiple_of(CHUNK * i, CHUNK), CHUNK)], w1.at[i], 3 + i)

    def load_w2(i):
        return local(w_out_hbm.at[pl.ds(pl.multiple_of(CHUNK * i, CHUNK), CHUNK), :], w2.at[i], 3 + NCHUNK + i)

    load_x = local(x_hbm, xs.at[0], 0)
    load_w1j = local(w_in_hbm.at[:, pl.ds(pl.multiple_of(me * HID, HID), HID)], w1j, 1)
    load_w2j = local(w_out_hbm.at[pl.ds(pl.multiple_of(me * HID, HID), HID), :], w2j, 2)
    load_x.start()
    load_w1j.start()
    load_w1(0).start()
    load_w2(0).start()

    barrier = pltpu.get_barrier_semaphore()
    for s in range(1, NUM_DEV):
        pl.semaphore_signal(barrier, inc=1, device_id=(peer(s),), device_id_type=MESH)

    counts = jnp.sum(mask_ref[...].astype(F32), axis=1, keepdims=True)
    cnt[0, 0:TASKS, :] = jnp.broadcast_to(counts, (TASKS, 128))
    cnt[0, TASKS:8, :] = jnp.zeros((8 - TASKS, 128), F32)
    hrow[...] = jnp.zeros_like(hrow)
    for c in range(CLASSES):
        hrow[8 * c:8 * c + TASKS, :] = head_ref[c].astype(F32)
    head = hrow[...].astype(BF16)

    block = lax.div(lax.broadcasted_iota(jnp.int32, (HEAD_ROWS, TASKS * CLASSES * 128), 1), 128)
    pick = lax.rem(block, CLASSES) * 8 + lax.div(block, CLASSES)
    ones = (lax.broadcasted_iota(jnp.int32, block.shape, 0) == pick).astype(F32).astype(BF16)
    wide = dot_nn(hrow[...].T.astype(BF16), ones)
    for k in range(TASKS * CLASSES):
        hbc[k] = wide[:, 128 * k:128 * k + 128]
    pl.semaphore_wait(barrier, NUM_DEV - 1)
    load_x.wait()
    hops[2]().start()
    swap_copy().start()
    for s in range(1, NUM_DEV):
        c_copy(s).start()
    for i in range(1, NCHUNK):
        load_w1(i).start()
        load_w2(i).start()
    load_w2j.start()

    load_w1j.wait()
    w1t[...] = w1j[...].astype(F32).T.astype(BF16)

    abuf1[...] = jnp.zeros_like(abuf1)
    zacc[...] = xs[0].astype(F32)
    half0, half1 = slice(0, ROWS), slice(ROWS, TOK)

    acts, slopes, dzs, qs = (act0, act1), (slope0, slope1), (dz0, dz1), (q0, q1)

    def preact(slot, part, quarter):
        r = pl.ds(pl.multiple_of(quarter * QUARTER, QUARTER), QUARTER)
        a, sl = gelu_both(dot_nt(w1t[...], xs[slot, r, :]))
        acts[part][:, r] = a.astype(BF16)
        slopes[part][:, r] = sl

    def forward(h, carry):
        load_w1(h).wait()
        load_w2(h).wait()
        acc1[h] = jnp.zeros((HID, DIM), F32)
        acc2[h] = jnp.zeros((HID, DIM), F32)
        @pl.when(h == 1)
        def _():
            swap_copy().wait_recv()
            hops[3]().start()

        abuf0[...] = gelu_value(dot_nn(xs[0, half0, :], w1[h])).astype(BF16)
        zacc[half1, :] += dot_nn(abuf1[...], w2[jnp.maximum(h - 1, 0)])
        abuf1[...] = gelu_value(dot_nn(xs[0, half1, :], w1[h])).astype(BF16)
        zacc[half0, :] += dot_nn(abuf0[...], w2[h])
        preact(0, 0, h)
        return carry

    lax.fori_loop(0, NCHUNK, forward, 0)
    zacc[half1, :] += dot_nn(abuf1[...], w2[NCHUNK - 1])

    for r in range(TOK // ROWS):
        cols = slice(r * ROWS, (r + 1) * ROWS)
        logits = dot_nt(head, zacc[cols, :].astype(BF16))
        l = [logits[8 * c:8 * c + TASKS] for c in range(CLASSES)]
        top = jnp.maximum(jnp.maximum(l[0], l[1]), l[2])
        ex = [jnp.exp(v - top) for v in l]
        total = ex[0] + ex[1] + ex[2]
        lab = lab_ref[:, cols]
        m = mask_ref[:, cols].astype(F32)
        for c in range(CLASSES):
            err = m * (ex[c] / total - (lab == c).astype(F32))
            for t in range(TASKS):
                ef[8 * t + c:8 * t + c + 1, cols] = err[t:t + 1]
    for t in range(TASKS):
        ef[8 * t + CLASSES:8 * t + 8, :] = jnp.zeros((8 - CLASSES, TOK), F32)
    es[0] = ef[...].astype(BF16)
    for t in range(TASKS):
        ecur[0, t] = es[0, 8 * t:8 * t + 8, :].astype(F32)

    def make_dz(dst, part, t):
        e = ecur[part, t]
        rows = [jnp.broadcast_to(e[c:c + 1, :], (8, TOK)) for c in range(CLASSES)]
        for k in range(DIM // 8):
            f = slice(8 * k, 8 * k + 8)
            h = [lanes(hbc[CLASSES * t + c, f, :], TOK) for c in range(CLASSES)]
            dst[f, 0:TOK] = (h[0] * rows[0] + h[1] * rows[1] + h[2] * rows[2]).astype(BF16)

    for s in range(1, NUM_DEV):
        e_copy(s).start()
    make_dz(dz0, 0, 0)
    load_w2j.wait()
    total_cnt = cnt[0]
    for s in range(1, NUM_DEV):
        c_copy(s).wait_recv()
        total_cnt = total_cnt + cnt[s]
    inv[...] = lanes(1.0 / jnp.maximum(total_cnt, 1.0), DIM)

    def link_half_ready(s):
        for k, slots in ((1, (2, 3)), (3, (4, 5)), (5, (6,)), (6, (7,))):
            @pl.when(s == k)
            def _():
                for m in slots:
                    arrived(m).wait_recv()
                    hand(m).start()
                if k == 3:
                    hops[6]().start()
                    hops[7]().start()

    def other_half_ready(s):
        for m in range(2, NUM_DEV):
            @pl.when(s == m - 1)
            def _():
                hand(m).wait_recv()

        @pl.when(s == 0)
        def _():
            hops[4]().start()
            hops[5]().start()

    def errors_ready(s, part):
        for k in range(1, NUM_DEV):
            @pl.when(s == k - 1)
            def _():
                e_arrived(k).wait_recv()
                for t in range(TASKS):
                    ecur[part, t] = es[k, 8 * t:8 * t + 8, :].astype(F32)

    def run_task(s, part, t, j, next_part, next_t):
        nxt = jnp.minimum(s + 1, NUM_DEV - 1)
        scale = inv[pl.ds(t, 1), :]
        qs[j][:, 0:TOK] = (dot_nn(w2j[...], dzs[j][:, 0:TOK]) * slopes[part][...]).astype(BF16)
        acc2[t] += (dot_nt(acts[part][:, 0:TOK], dzs[j][:, 0:TOK]) * scale).astype(BF16).astype(F32)
        make_dz(dzs[1 - j], next_part, next_t)
        preact(nxt, 1 - part, lax.rem(t + 2 * core, TASKS))
        acc1[t] += (dot_nn(qs[j][:, 0:TOK], xs[s]) * scale).astype(BF16).astype(F32)

    def shard_pair(sp, carry):
        for part in range(2):
            s = 2 * sp + part
            link_half_ready(s)

            def task_pair(tp, c):
                @pl.when(tp == 1)
                def _():
                    errors_ready(s, 1 - part)
                    other_half_ready(s)

                run_task(s, part, 2 * tp, 0, part, 2 * tp + 1)
                wrap = lax.div(2 * tp + 2, TASKS)
                run_task(s, part, 2 * tp + 1, 1, part + wrap * (1 - 2 * part), 2 * tp + 2 - TASKS * wrap)
                return c

            lax.fori_loop(0, TASKS // 2, task_pair, 0)
        return carry

    lax.fori_loop(0, NUM_DEV // 2, shard_pair, 0)

    def gram_rows(i, sums):
        r = pl.ds(pl.multiple_of(i * 8, 8), 8)
        out = list(sums)
        for acc in (acc1, acc2):
            for c in range(DIM // 128):
                g = [acc[t, r, 128 * c:128 * c + 128] for t in range(TASKS)]
                for k, (t, u) in enumerate(PAIRS):
                    out[k] = out[k] + g[t] * g[u]
        return tuple(out)

    sums = lax.fori_loop(0, HID // 8, gram_rows, tuple(jnp.zeros((8, 128), F32) for _ in PAIRS))
    for k in range(len(PAIRS)):
        gram[me, k:k + 1, :] = jnp.broadcast_to(jnp.sum(sums[k]), (1, 128))
    gram[me, len(PAIRS):16, :] = jnp.zeros((16 - len(PAIRS), 128), F32)

    def gram_copy(s, block):
        return remote(gram.at[block], gram.at[block], g_send.at[s], g_recv.at[s], peer(s))

    for s in range(1, NUM_DEV):
        gram_copy(s, me).start()
    for s in range(1, NUM_DEV):
        gram_copy(s, me).wait_recv()
    gram_sum = gram[0]
    for d in range(1, NUM_DEV):
        gram_sum = gram_sum + gram[d]
    m = {}
    for k, (t, u) in enumerate(PAIRS):
        m[t, u] = m[u, t] = gram_sum[k:k + 1, :]
    step_scale = (m[0, 0] + m[1, 1] + m[2, 2] + m[3, 3]) / TASKS
    al = [jnp.full((1, 128), 1.0 / TASKS, F32) for _ in range(TASKS)]
    for _ in range(SOLVER_STEPS):
        raised = []
        for t in range(TASKS):
            pull = (m[t, 0] * al[0] + m[t, 1] * al[1]) + (m[t, 2] * al[2] + m[t, 3] * al[3])
            raised.append(al[t] * jnp.exp(-pull / step_scale))
        norm = (raised[0] + raised[1]) + (raised[2] + raised[3])
        al = [r / norm for r in raised]
    for t in range(TASKS):
        alpha_ref[t:t + 1, :] = al[t]

    for c in range(DIM // 128):
        cols = slice(128 * c, 128 * c + 128)
        comb = al[0] * acc1[0, :, cols]
        for t in range(1, TASKS):
            comb = comb + al[t] * acc1[t, :, cols]
        gsend[cols, :] = comb.T

    def o_copy(s):
        dev = peer(s)
        rows = pl.ds(pl.multiple_of(dev * FEAT, FEAT), FEAT)
        return remote(gsend.at[rows, :], gx.at[me], o_send.at[s], o_recv.at[s], dev)

    order = (2, 4, 3, 5, 6, 7, 1)
    for s in order:
        o_copy(s).start()

    for c in range(DIM // 128):
        cols = slice(128 * c, 128 * c + 128)
        comb = al[0] * acc2[0, :, cols]
        for t in range(1, TASKS):
            comb = comb + al[t] * acc2[t, :, cols]
        stage2[pl.ds(c, HID, stride=DIM // 128), :] = comb

    gx[me] = gsend[pl.ds(pl.multiple_of(me * FEAT, FEAT), FEAT), :]
    for s in range(1, NUM_DEV):
        o_copy(s).wait_recv()

    swap_copy().wait_send()
    for m in range(2, NUM_DEV):
        hops[m]().wait_send()
        hand(m).wait_send()
    for s in range(1, NUM_DEV):
        e_copy(s).wait_send()
        c_copy(s).wait_send()
        gram_copy(s, me).wait_send()
        o_copy(s).wait_send()


PER = HID // 128
FLAT = DIM * HIDDEN // NUM_DEV // 128
HALF = FEAT // 2


def finish(alpha_in, blocks, stage2, alpha_ref, out1_hbm, out2_hbm, stage1, out_sem):
    stores = [pltpu.make_async_copy(stage2, out2_hbm, out_sem.at[2])]
    stores[0].start()
    for t in range(TASKS):
        alpha_ref[t] = jnp.max(alpha_in[t:t + 1, :])
    for h in range(2):
        for d in range(NUM_DEV):
            for b in range(PER):
                first = h * HALF * (HIDDEN // 128) + d * PER + b
                stage1[pl.ds(first, HALF, stride=HIDDEN // 128), :] = blocks[d, h * HALF:h * HALF + HALF, 128 * b:128 * b + 128]
        rows = pl.ds(h * FLAT // 2, FLAT // 2)
        stores.append(pltpu.make_async_copy(stage1.at[rows, :], out1_hbm.at[rows, :], out_sem.at[h]))
        stores[-1].start()
    for c in stores:
        c.wait()


def solution(mesh):
    def local_step(x_loc, w_in, w_out, heads, lab_loc, mask_loc):
        hbm = pl.BlockSpec(memory_space=pl.ANY)
        vmem = pl.BlockSpec(memory_space=pltpu.VMEM)
        sem = pltpu.SemaphoreType.DMA((NUM_DEV,))
        v = pltpu.VMEM
        alpha, gx, g2 = pl.pallas_call(
            kernel,
            out_shape=(
                v((TASKS, 128), F32),
                v((NUM_DEV, FEAT, HID), F32),
                v((FLAT, 128), F32),
            ),
            in_specs=[hbm, hbm, hbm, vmem, vmem, vmem],
            out_specs=(vmem, vmem, vmem),
            scratch_shapes=[
                v((NUM_DEV, TOK, DIM), BF16),
                v((NCHUNK, DIM, CHUNK), BF16),
                v((NCHUNK, CHUNK, DIM), BF16),
                v((DIM, HID), BF16),
                v((HID, DIM), BF16),
                v((HID, DIM), BF16),
                v((ROWS, CHUNK), BF16),
                v((ROWS, CHUNK), BF16),
                v((TOK, DIM), F32),
                v((HEAD_ROWS, DIM), F32),
                v((TASKS * CLASSES, DIM, 128), F32),
                v((HEAD_ROWS, TOK), F32),
                v((NUM_DEV, HEAD_ROWS, TOK), BF16),
                v((2, TASKS, 8, TOK), F32),
                v((HID, PITCH), BF16),
                v((HID, PITCH), BF16),
                v((HID, TOK), F32),
                v((HID, TOK), F32),
                v((DIM, PITCH), BF16),
                v((DIM, PITCH), BF16),
                v((HID, PITCH), BF16),
                v((HID, PITCH), BF16),
                v((TASKS, HID, DIM), F32),
                v((TASKS, HID, DIM), F32),
                v((NUM_DEV, 8, 128), F32),
                v((8, DIM), F32),
                v((NUM_DEV, 16, 128), F32),
                v((DIM, HID), F32),
                sem, sem, sem, sem, sem, sem, sem, sem, sem, sem, sem, sem,
                pltpu.SemaphoreType.DMA((3 + 2 * NCHUNK,)),
            ],
            compiler_params=pltpu.CompilerParams(collective_id=0, has_side_effects=True, vmem_limit_bytes=62_000_000),
            name="trunk",
        )(x_loc, w_in, w_out, heads.transpose(2, 0, 1), lab_loc, mask_loc)
        smem = pl.BlockSpec(memory_space=pltpu.SMEM)
        alpha, out1, out2 = pl.pallas_call(
            finish,
            out_shape=(
                jax.ShapeDtypeStruct((TASKS,), F32),
                jax.ShapeDtypeStruct((FLAT, 128), F32),
                jax.ShapeDtypeStruct((FLAT, 128), F32),
            ),
            in_specs=[vmem, vmem, vmem],
            out_specs=(smem, hbm, hbm),
            scratch_shapes=[
                v((FLAT, 128), F32),
                pltpu.SemaphoreType.DMA((3,)),
            ],
            compiler_params=pltpu.CompilerParams(vmem_limit_bytes=8_000_000),
            name="finish",
        )(alpha, gx, g2)
        return alpha, out1.reshape(-1), out2.reshape(-1)

    return jax.shard_map(local_step, mesh=mesh, in_specs=(P("data", None), P(), P(), P(), P(None, "data"), P(None, "data")), out_specs=(P(), P("data"), P("data")), check_vma=False)
```

```python
import jax
import jax.numpy as jnp
from jax import lax
from jax.experimental import pallas as pl
from jax.experimental.pallas import tpu as pltpu
from jax.sharding import PartitionSpec as P

SOLVER_STEPS = 20
MESH = pl.DeviceIdType.MESH
F32, BF16 = jnp.float32, jnp.bfloat16
NUM_DEV = 8
TASKS = 4
CLASSES = 3
TOK = 1024
DIM = 768
HIDDEN = 3072
HID = HIDDEN // NUM_DEV
FEAT = DIM // NUM_DEV
HEAD_ROWS = 32
PITCH = TOK + 128
CHUNK = 768
ROWS = 512
NCHUNK = HIDDEN // CHUNK
QUARTER = TOK // TASKS
PAIRS = [(t, s) for t in range(TASKS) for s in range(t, TASKS)]
GELU_C = 0.7978845608028654
GELU_K = 0.044715


def dot_nn(a, b):
    return lax.dot_general(a, b, (((1,), (0,)), ((), ())), preferred_element_type=F32)


def dot_nt(a, b):
    return lax.dot_general(a, b, (((1,), (1,)), ((), ())), preferred_element_type=F32)


def lanes(row, width):
    return jnp.concatenate([row] * (width // row.shape[1]), axis=1)


def gelu_parts(p):
    a = (GELU_C * GELU_K) * (p * p)
    th = jnp.tanh(p * (a + GELU_C))
    return a, th, 0.5 + 0.5 * th


def gelu_value(p):
    return p * gelu_parts(p)[2]


def gelu_both(p):
    a, th, cdf = gelu_parts(p)
    slope = cdf + ((1.0 - th * th) * p) * (1.5 * a + 0.5 * GELU_C)
    return p * cdf, slope


def kernel(x_hbm, w_in_hbm, w_out_hbm, head_ref, lab_ref, mask_ref, alpha_ref, gx, stage2,
           xs, w1, w2, w1j, w1t, w2j, abuf0, abuf1, zacc, hrow, hbc, ef, es, ecur, act0, act1, slope0, slope1,
           dz0, dz1, q0, q1, acc1, acc2, cnt, inv, gram, gsend,
           x_send, x_recv, f_send, f_recv, e_send, e_recv, c_send, c_recv, g_send, g_recv, o_send, o_recv, l_sem):
    me = lax.axis_index("data")
    core = lax.rem(me, 2)
    cx = lax.rem(lax.div(me, 2), 2)
    cy = lax.div(me, 4)

    def flip(v, b):
        return v + b - 2 * v * b

    def peer(s):
        return flip(cx, s // 2 % 2) * 2 + flip(cy, s // 4) * 4 + flip(core, jnp.int32(s % 2))

    def remote(src, dst, send, recv, dev):
        return pltpu.make_async_remote_copy(src_ref=src, dst_ref=dst, send_sem=send, recv_sem=recv, device_id=(dev,), device_id_type=MESH)

    half = pl.ds(pl.multiple_of(core * ROWS, ROWS), ROWS)
    x_dev, y_dev = peer(2), peer(4)
    first_dev = core * y_dev + (1 - core) * x_dev
    second_dev = core * x_dev + (1 - core) * y_dev

    def swap_copy():
        return remote(xs.at[0], xs.at[1], x_send.at[1], x_recv.at[1], peer(1))

    def hop(src, dst, i, dev):
        return remote(xs.at[src, half, :], xs.at[dst, half, :], x_send.at[i], x_recv.at[dst], dev)

    def arrived(m):
        return hop(0, m, 2, x_dev)

    hops = {
        2: lambda: hop(0, 2 + core, 2, first_dev),
        3: lambda: hop(1, 3 - core, 3, second_dev),
        4: lambda: hop(1, 4 + core, 4, first_dev),
        5: lambda: hop(0, 5 - core, 5, second_dev),
        6: lambda: hop(2 + 3 * core, 6, 6, second_dev),
        7: lambda: hop(4 - core, 7, 7, second_dev),
    }

    def hand(m):
        return remote(xs.at[m, half, :], xs.at[m, half, :], f_send.at[m], f_recv.at[m], peer(1))

    def arrival_slot(s):
        bx, by = s // 2 % 2, s // 4
        return 6 + core if bx and by else 2 + 2 * core if bx else 5 - 2 * core if by else 1

    def e_copy(s):
        slot = arrival_slot(s)
        return remote(es.at[0], es.at[slot], e_send.at[s], e_recv.at[slot], peer(s))

    def e_arrived(slot):
        return remote(es.at[0], es.at[slot], e_send.at[1], e_recv.at[slot], peer(1))

    def c_copy(s):
        return remote(cnt.at[0], cnt.at[s], c_send.at[s], c_recv.at[s], peer(s))

    def local(src, dst, i):
        return pltpu.make_async_copy(src, dst, l_sem.at[i])

    def load_w1(i):
        return local(w_in_hbm.at[:, pl.ds(pl.multiple_of(CHUNK * i, CHUNK), CHUNK)], w1.at[i], 3 + i)

    def load_w2(i):
        return local(w_out_hbm.at[pl.ds(pl.multiple_of(CHUNK * i, CHUNK), CHUNK), :], w2.at[i], 3 + NCHUNK + i)

    load_x = local(x_hbm, xs.at[0], 0)
    load_w1j = local(w_in_hbm.at[:, pl.ds(pl.multiple_of(me * HID, HID), HID)], w1j, 1)
    load_w2j = local(w_out_hbm.at[pl.ds(pl.multiple_of(me * HID, HID), HID), :], w2j, 2)
    load_x.start()
    load_w1j.start()
    load_w1(0).start()
    load_w2(0).start()

    barrier = pltpu.get_barrier_semaphore()
    for s in range(1, NUM_DEV):
        pl.semaphore_signal(barrier, inc=1, device_id=(peer(s),), device_id_type=MESH)

    counts = jnp.sum(mask_ref[...].astype(F32), axis=1, keepdims=True)
    cnt[0, 0:TASKS, :] = jnp.broadcast_to(counts, (TASKS, 128))
    cnt[0, TASKS:8, :] = jnp.zeros((8 - TASKS, 128), F32)
    hrow[...] = jnp.zeros_like(hrow)
    for c in range(CLASSES):
        hrow[8 * c:8 * c + TASKS, :] = head_ref[c].astype(F32)
    head = hrow[...].astype(BF16)

    block = lax.div(lax.broadcasted_iota(jnp.int32, (HEAD_ROWS, TASKS * CLASSES * 128), 1), 128)
    pick = lax.rem(block, CLASSES) * 8 + lax.div(block, CLASSES)
    ones = (lax.broadcasted_iota(jnp.int32, block.shape, 0) == pick).astype(F32).astype(BF16)
    wide = dot_nn(hrow[...].T.astype(BF16), ones)
    for k in range(TASKS * CLASSES):
        hbc[k] = wide[:, 128 * k:128 * k + 128]
    pl.semaphore_wait(barrier, NUM_DEV - 1)
    load_x.wait()
    hops[2]().start()
    swap_copy().start()
    for s in range(1, NUM_DEV):
        c_copy(s).start()
    for i in range(1, NCHUNK):
        load_w1(i).start()
        load_w2(i).start()
    load_w2j.start()

    load_w1j.wait()
    w1t[...] = w1j[...].astype(F32).T.astype(BF16)

    abuf1[...] = jnp.zeros_like(abuf1)
    zacc[...] = xs[0].astype(F32)
    half0, half1 = slice(0, ROWS), slice(ROWS, TOK)

    acts, slopes, dzs, qs = (act0, act1), (slope0, slope1), (dz0, dz1), (q0, q1)

    def preact(slot, part, quarter):
        r = pl.ds(pl.multiple_of(quarter * QUARTER, QUARTER), QUARTER)
        a, sl = gelu_both(dot_nt(w1t[...], xs[slot, r, :]))
        acts[part][:, r] = a.astype(BF16)
        slopes[part][:, r] = sl

    def forward(h, carry):
        load_w1(h).wait()
        load_w2(h).wait()
        acc1[h] = jnp.zeros((HID, DIM), F32)
        acc2[h] = jnp.zeros((HID, DIM), F32)
        @pl.when(h == 1)
        def _():
            swap_copy().wait_recv()
            hops[3]().start()

        abuf0[...] = gelu_value(dot_nn(xs[0, half0, :], w1[h])).astype(BF16)
        zacc[half1, :] += dot_nn(abuf1[...], w2[jnp.maximum(h - 1, 0)])
        abuf1[...] = gelu_value(dot_nn(xs[0, half1, :], w1[h])).astype(BF16)
        zacc[half0, :] += dot_nn(abuf0[...], w2[h])
        preact(0, 0, h)
        return carry

    lax.fori_loop(0, NCHUNK, forward, 0)
    zacc[half1, :] += dot_nn(abuf1[...], w2[NCHUNK - 1])

    for r in range(TOK // ROWS):
        cols = slice(r * ROWS, (r + 1) * ROWS)
        logits = dot_nt(head, zacc[cols, :].astype(BF16))
        l = [logits[8 * c:8 * c + TASKS] for c in range(CLASSES)]
        top = jnp.maximum(jnp.maximum(l[0], l[1]), l[2])
        ex = [jnp.exp(v - top) for v in l]
        total = ex[0] + ex[1] + ex[2]
        lab = lab_ref[:, cols]
        m = mask_ref[:, cols].astype(F32)
        for c in range(CLASSES):
            err = m * (ex[c] / total - (lab == c).astype(F32))
            for t in range(TASKS):
                ef[8 * t + c:8 * t + c + 1, cols] = err[t:t + 1]
    for t in range(TASKS):
        ef[8 * t + CLASSES:8 * t + 8, :] = jnp.zeros((8 - CLASSES, TOK), F32)
    es[0] = ef[...].astype(BF16)
    for t in range(TASKS):
        ecur[0, t] = es[0, 8 * t:8 * t + 8, :].astype(F32)

    def make_dz(dst, part, t):
        e = ecur[part, t]
        rows = [jnp.broadcast_to(e[c:c + 1, :], (8, TOK)) for c in range(CLASSES)]
        for k in range(DIM // 8):
            f = slice(8 * k, 8 * k + 8)
            h = [lanes(hbc[CLASSES * t + c, f, :], TOK) for c in range(CLASSES)]
            dst[f, 0:TOK] = (h[0] * rows[0] + h[1] * rows[1] + h[2] * rows[2]).astype(BF16)

    for s in range(1, NUM_DEV):
        e_copy(s).start()
    make_dz(dz0, 0, 0)
    load_w2j.wait()
    total_cnt = cnt[0]
    for s in range(1, NUM_DEV):
        c_copy(s).wait_recv()
        total_cnt = total_cnt + cnt[s]
    inv[...] = lanes(1.0 / jnp.maximum(total_cnt, 1.0), DIM)

    def link_half_ready(s):
        for k, slots in ((1, (2, 3)), (3, (4, 5)), (5, (6,)), (6, (7,))):
            @pl.when(s == k)
            def _():
                for m in slots:
                    arrived(m).wait_recv()
                    hand(m).start()
                if k == 3:
                    hops[6]().start()
                    hops[7]().start()

    def other_half_ready(s):
        for m in range(2, NUM_DEV):
            @pl.when(s == m - 1)
            def _():
                hand(m).wait_recv()

    def errors_ready(s, part):
        for k in range(1, NUM_DEV):
            @pl.when(s == k - 1)
            def _():
                e_arrived(k).wait_recv()
                for t in range(TASKS):
                    ecur[part, t] = es[k, 8 * t:8 * t + 8, :].astype(F32)

    def run_task(s, part, t, j, next_part, next_t):
        nxt = jnp.minimum(s + 1, NUM_DEV - 1)
        scale = inv[pl.ds(t, 1), :]
        qs[j][:, 0:TOK] = (dot_nn(w2j[...], dzs[j][:, 0:TOK]) * slopes[part][...]).astype(BF16)
        acc2[t] += (dot_nt(acts[part][:, 0:TOK], dzs[j][:, 0:TOK]) * scale).astype(BF16).astype(F32)
        make_dz(dzs[1 - j], next_part, next_t)
        preact(nxt, 1 - part, lax.rem(t + 2 * core, TASKS))
        acc1[t] += (dot_nn(qs[j][:, 0:TOK], xs[s]) * scale).astype(BF16).astype(F32)

    def shard_pair(sp, carry):
        for part in range(2):
            s = 2 * sp + part
            link_half_ready(s)

            def task_pair(tp, c):
                @pl.when(tp == 1)
                def _():
                    errors_ready(s, 1 - part)
                    other_half_ready(s)

                run_task(s, part, 2 * tp, 0, part, 2 * tp + 1)
                wrap = lax.div(2 * tp + 2, TASKS)
                run_task(s, part, 2 * tp + 1, 1, part + wrap * (1 - 2 * part), 2 * tp + 2 - TASKS * wrap)
                return c

            lax.fori_loop(0, TASKS // 2, task_pair, 0)
        return carry

    hops[4]().start()
    hops[5]().start()
    lax.fori_loop(0, NUM_DEV // 2, shard_pair, 0)

    def gram_rows(i, sums):
        r = pl.ds(pl.multiple_of(i * 8, 8), 8)
        out = list(sums)
        for acc in (acc1, acc2):
            for c in range(DIM // 128):
                g = [acc[t, r, 128 * c:128 * c + 128] for t in range(TASKS)]
                for k, (t, u) in enumerate(PAIRS):
                    out[k] = out[k] + g[t] * g[u]
        return tuple(out)

    sums = lax.fori_loop(0, HID // 8, gram_rows, tuple(jnp.zeros((8, 128), F32) for _ in PAIRS))
    for k in range(len(PAIRS)):
        gram[me, k:k + 1, :] = jnp.broadcast_to(jnp.sum(sums[k]), (1, 128))
    gram[me, len(PAIRS):16, :] = jnp.zeros((16 - len(PAIRS), 128), F32)

    def gram_copy(s, block):
        return remote(gram.at[block], gram.at[block], g_send.at[s], g_recv.at[s], peer(s))

    for s in range(1, NUM_DEV):
        gram_copy(s, me).start()
    for s in range(1, NUM_DEV):
        gram_copy(s, me).wait_recv()
    gram_sum = gram[0]
    for d in range(1, NUM_DEV):
        gram_sum = gram_sum + gram[d]
    m = {}
    for k, (t, u) in enumerate(PAIRS):
        m[t, u] = m[u, t] = gram_sum[k:k + 1, :]
    step_scale = (m[0, 0] + m[1, 1] + m[2, 2] + m[3, 3]) / TASKS
    al = [jnp.full((1, 128), 1.0 / TASKS, F32) for _ in range(TASKS)]
    for _ in range(SOLVER_STEPS):
        raised = []
        for t in range(TASKS):
            pull = (m[t, 0] * al[0] + m[t, 1] * al[1]) + (m[t, 2] * al[2] + m[t, 3] * al[3])
            raised.append(al[t] * jnp.exp(-pull / step_scale))
        norm = (raised[0] + raised[1]) + (raised[2] + raised[3])
        al = [r / norm for r in raised]
    for t in range(TASKS):
        alpha_ref[t:t + 1, :] = al[t]

    for c in range(DIM // 128):
        cols = slice(128 * c, 128 * c + 128)
        comb = al[0] * acc1[0, :, cols]
        for t in range(1, TASKS):
            comb = comb + al[t] * acc1[t, :, cols]
        gsend[cols, :] = comb.T

    def o_copy(s):
        dev = peer(s)
        rows = pl.ds(pl.multiple_of(dev * FEAT, FEAT), FEAT)
        return remote(gsend.at[rows, :], gx.at[me], o_send.at[s], o_recv.at[s], dev)

    order = (2, 4, 3, 5, 6, 7, 1)
    for s in order:
        o_copy(s).start()

    for c in range(DIM // 128):
        cols = slice(128 * c, 128 * c + 128)
        comb = al[0] * acc2[0, :, cols]
        for t in range(1, TASKS):
            comb = comb + al[t] * acc2[t, :, cols]
        stage2[pl.ds(c, HID, stride=DIM // 128), :] = comb

    gx[me] = gsend[pl.ds(pl.multiple_of(me * FEAT, FEAT), FEAT), :]
    for s in range(1, NUM_DEV):
        o_copy(s).wait_recv()

    swap_copy().wait_send()
    for m in range(2, NUM_DEV):
        hops[m]().wait_send()
        hand(m).wait_send()
    for s in range(1, NUM_DEV):
        e_copy(s).wait_send()
        c_copy(s).wait_send()
        gram_copy(s, me).wait_send()
        o_copy(s).wait_send()


PER = HID // 128
FLAT = DIM * HIDDEN // NUM_DEV // 128
HALF = FEAT // 2


def finish(alpha_in, blocks, stage2, alpha_ref, out1_hbm, out2_hbm, stage1, out_sem):
    stores = [pltpu.make_async_copy(stage2, out2_hbm, out_sem.at[2])]
    stores[0].start()
    for t in range(TASKS):
        alpha_ref[t] = jnp.max(alpha_in[t:t + 1, :])
    for h in range(2):
        for d in range(NUM_DEV):
            for b in range(PER):
                first = h * HALF * (HIDDEN // 128) + d * PER + b
                stage1[pl.ds(first, HALF, stride=HIDDEN // 128), :] = blocks[d, h * HALF:h * HALF + HALF, 128 * b:128 * b + 128]
        rows = pl.ds(h * FLAT // 2, FLAT // 2)
        stores.append(pltpu.make_async_copy(stage1.at[rows, :], out1_hbm.at[rows, :], out_sem.at[h]))
        stores[-1].start()
    for c in stores:
        c.wait()


def solution(mesh):
    def local_step(x_loc, w_in, w_out, heads, lab_loc, mask_loc):
        hbm = pl.BlockSpec(memory_space=pl.ANY)
        vmem = pl.BlockSpec(memory_space=pltpu.VMEM)
        sem = pltpu.SemaphoreType.DMA((NUM_DEV,))
        v = pltpu.VMEM
        alpha, gx, g2 = pl.pallas_call(
            kernel,
            out_shape=(
                v((TASKS, 128), F32),
                v((NUM_DEV, FEAT, HID), F32),
                v((FLAT, 128), F32),
            ),
            in_specs=[hbm, hbm, hbm, vmem, vmem, vmem],
            out_specs=(vmem, vmem, vmem),
            scratch_shapes=[
                v((NUM_DEV, TOK, DIM), BF16),
                v((NCHUNK, DIM, CHUNK), BF16),
                v((NCHUNK, CHUNK, DIM), BF16),
                v((DIM, HID), BF16),
                v((HID, DIM), BF16),
                v((HID, DIM), BF16),
                v((ROWS, CHUNK), BF16),
                v((ROWS, CHUNK), BF16),
                v((TOK, DIM), F32),
                v((HEAD_ROWS, DIM), F32),
                v((TASKS * CLASSES, DIM, 128), F32),
                v((HEAD_ROWS, TOK), F32),
                v((NUM_DEV, HEAD_ROWS, TOK), BF16),
                v((2, TASKS, 8, TOK), F32),
                v((HID, PITCH), BF16),
                v((HID, PITCH), BF16),
                v((HID, TOK), F32),
                v((HID, TOK), F32),
                v((DIM, PITCH), BF16),
                v((DIM, PITCH), BF16),
                v((HID, PITCH), BF16),
                v((HID, PITCH), BF16),
                v((TASKS, HID, DIM), F32),
                v((TASKS, HID, DIM), F32),
                v((NUM_DEV, 8, 128), F32),
                v((8, DIM), F32),
                v((NUM_DEV, 16, 128), F32),
                v((DIM, HID), F32),
                sem, sem, sem, sem, sem, sem, sem, sem, sem, sem, sem, sem,
                pltpu.SemaphoreType.DMA((3 + 2 * NCHUNK,)),
            ],
            compiler_params=pltpu.CompilerParams(collective_id=0, has_side_effects=True, vmem_limit_bytes=62_000_000),
            name="trunk",
        )(x_loc, w_in, w_out, heads.transpose(2, 0, 1), lab_loc, mask_loc)
        smem = pl.BlockSpec(memory_space=pltpu.SMEM)
        alpha, out1, out2 = pl.pallas_call(
            finish,
            out_shape=(
                jax.ShapeDtypeStruct((TASKS,), F32),
                jax.ShapeDtypeStruct((FLAT, 128), F32),
                jax.ShapeDtypeStruct((FLAT, 128), F32),
            ),
            in_specs=[vmem, vmem, vmem],
            out_specs=(smem, hbm, hbm),
            scratch_shapes=[
                v((FLAT, 128), F32),
                pltpu.SemaphoreType.DMA((3,)),
            ],
            compiler_params=pltpu.CompilerParams(vmem_limit_bytes=8_000_000),
            name="finish",
        )(alpha, gx, g2)
        return alpha, out1.reshape(-1), out2.reshape(-1)

    return jax.shard_map(local_step, mesh=mesh, in_specs=(P("data", None), P(), P(), P(), P(None, "data"), P(None, "data")), out_specs=(P(), P("data"), P("data")), check_vma=False)
```

```python
import jax
import jax.numpy as jnp
from jax import lax
from jax.experimental import pallas as pl
from jax.experimental.pallas import tpu as pltpu
from jax.sharding import PartitionSpec as P

SOLVER_STEPS = 20
MESH = pl.DeviceIdType.MESH
F32, BF16 = jnp.float32, jnp.bfloat16
NUM_DEV = 8
TASKS = 4
CLASSES = 3
TOK = 1024
DIM = 768
HIDDEN = 3072
HID = HIDDEN // NUM_DEV
FEAT = DIM // NUM_DEV
HEAD_ROWS = 32
PITCH = TOK + 128
CHUNK = 768
ROWS = 512
NCHUNK = HIDDEN // CHUNK
QUARTER = TOK // TASKS
PAIRS = [(t, s) for t in range(TASKS) for s in range(t, TASKS)]
GELU_C = 0.7978845608028654
GELU_K = 0.044715


def dot_nn(a, b):
    return lax.dot_general(a, b, (((1,), (0,)), ((), ())), preferred_element_type=F32)


def dot_nt(a, b):
    return lax.dot_general(a, b, (((1,), (1,)), ((), ())), preferred_element_type=F32)


def lanes(row, width):
    return jnp.concatenate([row] * (width // row.shape[1]), axis=1)


def gelu_parts(p):
    a = (GELU_C * GELU_K) * (p * p)
    th = jnp.tanh(p * (a + GELU_C))
    return a, th, 0.5 + 0.5 * th


def gelu_value(p):
    return p * gelu_parts(p)[2]


def gelu_both(p):
    a, th, cdf = gelu_parts(p)
    slope = cdf + ((1.0 - th * th) * p) * (1.5 * a + 0.5 * GELU_C)
    return p * cdf, slope


def kernel(x_hbm, w_in_hbm, w_out_hbm, head_hbm, lab_hbm, mask_hbm, alpha_ref, gx, stage2,
           head_ref, lab_ref, mask_ref, xs, w1, w2, w1j, w1t, w2j, abuf0, abuf1, zacc, hrow, hbc, ef, es, ecur, act0, act1, slope0, slope1,
           dz0, dz1, q0, q1, acc1, acc2, cnt, inv, gram, gsend,
           x_send, x_recv, f_send, f_recv, e_send, e_recv, c_send, c_recv, g_send, g_recv, o_send, o_recv, l_sem):
    me = lax.axis_index("data")
    core = lax.rem(me, 2)
    cx = lax.rem(lax.div(me, 2), 2)
    cy = lax.div(me, 4)

    def flip(v, b):
        return v + b - 2 * v * b

    def peer(s):
        return flip(cx, s // 2 % 2) * 2 + flip(cy, s // 4) * 4 + flip(core, jnp.int32(s % 2))

    def remote(src, dst, send, recv, dev):
        return pltpu.make_async_remote_copy(src_ref=src, dst_ref=dst, send_sem=send, recv_sem=recv, device_id=(dev,), device_id_type=MESH)

    half = pl.ds(pl.multiple_of(core * ROWS, ROWS), ROWS)
    x_dev, y_dev = peer(2), peer(4)
    first_dev = core * y_dev + (1 - core) * x_dev
    second_dev = core * x_dev + (1 - core) * y_dev

    def swap_copy():
        return remote(xs.at[0], xs.at[1], x_send.at[1], x_recv.at[1], peer(1))

    def hop(src, dst, i, dev):
        return remote(xs.at[src, half, :], xs.at[dst, half, :], x_send.at[i], x_recv.at[dst], dev)

    def arrived(m):
        return hop(0, m, 2, x_dev)

    hops = {
        2: lambda: hop(0, 2 + core, 2, first_dev),
        3: lambda: hop(1, 3 - core, 3, second_dev),
        4: lambda: hop(1, 4 + core, 4, first_dev),
        5: lambda: hop(0, 5 - core, 5, second_dev),
        6: lambda: hop(2 + 3 * core, 6, 6, second_dev),
        7: lambda: hop(4 - core, 7, 7, second_dev),
    }

    def hand(m):
        return remote(xs.at[m, half, :], xs.at[m, half, :], f_send.at[m], f_recv.at[m], peer(1))

    def arrival_slot(s):
        bx, by = s // 2 % 2, s // 4
        return 6 + core if bx and by else 2 + 2 * core if bx else 5 - 2 * core if by else 1

    def e_copy(s):
        slot = arrival_slot(s)
        return remote(es.at[0], es.at[slot], e_send.at[s], e_recv.at[slot], peer(s))

    def e_arrived(slot):
        return remote(es.at[0], es.at[slot], e_send.at[1], e_recv.at[slot], peer(1))

    def c_copy(s):
        return remote(cnt.at[0], cnt.at[s], c_send.at[s], c_recv.at[s], peer(s))

    def local(src, dst, i):
        return pltpu.make_async_copy(src, dst, l_sem.at[i])

    def load_w1(i):
        return local(w_in_hbm.at[:, pl.ds(pl.multiple_of(CHUNK * i, CHUNK), CHUNK)], w1.at[i], 3 + i)

    def load_w2(i):
        return local(w_out_hbm.at[pl.ds(pl.multiple_of(CHUNK * i, CHUNK), CHUNK), :], w2.at[i], 3 + NCHUNK + i)

    load_x = local(x_hbm, xs.at[0], 0)
    load_w1j = local(w_in_hbm.at[:, pl.ds(pl.multiple_of(me * HID, HID), HID)], w1j, 1)
    load_w2j = local(w_out_hbm.at[pl.ds(pl.multiple_of(me * HID, HID), HID), :], w2j, 2)
    load_head = local(head_hbm, head_ref, 3 + 2 * NCHUNK)
    load_lab = local(lab_hbm, lab_ref, 4 + 2 * NCHUNK)
    load_mask = local(mask_hbm, mask_ref, 5 + 2 * NCHUNK)
    load_x.start()
    load_head.start()
    load_mask.start()
    load_lab.start()
    load_w1j.start()
    load_w1(0).start()
    load_w2(0).start()

    barrier = pltpu.get_barrier_semaphore()
    for s in range(1, NUM_DEV):
        pl.semaphore_signal(barrier, inc=1, device_id=(peer(s),), device_id_type=MESH)

    load_head.wait()
    hrow[...] = jnp.zeros_like(hrow)
    for c in range(CLASSES):
        hrow[8 * c:8 * c + TASKS, :] = head_ref[c].astype(F32)
    head = hrow[...].astype(BF16)

    block = lax.div(lax.broadcasted_iota(jnp.int32, (HEAD_ROWS, TASKS * CLASSES * 128), 1), 128)
    pick = lax.rem(block, CLASSES) * 8 + lax.div(block, CLASSES)
    ones = (lax.broadcasted_iota(jnp.int32, block.shape, 0) == pick).astype(F32).astype(BF16)
    wide = dot_nn(hrow[...].T.astype(BF16), ones)
    for k in range(TASKS * CLASSES):
        hbc[k] = wide[:, 128 * k:128 * k + 128]
    load_x.wait()
    for i in range(1, NCHUNK):
        load_w1(i).start()
        load_w2(i).start()
    load_w2j.start()
    load_mask.wait()
    load_lab.wait()
    counts = jnp.sum(mask_ref[...].astype(F32), axis=1, keepdims=True)
    cnt[0, 0:TASKS, :] = jnp.broadcast_to(counts, (TASKS, 128))
    cnt[0, TASKS:8, :] = jnp.zeros((8 - TASKS, 128), F32)
    load_w1j.wait()
    w1t[...] = w1j[...].astype(F32).T.astype(BF16)

    pl.semaphore_wait(barrier, NUM_DEV - 1)
    hops[2]().start()
    swap_copy().start()
    for s in range(1, NUM_DEV):
        c_copy(s).start()

    abuf1[...] = jnp.zeros_like(abuf1)
    zacc[...] = xs[0].astype(F32)
    half0, half1 = slice(0, ROWS), slice(ROWS, TOK)

    acts, slopes, dzs, qs = (act0, act1), (slope0, slope1), (dz0, dz1), (q0, q1)

    def preact(slot, part, quarter):
        r = pl.ds(pl.multiple_of(quarter * QUARTER, QUARTER), QUARTER)
        a, sl = gelu_both(dot_nt(w1t[...], xs[slot, r, :]))
        acts[part][:, r] = a.astype(BF16)
        slopes[part][:, r] = sl

    def forward(h, carry):
        load_w1(h).wait()
        load_w2(h).wait()
        acc1[h] = jnp.zeros((HID, DIM), F32)
        acc2[h] = jnp.zeros((HID, DIM), F32)
        @pl.when(h == 1)
        def _():
            swap_copy().wait_recv()
            hops[3]().start()

        abuf0[...] = gelu_value(dot_nn(xs[0, half0, :], w1[h])).astype(BF16)
        zacc[half1, :] += dot_nn(abuf1[...], w2[jnp.maximum(h - 1, 0)])
        abuf1[...] = gelu_value(dot_nn(xs[0, half1, :], w1[h])).astype(BF16)
        zacc[half0, :] += dot_nn(abuf0[...], w2[h])
        preact(0, 0, h)
        return carry

    lax.fori_loop(0, NCHUNK, forward, 0)
    zacc[half1, :] += dot_nn(abuf1[...], w2[NCHUNK - 1])

    for r in range(TOK // ROWS):
        cols = slice(r * ROWS, (r + 1) * ROWS)
        logits = dot_nt(head, zacc[cols, :].astype(BF16))
        l = [logits[8 * c:8 * c + TASKS] for c in range(CLASSES)]
        top = jnp.maximum(jnp.maximum(l[0], l[1]), l[2])
        ex = [jnp.exp(v - top) for v in l]
        total = ex[0] + ex[1] + ex[2]
        lab = lab_ref[:, cols]
        m = mask_ref[:, cols].astype(F32)
        for c in range(CLASSES):
            err = m * (ex[c] / total - (lab == c).astype(F32))
            for t in range(TASKS):
                ef[8 * t + c:8 * t + c + 1, cols] = err[t:t + 1]
    for t in range(TASKS):
        ef[8 * t + CLASSES:8 * t + 8, :] = jnp.zeros((8 - CLASSES, TOK), F32)
    es[0] = ef[...].astype(BF16)
    for t in range(TASKS):
        ecur[0, t] = es[0, 8 * t:8 * t + 8, :].astype(F32)

    def make_dz(dst, part, t):
        e = ecur[part, t]
        rows = [jnp.broadcast_to(e[c:c + 1, :], (8, TOK)) for c in range(CLASSES)]
        for k in range(DIM // 8):
            f = slice(8 * k, 8 * k + 8)
            h = [lanes(hbc[CLASSES * t + c, f, :], TOK) for c in range(CLASSES)]
            dst[f, 0:TOK] = (h[0] * rows[0] + h[1] * rows[1] + h[2] * rows[2]).astype(BF16)

    for s in range(1, NUM_DEV):
        e_copy(s).start()
    make_dz(dz0, 0, 0)
    load_w2j.wait()
    total_cnt = cnt[0]
    for s in range(1, NUM_DEV):
        c_copy(s).wait_recv()
        total_cnt = total_cnt + cnt[s]
    inv[...] = lanes(1.0 / jnp.maximum(total_cnt, 1.0), DIM)

    def link_half_ready(s):
        for k, slots in ((1, (2, 3)), (3, (4, 5)), (5, (6,)), (6, (7,))):
            @pl.when(s == k)
            def _():
                for m in slots:
                    arrived(m).wait_recv()
                    hand(m).start()
                if k == 3:
                    hops[6]().start()
                    hops[7]().start()

    def other_half_ready(s):
        for m in range(2, NUM_DEV):
            @pl.when(s == m - 1)
            def _():
                hand(m).wait_recv()

    def errors_ready(s, part):
        for k in range(1, NUM_DEV):
            @pl.when(s == k - 1)
            def _():
                e_arrived(k).wait_recv()
                for t in range(TASKS):
                    ecur[part, t] = es[k, 8 * t:8 * t + 8, :].astype(F32)

    def run_task(s, part, t, j, next_part, next_t):
        nxt = jnp.minimum(s + 1, NUM_DEV - 1)
        scale = inv[pl.ds(t, 1), :]
        qs[j][:, 0:TOK] = (dot_nn(w2j[...], dzs[j][:, 0:TOK]) * slopes[part][...]).astype(BF16)
        acc2[t] += (dot_nt(acts[part][:, 0:TOK], dzs[j][:, 0:TOK]) * scale).astype(BF16).astype(F32)
        make_dz(dzs[1 - j], next_part, next_t)
        preact(nxt, 1 - part, lax.rem(t + 2 * core, TASKS))
        acc1[t] += (dot_nn(qs[j][:, 0:TOK], xs[s]) * scale).astype(BF16).astype(F32)

    def shard_pair(sp, carry):
        for part in range(2):
            s = 2 * sp + part
            link_half_ready(s)

            def task_pair(tp, c):
                @pl.when(tp == 1)
                def _():
                    errors_ready(s, 1 - part)
                    other_half_ready(s)

                run_task(s, part, 2 * tp, 0, part, 2 * tp + 1)
                wrap = lax.div(2 * tp + 2, TASKS)
                run_task(s, part, 2 * tp + 1, 1, part + wrap * (1 - 2 * part), 2 * tp + 2 - TASKS * wrap)
                return c

            lax.fori_loop(0, TASKS // 2, task_pair, 0)
        return carry

    hops[4]().start()
    hops[5]().start()
    lax.fori_loop(0, NUM_DEV // 2, shard_pair, 0)

    def gram_rows(i, sums):
        r = pl.ds(pl.multiple_of(i * 8, 8), 8)
        out = list(sums)
        for acc in (acc1, acc2):
            for c in range(DIM // 128):
                g = [acc[t, r, 128 * c:128 * c + 128] for t in range(TASKS)]
                for k, (t, u) in enumerate(PAIRS):
                    out[k] = out[k] + g[t] * g[u]
        return tuple(out)

    sums = lax.fori_loop(0, HID // 8, gram_rows, tuple(jnp.zeros((8, 128), F32) for _ in PAIRS))
    for k in range(len(PAIRS)):
        gram[me, k:k + 1, :] = jnp.broadcast_to(jnp.sum(sums[k]), (1, 128))
    gram[me, len(PAIRS):16, :] = jnp.zeros((16 - len(PAIRS), 128), F32)

    def gram_copy(s, block):
        return remote(gram.at[block], gram.at[block], g_send.at[s], g_recv.at[s], peer(s))

    for s in range(1, NUM_DEV):
        gram_copy(s, me).start()
    for s in range(1, NUM_DEV):
        gram_copy(s, me).wait_recv()
    gram_sum = gram[0]
    for d in range(1, NUM_DEV):
        gram_sum = gram_sum + gram[d]
    m = {}
    for k, (t, u) in enumerate(PAIRS):
        m[t, u] = m[u, t] = gram_sum[k:k + 1, :]
    step_scale = (m[0, 0] + m[1, 1] + m[2, 2] + m[3, 3]) / TASKS
    al = [jnp.full((1, 128), 1.0 / TASKS, F32) for _ in range(TASKS)]
    for _ in range(SOLVER_STEPS):
        raised = []
        for t in range(TASKS):
            pull = (m[t, 0] * al[0] + m[t, 1] * al[1]) + (m[t, 2] * al[2] + m[t, 3] * al[3])
            raised.append(al[t] * jnp.exp(-pull / step_scale))
        norm = (raised[0] + raised[1]) + (raised[2] + raised[3])
        al = [r / norm for r in raised]
    for t in range(TASKS):
        alpha_ref[t:t + 1, :] = al[t]

    for c in range(DIM // 128):
        cols = slice(128 * c, 128 * c + 128)
        comb = al[0] * acc1[0, :, cols]
        for t in range(1, TASKS):
            comb = comb + al[t] * acc1[t, :, cols]
        gsend[cols, :] = comb.T

    def o_copy(s):
        dev = peer(s)
        rows = pl.ds(pl.multiple_of(dev * FEAT, FEAT), FEAT)
        return remote(gsend.at[rows, :], gx.at[me], o_send.at[s], o_recv.at[s], dev)

    order = (2, 4, 3, 5, 6, 7, 1)
    for s in order:
        o_copy(s).start()

    for c in range(DIM // 128):
        cols = slice(128 * c, 128 * c + 128)
        comb = al[0] * acc2[0, :, cols]
        for t in range(1, TASKS):
            comb = comb + al[t] * acc2[t, :, cols]
        stage2[pl.ds(c, HID, stride=DIM // 128), :] = comb

    gx[me] = gsend[pl.ds(pl.multiple_of(me * FEAT, FEAT), FEAT), :]
    for s in range(1, NUM_DEV):
        o_copy(s).wait_recv()

    swap_copy().wait_send()
    for m in range(2, NUM_DEV):
        hops[m]().wait_send()
        hand(m).wait_send()
    for s in range(1, NUM_DEV):
        e_copy(s).wait_send()
        c_copy(s).wait_send()
        gram_copy(s, me).wait_send()
        o_copy(s).wait_send()


PER = HID // 128
FLAT = DIM * HIDDEN // NUM_DEV // 128
HALF = FEAT // 2


def finish(alpha_in, blocks, stage2, alpha_ref, out1_hbm, out2_hbm, stage1, out_sem):
    stores = [pltpu.make_async_copy(stage2, out2_hbm, out_sem.at[2])]
    stores[0].start()
    for t in range(TASKS):
        alpha_ref[t] = jnp.max(alpha_in[t:t + 1, :])
    for h in range(2):
        for d in range(NUM_DEV):
            for b in range(PER):
                first = h * HALF * (HIDDEN // 128) + d * PER + b
                stage1[pl.ds(first, HALF, stride=HIDDEN // 128), :] = blocks[d, h * HALF:h * HALF + HALF, 128 * b:128 * b + 128]
        rows = pl.ds(h * FLAT // 2, FLAT // 2)
        stores.append(pltpu.make_async_copy(stage1.at[rows, :], out1_hbm.at[rows, :], out_sem.at[h]))
        stores[-1].start()
    for c in stores:
        c.wait()


def solution(mesh):
    def local_step(x_loc, w_in, w_out, heads, lab_loc, mask_loc):
        hbm = pl.BlockSpec(memory_space=pl.ANY)
        vmem = pl.BlockSpec(memory_space=pltpu.VMEM)
        sem = pltpu.SemaphoreType.DMA((NUM_DEV,))
        v = pltpu.VMEM
        alpha, gx, g2 = pl.pallas_call(
            kernel,
            out_shape=(
                v((TASKS, 128), F32),
                v((NUM_DEV, FEAT, HID), F32),
                v((FLAT, 128), F32),
            ),
            in_specs=[hbm, hbm, hbm, hbm, hbm, hbm],
            out_specs=(vmem, vmem, vmem),
            scratch_shapes=[
                v((CLASSES, TASKS, DIM), BF16),
                v((TASKS, TOK), jnp.int32),
                v((TASKS, TOK), jnp.int32),
                v((NUM_DEV, TOK, DIM), BF16),
                v((NCHUNK, DIM, CHUNK), BF16),
                v((NCHUNK, CHUNK, DIM), BF16),
                v((DIM, HID), BF16),
                v((HID, DIM), BF16),
                v((HID, DIM), BF16),
                v((ROWS, CHUNK), BF16),
                v((ROWS, CHUNK), BF16),
                v((TOK, DIM), F32),
                v((HEAD_ROWS, DIM), F32),
                v((TASKS * CLASSES, DIM, 128), F32),
                v((HEAD_ROWS, TOK), F32),
                v((NUM_DEV, HEAD_ROWS, TOK), BF16),
                v((2, TASKS, 8, TOK), F32),
                v((HID, PITCH), BF16),
                v((HID, PITCH), BF16),
                v((HID, TOK), F32),
                v((HID, TOK), F32),
                v((DIM, PITCH), BF16),
                v((DIM, PITCH), BF16),
                v((HID, PITCH), BF16),
                v((HID, PITCH), BF16),
                v((TASKS, HID, DIM), F32),
                v((TASKS, HID, DIM), F32),
                v((NUM_DEV, 8, 128), F32),
                v((8, DIM), F32),
                v((NUM_DEV, 16, 128), F32),
                v((DIM, HID), F32),
                sem, sem, sem, sem, sem, sem, sem, sem, sem, sem, sem, sem,
                pltpu.SemaphoreType.DMA((6 + 2 * NCHUNK,)),
            ],
            compiler_params=pltpu.CompilerParams(collective_id=0, has_side_effects=True, vmem_limit_bytes=62_000_000),
            name="trunk",
        )(x_loc, w_in, w_out, heads.transpose(2, 0, 1), lab_loc, mask_loc)
        smem = pl.BlockSpec(memory_space=pltpu.SMEM)
        alpha, out1, out2 = pl.pallas_call(
            finish,
            out_shape=(
                jax.ShapeDtypeStruct((TASKS,), F32),
                jax.ShapeDtypeStruct((FLAT, 128), F32),
                jax.ShapeDtypeStruct((FLAT, 128), F32),
            ),
            in_specs=[vmem, vmem, vmem],
            out_specs=(smem, hbm, hbm),
            scratch_shapes=[
                v((FLAT, 128), F32),
                pltpu.SemaphoreType.DMA((3,)),
            ],
            compiler_params=pltpu.CompilerParams(vmem_limit_bytes=8_000_000),
            name="finish",
        )(alpha, gx, g2)
        return alpha, out1.reshape(-1), out2.reshape(-1)

    return jax.shard_map(local_step, mesh=mesh, in_specs=(P("data", None), P(), P(), P(), P(None, "data"), P(None, "data")), out_specs=(P(), P("data"), P("data")), check_vma=False)
```

```python
import jax
import jax.numpy as jnp
from jax import lax
from jax.experimental import pallas as pl
from jax.experimental.pallas import tpu as pltpu
from jax.sharding import PartitionSpec as P

SOLVER_STEPS = 20
MESH = pl.DeviceIdType.MESH
F32, BF16 = jnp.float32, jnp.bfloat16
NUM_DEV = 8
TASKS = 4
CLASSES = 3
TOK = 1024
DIM = 768
HIDDEN = 3072
HID = HIDDEN // NUM_DEV
FEAT = DIM // NUM_DEV
HEAD_ROWS = 32
PITCH = TOK + 128
CHUNK = 768
ROWS = 512
NCHUNK = HIDDEN // CHUNK
QUARTER = TOK // TASKS
PAIRS = [(t, s) for t in range(TASKS) for s in range(t, TASKS)]
GELU_C = 0.7978845608028654
GELU_K = 0.044715


def dot_nn(a, b):
    return lax.dot_general(a, b, (((1,), (0,)), ((), ())), preferred_element_type=F32)


def dot_nt(a, b):
    return lax.dot_general(a, b, (((1,), (1,)), ((), ())), preferred_element_type=F32)


def lanes(row, width):
    return jnp.concatenate([row] * (width // row.shape[1]), axis=1)


def gelu_parts(p):
    a = (GELU_C * GELU_K) * (p * p)
    th = jnp.tanh(p * (a + GELU_C))
    return a, th, 0.5 + 0.5 * th


def gelu_value(p):
    return p * gelu_parts(p)[2]


def gelu_both(p):
    a, th, cdf = gelu_parts(p)
    slope = cdf + ((1.0 - th * th) * p) * (1.5 * a + 0.5 * GELU_C)
    return p * cdf, slope


def kernel(x_hbm, w_in_hbm, w_out_hbm, head_ref, lab_ref, mask_ref, alpha_ref, gx, stage2,
           xs, w1, w2, w1j, w1t, w2j, abuf0, abuf1, zacc, hrow, hbc, ef, es, ecur, act0, act1, slope0, slope1,
           dz0, dz1, q0, q1, acc1, acc2, cnt, inv, gram, gsend,
           x_send, x_recv, f_send, f_recv, e_send, e_recv, c_send, c_recv, g_send, g_recv, o_send, o_recv, l_sem):
    me = lax.axis_index("data")
    core = lax.rem(me, 2)
    cx = lax.rem(lax.div(me, 2), 2)
    cy = lax.div(me, 4)

    def flip(v, b):
        return v + b - 2 * v * b

    def peer(s):
        return flip(cx, s // 2 % 2) * 2 + flip(cy, s // 4) * 4 + flip(core, jnp.int32(s % 2))

    def remote(src, dst, send, recv, dev):
        return pltpu.make_async_remote_copy(src_ref=src, dst_ref=dst, send_sem=send, recv_sem=recv, device_id=(dev,), device_id_type=MESH)

    half = pl.ds(pl.multiple_of(core * ROWS, ROWS), ROWS)
    x_dev, y_dev = peer(2), peer(4)
    first_dev = core * y_dev + (1 - core) * x_dev
    second_dev = core * x_dev + (1 - core) * y_dev

    def swap_copy():
        return remote(x_hbm, xs.at[1], x_send.at[1], x_recv.at[1], peer(1))

    def hop(src, dst, i, dev):
        return remote(xs.at[src, half, :], xs.at[dst, half, :], x_send.at[i], x_recv.at[dst], dev)

    def arrived(m):
        return hop(0, m, 2, x_dev)

    hops = {
        2: lambda: remote(x_hbm.at[half, :], xs.at[2 + core, half, :], x_send.at[2], x_recv.at[2 + core], first_dev),
        3: lambda: hop(1, 3 - core, 3, second_dev),
        4: lambda: hop(1, 4 + core, 4, first_dev),
        5: lambda: hop(0, 5 - core, 5, second_dev),
        6: lambda: hop(2 + 3 * core, 6, 6, second_dev),
        7: lambda: hop(4 - core, 7, 7, second_dev),
    }

    def hand(m):
        return remote(xs.at[m, half, :], xs.at[m, half, :], f_send.at[m], f_recv.at[m], peer(1))

    def arrival_slot(s):
        bx, by = s // 2 % 2, s // 4
        return 6 + core if bx and by else 2 + 2 * core if bx else 5 - 2 * core if by else 1

    def e_copy(s):
        slot = arrival_slot(s)
        return remote(es.at[0], es.at[slot], e_send.at[s], e_recv.at[slot], peer(s))

    def e_arrived(slot):
        return remote(es.at[0], es.at[slot], e_send.at[1], e_recv.at[slot], peer(1))

    def c_copy(s):
        return remote(cnt.at[0], cnt.at[s], c_send.at[s], c_recv.at[s], peer(s))

    def local(src, dst, i):
        return pltpu.make_async_copy(src, dst, l_sem.at[i])

    def load_w1(i):
        return local(w_in_hbm.at[:, pl.ds(pl.multiple_of(CHUNK * i, CHUNK), CHUNK)], w1.at[i], 3 + i)

    def load_w2(i):
        return local(w_out_hbm.at[pl.ds(pl.multiple_of(CHUNK * i, CHUNK), CHUNK), :], w2.at[i], 3 + NCHUNK + i)

    load_x = local(x_hbm, xs.at[0], 0)
    load_w1j = local(w_in_hbm.at[:, pl.ds(pl.multiple_of(me * HID, HID), HID)], w1j, 1)
    load_w2j = local(w_out_hbm.at[pl.ds(pl.multiple_of(me * HID, HID), HID), :], w2j, 2)
    load_x.start()
    load_w1j.start()
    load_w1(0).start()
    load_w2(0).start()

    barrier = pltpu.get_barrier_semaphore()
    for s in range(1, NUM_DEV):
        pl.semaphore_signal(barrier, inc=1, device_id=(peer(s),), device_id_type=MESH)

    counts = jnp.sum(mask_ref[...].astype(F32), axis=1, keepdims=True)
    cnt[0, 0:TASKS, :] = jnp.broadcast_to(counts, (TASKS, 128))
    cnt[0, TASKS:8, :] = jnp.zeros((8 - TASKS, 128), F32)
    hrow[...] = jnp.zeros_like(hrow)
    for c in range(CLASSES):
        hrow[8 * c:8 * c + TASKS, :] = head_ref[c].astype(F32)
    head = hrow[...].astype(BF16)

    pl.semaphore_wait(barrier, NUM_DEV - 1)
    hops[2]().start()
    swap_copy().start()
    for s in range(1, NUM_DEV):
        c_copy(s).start()

    block = lax.div(lax.broadcasted_iota(jnp.int32, (HEAD_ROWS, TASKS * CLASSES * 128), 1), 128)
    pick = lax.rem(block, CLASSES) * 8 + lax.div(block, CLASSES)
    ones = (lax.broadcasted_iota(jnp.int32, block.shape, 0) == pick).astype(F32).astype(BF16)
    wide = dot_nn(hrow[...].T.astype(BF16), ones)
    for k in range(TASKS * CLASSES):
        hbc[k] = wide[:, 128 * k:128 * k + 128]
    load_x.wait()
    for i in range(1, NCHUNK):
        load_w1(i).start()
        load_w2(i).start()
    load_w2j.start()

    load_w1j.wait()
    w1t[...] = w1j[...].astype(F32).T.astype(BF16)

    abuf1[...] = jnp.zeros_like(abuf1)
    zacc[...] = xs[0].astype(F32)
    half0, half1 = slice(0, ROWS), slice(ROWS, TOK)

    acts, slopes, dzs, qs = (act0, act1), (slope0, slope1), (dz0, dz1), (q0, q1)

    def preact(slot, part, quarter):
        r = pl.ds(pl.multiple_of(quarter * QUARTER, QUARTER), QUARTER)
        a, sl = gelu_both(dot_nt(w1t[...], xs[slot, r, :]))
        acts[part][:, r] = a.astype(BF16)
        slopes[part][:, r] = sl

    def forward(h, carry):
        load_w1(h).wait()
        load_w2(h).wait()
        acc1[h] = jnp.zeros((HID, DIM), F32)
        acc2[h] = jnp.zeros((HID, DIM), F32)
        @pl.when(h == 1)
        def _():
            swap_copy().wait_recv()
            hops[3]().start()

        abuf0[...] = gelu_value(dot_nn(xs[0, half0, :], w1[h])).astype(BF16)
        zacc[half1, :] += dot_nn(abuf1[...], w2[jnp.maximum(h - 1, 0)])
        abuf1[...] = gelu_value(dot_nn(xs[0, half1, :], w1[h])).astype(BF16)
        zacc[half0, :] += dot_nn(abuf0[...], w2[h])
        preact(0, 0, h)
        return carry

    lax.fori_loop(0, NCHUNK, forward, 0)
    zacc[half1, :] += dot_nn(abuf1[...], w2[NCHUNK - 1])

    for r in range(TOK // ROWS):
        cols = slice(r * ROWS, (r + 1) * ROWS)
        logits = dot_nt(head, zacc[cols, :].astype(BF16))
        l = [logits[8 * c:8 * c + TASKS] for c in range(CLASSES)]
        top = jnp.maximum(jnp.maximum(l[0], l[1]), l[2])
        ex = [jnp.exp(v - top) for v in l]
        total = ex[0] + ex[1] + ex[2]
        lab = lab_ref[:, cols]
        m = mask_ref[:, cols].astype(F32)
        for c in range(CLASSES):
            err = m * (ex[c] / total - (lab == c).astype(F32))
            for t in range(TASKS):
                ef[8 * t + c:8 * t + c + 1, cols] = err[t:t + 1]
    for t in range(TASKS):
        ef[8 * t + CLASSES:8 * t + 8, :] = jnp.zeros((8 - CLASSES, TOK), F32)
    es[0] = ef[...].astype(BF16)
    for t in range(TASKS):
        ecur[0, t] = es[0, 8 * t:8 * t + 8, :].astype(F32)

    def make_dz(dst, part, t):
        e = ecur[part, t]
        rows = [jnp.broadcast_to(e[c:c + 1, :], (8, TOK)) for c in range(CLASSES)]
        for k in range(DIM // 8):
            f = slice(8 * k, 8 * k + 8)
            h = [lanes(hbc[CLASSES * t + c, f, :], TOK) for c in range(CLASSES)]
            dst[f, 0:TOK] = (h[0] * rows[0] + h[1] * rows[1] + h[2] * rows[2]).astype(BF16)

    for s in range(1, NUM_DEV):
        e_copy(s).start()
    make_dz(dz0, 0, 0)
    load_w2j.wait()
    total_cnt = cnt[0]
    for s in range(1, NUM_DEV):
        c_copy(s).wait_recv()
        total_cnt = total_cnt + cnt[s]
    inv[...] = lanes(1.0 / jnp.maximum(total_cnt, 1.0), DIM)

    def link_half_ready(s):
        for k, slots in ((1, (2, 3)), (3, (4, 5)), (5, (6,)), (6, (7,))):
            @pl.when(s == k)
            def _():
                for m in slots:
                    arrived(m).wait_recv()
                    hand(m).start()
                if k == 3:
                    hops[6]().start()
                    hops[7]().start()

    def other_half_ready(s):
        for m in range(2, NUM_DEV):
            @pl.when(s == m - 1)
            def _():
                hand(m).wait_recv()

    def errors_ready(s, part):
        for k in range(1, NUM_DEV):
            @pl.when(s == k - 1)
            def _():
                e_arrived(k).wait_recv()
                for t in range(TASKS):
                    ecur[part, t] = es[k, 8 * t:8 * t + 8, :].astype(F32)

    def run_task(s, part, t, j, next_part, next_t):
        nxt = jnp.minimum(s + 1, NUM_DEV - 1)
        scale = inv[pl.ds(t, 1), :]
        qs[j][:, 0:TOK] = (dot_nn(w2j[...], dzs[j][:, 0:TOK]) * slopes[part][...]).astype(BF16)
        acc2[t] += (dot_nt(acts[part][:, 0:TOK], dzs[j][:, 0:TOK]) * scale).astype(BF16).astype(F32)
        make_dz(dzs[1 - j], next_part, next_t)
        preact(nxt, 1 - part, lax.rem(t + 2 * core, TASKS))
        acc1[t] += (dot_nn(qs[j][:, 0:TOK], xs[s]) * scale).astype(BF16).astype(F32)

    def shard_pair(sp, carry):
        for part in range(2):
            s = 2 * sp + part
            link_half_ready(s)

            def task_pair(tp, c):
                @pl.when(tp == 1)
                def _():
                    errors_ready(s, 1 - part)
                    other_half_ready(s)

                run_task(s, part, 2 * tp, 0, part, 2 * tp + 1)
                wrap = lax.div(2 * tp + 2, TASKS)
                run_task(s, part, 2 * tp + 1, 1, part + wrap * (1 - 2 * part), 2 * tp + 2 - TASKS * wrap)
                return c

            lax.fori_loop(0, TASKS // 2, task_pair, 0)
        return carry

    hops[4]().start()
    hops[5]().start()
    lax.fori_loop(0, NUM_DEV // 2, shard_pair, 0)

    def gram_rows(i, sums):
        r = pl.ds(pl.multiple_of(i * 8, 8), 8)
        out = list(sums)
        for acc in (acc1, acc2):
            for c in range(DIM // 128):
                g = [acc[t, r, 128 * c:128 * c + 128] for t in range(TASKS)]
                for k, (t, u) in enumerate(PAIRS):
                    out[k] = out[k] + g[t] * g[u]
        return tuple(out)

    sums = lax.fori_loop(0, HID // 8, gram_rows, tuple(jnp.zeros((8, 128), F32) for _ in PAIRS))
    for k in range(len(PAIRS)):
        gram[me, k:k + 1, :] = jnp.broadcast_to(jnp.sum(sums[k]), (1, 128))
    gram[me, len(PAIRS):16, :] = jnp.zeros((16 - len(PAIRS), 128), F32)

    def gram_copy(s, block):
        return remote(gram.at[block], gram.at[block], g_send.at[s], g_recv.at[s], peer(s))

    for s in range(1, NUM_DEV):
        gram_copy(s, me).start()
    for s in range(1, NUM_DEV):
        gram_copy(s, me).wait_recv()
    gram_sum = gram[0]
    for d in range(1, NUM_DEV):
        gram_sum = gram_sum + gram[d]
    m = {}
    for k, (t, u) in enumerate(PAIRS):
        m[t, u] = m[u, t] = gram_sum[k:k + 1, :]
    step_scale = (m[0, 0] + m[1, 1] + m[2, 2] + m[3, 3]) / TASKS
    al = [jnp.full((1, 128), 1.0 / TASKS, F32) for _ in range(TASKS)]
    for _ in range(SOLVER_STEPS):
        raised = []
        for t in range(TASKS):
            pull = (m[t, 0] * al[0] + m[t, 1] * al[1]) + (m[t, 2] * al[2] + m[t, 3] * al[3])
            raised.append(al[t] * jnp.exp(-pull / step_scale))
        norm = (raised[0] + raised[1]) + (raised[2] + raised[3])
        al = [r / norm for r in raised]
    for t in range(TASKS):
        alpha_ref[t:t + 1, :] = al[t]

    for c in range(DIM // 128):
        cols = slice(128 * c, 128 * c + 128)
        comb = al[0] * acc1[0, :, cols]
        for t in range(1, TASKS):
            comb = comb + al[t] * acc1[t, :, cols]
        gsend[cols, :] = comb.T

    def o_copy(s):
        dev = peer(s)
        rows = pl.ds(pl.multiple_of(dev * FEAT, FEAT), FEAT)
        return remote(gsend.at[rows, :], gx.at[me], o_send.at[s], o_recv.at[s], dev)

    order = (2, 4, 3, 5, 6, 7, 1)
    for s in order:
        o_copy(s).start()

    for c in range(DIM // 128):
        cols = slice(128 * c, 128 * c + 128)
        comb = al[0] * acc2[0, :, cols]
        for t in range(1, TASKS):
            comb = comb + al[t] * acc2[t, :, cols]
        stage2[pl.ds(c, HID, stride=DIM // 128), :] = comb

    gx[me] = gsend[pl.ds(pl.multiple_of(me * FEAT, FEAT), FEAT), :]
    for s in range(1, NUM_DEV):
        o_copy(s).wait_recv()

    swap_copy().wait_send()
    for m in range(2, NUM_DEV):
        hops[m]().wait_send()
        hand(m).wait_send()
    for s in range(1, NUM_DEV):
        e_copy(s).wait_send()
        c_copy(s).wait_send()
        gram_copy(s, me).wait_send()
        o_copy(s).wait_send()


PER = HID // 128
FLAT = DIM * HIDDEN // NUM_DEV // 128
HALF = FEAT // 2


def finish(alpha_in, blocks, stage2, alpha_ref, out1_hbm, out2_hbm, stage1, out_sem):
    stores = [pltpu.make_async_copy(stage2, out2_hbm, out_sem.at[2])]
    stores[0].start()
    for t in range(TASKS):
        alpha_ref[t] = jnp.max(alpha_in[t:t + 1, :])
    for h in range(2):
        for d in range(NUM_DEV):
            for b in range(PER):
                first = h * HALF * (HIDDEN // 128) + d * PER + b
                stage1[pl.ds(first, HALF, stride=HIDDEN // 128), :] = blocks[d, h * HALF:h * HALF + HALF, 128 * b:128 * b + 128]
        rows = pl.ds(h * FLAT // 2, FLAT // 2)
        stores.append(pltpu.make_async_copy(stage1.at[rows, :], out1_hbm.at[rows, :], out_sem.at[h]))
        stores[-1].start()
    for c in stores:
        c.wait()


def solution(mesh):
    def local_step(x_loc, w_in, w_out, heads, lab_loc, mask_loc):
        hbm = pl.BlockSpec(memory_space=pl.ANY)
        vmem = pl.BlockSpec(memory_space=pltpu.VMEM)
        sem = pltpu.SemaphoreType.DMA((NUM_DEV,))
        v = pltpu.VMEM
        alpha, gx, g2 = pl.pallas_call(
            kernel,
            out_shape=(
                v((TASKS, 128), F32),
                v((NUM_DEV, FEAT, HID), F32),
                v((FLAT, 128), F32),
            ),
            in_specs=[hbm, hbm, hbm, vmem, vmem, vmem],
            out_specs=(vmem, vmem, vmem),
            scratch_shapes=[
                v((NUM_DEV, TOK, DIM), BF16),
                v((NCHUNK, DIM, CHUNK), BF16),
                v((NCHUNK, CHUNK, DIM), BF16),
                v((DIM, HID), BF16),
                v((HID, DIM), BF16),
                v((HID, DIM), BF16),
                v((ROWS, CHUNK), BF16),
                v((ROWS, CHUNK), BF16),
                v((TOK, DIM), F32),
                v((HEAD_ROWS, DIM), F32),
                v((TASKS * CLASSES, DIM, 128), F32),
                v((HEAD_ROWS, TOK), F32),
                v((NUM_DEV, HEAD_ROWS, TOK), BF16),
                v((2, TASKS, 8, TOK), F32),
                v((HID, PITCH), BF16),
                v((HID, PITCH), BF16),
                v((HID, TOK), F32),
                v((HID, TOK), F32),
                v((DIM, PITCH), BF16),
                v((DIM, PITCH), BF16),
                v((HID, PITCH), BF16),
                v((HID, PITCH), BF16),
                v((TASKS, HID, DIM), F32),
                v((TASKS, HID, DIM), F32),
                v((NUM_DEV, 8, 128), F32),
                v((8, DIM), F32),
                v((NUM_DEV, 16, 128), F32),
                v((DIM, HID), F32),
                sem, sem, sem, sem, sem, sem, sem, sem, sem, sem, sem, sem,
                pltpu.SemaphoreType.DMA((3 + 2 * NCHUNK,)),
            ],
            compiler_params=pltpu.CompilerParams(collective_id=0, has_side_effects=True, vmem_limit_bytes=62_000_000),
            name="trunk",
        )(x_loc, w_in, w_out, heads.transpose(2, 0, 1), lab_loc, mask_loc)
        smem = pl.BlockSpec(memory_space=pltpu.SMEM)
        alpha, out1, out2 = pl.pallas_call(
            finish,
            out_shape=(
                jax.ShapeDtypeStruct((TASKS,), F32),
                jax.ShapeDtypeStruct((FLAT, 128), F32),
                jax.ShapeDtypeStruct((FLAT, 128), F32),
            ),
            in_specs=[vmem, vmem, vmem],
            out_specs=(smem, hbm, hbm),
            scratch_shapes=[
                v((FLAT, 128), F32),
                pltpu.SemaphoreType.DMA((3,)),
            ],
            compiler_params=pltpu.CompilerParams(vmem_limit_bytes=8_000_000),
            name="finish",
        )(alpha, gx, g2)
        return alpha, out1.reshape(-1), out2.reshape(-1)

    return jax.shard_map(local_step, mesh=mesh, in_specs=(P("data", None), P(), P(), P(), P(None, "data"), P(None, "data")), out_specs=(P(), P("data"), P("data")), check_vma=False)
```
